128 devices in a mesh: fsdp: 8 (over x_lo, y), seq: 16 (over x_hi, z, core).
Axes of the slice: x: 4 (x_hi: 2, x_lo: 2; x = x_hi * 2 + x_lo), y: 4, z: 4, core: 2. Of those that a mesh axis runs over, the one named last changes fastest.
Arguments:
- image_input: bfloat16 [8, 2048, 1536], P('fsdp', 'seq'), may hold values from -6 to 6
- text_input: bfloat16 [8, 128, 1536], P('fsdp'), may hold values from -6 to 6
- w_qkv: bfloat16 [1536, 3, 2048], P('fsdp'), may hold values from -0.15625 to 0.15625
- query_gain: float32 [128], replicated, may hold values from 1.2 to 2.4
- key_gain: float32 [128], replicated, may hold values from 1.2 to 2.4
- image_cotangent: bfloat16 [8, 2048, 2048], P('fsdp', 'seq'), may hold values from -6 to 6
- text_cotangent: bfloat16 [8, 128, 2048], P('fsdp'), may hold values from -6 to 6
Outputs:
- image_grad: bfloat16 [8, 2048, 1536], P('fsdp', 'seq')
- text_grad: bfloat16 [8, 128, 1536], P('fsdp')
- weight_grad: float32 [1536, 3, 2048], P('fsdp', None, 'seq')
- gain_grad: float32 [2, 128], replicated
The draws below stay inside these ranges and needn't reach their ends.
All inputs are finite; a program needn't handle non-finite values.
Results may differ from the reference program's by a relative error of at most 0.018.
The reference program's roundings to bfloat16 on the way count: a program that leaves them out, or rounds other values in their place, can miss the bound.
Values may be sent and summed in bfloat16 or wider, within the bound.
A program may use at most 192 MiB of HBM per device.

```python
import math
import jax
import jax.numpy as jnp
from jax import lax

D = 1536
HEADS = 16
HEAD = 128
TXT = 128
IMG_DEV = 128
B_DEV = 1
BATCH = 8
IMG = 2048
N_FSDP = 8
N_SEQ = 16


def steps_of(own_key, dims, cuts, smallest, high):
    factor_of, own = 1.0, jax.random.fold_in(own_key, 6)
    for dim, shards_of in cuts:
        steps = jnp.exp(jax.random.uniform(jax.random.fold_in(own, dim), (shards_of,), jnp.float32, smallest / len(cuts), high / len(cuts)))
        factor_of = factor_of * jnp.repeat(steps, dims[dim] // shards_of).reshape([-1 if axis == dim else 1 for axis in range(len(dims))])
    return factor_of


def gaussian(rng, shape, scale, reach, cuts=(), kind=jnp.bfloat16):
    result = jax.random.normal(rng, shape, jnp.float32) * scale
    if len(cuts) > 0:
        result = steps_of(rng, shape, cuts, -0.22, 0.18) * result
    return jnp.clip(result, min=-reach, max=reach).astype(kind)


def setup_inputs(seed: int = 0) -> dict:
    key_list = jax.random.split(jax.random.key(seed), 8)
    image_input = gaussian(key_list[0], (BATCH, IMG, D), 1.0, 6.0, ((0, 8), (1, 16)))
    text_input = gaussian(key_list[1], (BATCH, TXT, D), 1.0, 6.0, ((0, 8),))
    w_qkv = gaussian(key_list[2], (D, 3, HEADS * HEAD), D ** -0.5, 0.15625, ((0, 8),))
    query_gain = jnp.clip(jnp.exp(jax.random.uniform(key_list[3], (HEAD,), jnp.float32, math.log(1.2), math.log(2.4))), 1.2, 2.4)
    key_gain = jnp.clip(jnp.exp(jax.random.uniform(key_list[4], (HEAD,), jnp.float32, math.log(1.2), math.log(2.4))), 1.2, 2.4)
    image_cotangent = gaussian(key_list[5], (BATCH, IMG, HEADS * HEAD), 1.0, 6.0, ((0, 8), (1, 16)))
    text_cotangent = gaussian(key_list[6], (BATCH, TXT, HEADS * HEAD), 1.0, 6.0, ((0, 8),))
    return dict(image_input=image_input, text_input=text_input, w_qkv=w_qkv, query_gain=query_gain, key_gain=key_gain, image_cotangent=image_cotangent, text_cotangent=text_cotangent)


epsilon = 1e-06
query_parts = 4

def rms_forward(values, gain):
    floated = values.astype(jnp.float32)
    inverse = lax.rsqrt(lax.optimization_barrier(jnp.mean(floated * floated, axis=-1, keepdims=True)) + epsilon)
    return (floated, inverse, (floated * inverse * gain).astype(jnp.bfloat16))

def rms_backward(floated, inverse, gain, incoming):
    weighted = incoming * gain
    inner_mean = lax.optimization_barrier(jnp.mean(weighted * floated, axis=-1, keepdims=True))
    grad_input = inverse * weighted - floated * inverse * inverse * inverse * inner_mean
    grad_gain = lax.optimization_barrier(jnp.sum(incoming * floated * inverse, axis=0))
    return (grad_input, grad_gain)

def head_backward(query_rows, key_rows, value_rows, incoming, query_gain, key_gain):
    query_float, query_inverse, query_normed = rms_forward(query_rows, query_gain)
    key_float, key_inverse, key_normed = rms_forward(key_rows, key_gain)
    length = query_rows.shape[0]
    width = query_rows.shape[1]
    block_rows = length // query_parts
    factor = 1.0 / math.sqrt(width)
    query_blocks = query_normed.reshape(query_parts, block_rows, width)
    incoming_blocks = incoming.reshape(query_parts, block_rows, width)

    def visit(carried, pieces):
        key_total, value_total = carried
        query_piece, incoming_piece = pieces
        scores = jnp.dot(query_piece, key_normed.T, preferred_element_type=jnp.float32) * factor
        attention = jax.nn.softmax(scores, axis=-1)
        attention_grad = jnp.dot(incoming_piece, value_rows.T, preferred_element_type=jnp.float32)
        row_dot = lax.optimization_barrier(jnp.sum(attention * attention_grad, axis=-1, keepdims=True))
        score_grad = (attention * (attention_grad - row_dot)).astype(jnp.bfloat16)
        value_total = value_total + jnp.dot(attention.astype(jnp.bfloat16).T, incoming_piece, preferred_element_type=jnp.float32)
        key_total = key_total + jnp.dot(score_grad.T, query_piece, preferred_element_type=jnp.float32) * factor
        query_grad = jnp.dot(score_grad, key_normed, preferred_element_type=jnp.float32) * factor
        return ((key_total, value_total), query_grad)
    zeros_init = jnp.zeros((length, width), jnp.float32)
    (key_total, value_total), query_pieces = lax.scan(visit, (zeros_init, zeros_init), (query_blocks, incoming_blocks))
    query_grad = query_pieces.reshape(length, width)
    query_input_grad, query_gain_grad = rms_backward(query_float, query_inverse, query_gain, query_grad)
    key_input_grad, key_gain_grad = rms_backward(key_float, key_inverse, key_gain, key_total)
    stacked = jnp.stack([query_input_grad, key_input_grad, value_total], axis=1).astype(jnp.bfloat16)
    return (stacked, jnp.stack([query_gain_grad, key_gain_grad], axis=0))

def reference(image_input, text_input, w_qkv, query_gain, key_gain, image_cotangent, text_cotangent):
    tokens = jnp.concatenate([text_input, image_input], axis=1)
    upstream = jnp.concatenate([text_cotangent, image_cotangent], axis=1)
    weights = w_qkv.astype(jnp.float32)
    triple = jnp.einsum('btd,dch->btch', tokens.astype(jnp.float32), weights).astype(jnp.bfloat16)
    batch_count = triple.shape[0]
    length = triple.shape[1]
    by_heads = triple.reshape(batch_count, length, 3, HEADS, HEAD).transpose(0, 3, 1, 2, 4).reshape(batch_count * HEADS, length, 3, HEAD)
    incoming_heads = upstream.reshape(batch_count, length, HEADS, HEAD).transpose(0, 2, 1, 3).reshape(batch_count * HEADS, length, HEAD)

    def one_head(pair):
        inputs, incoming = pair
        return head_backward(inputs[:, 0], inputs[:, 1], inputs[:, 2], incoming, query_gain, key_gain)
    all_grads, gain_rows = lax.map(one_head, (by_heads, incoming_heads))
    triple_grad = all_grads.reshape(batch_count, HEADS, length, 3, HEAD).transpose(0, 2, 3, 1, 4).reshape(batch_count, length, 3, HEADS * HEAD)
    gain_grad = lax.optimization_barrier(jnp.sum(gain_rows, axis=0))
    full_grad = jnp.einsum('btch,dch->btd', triple_grad.astype(jnp.float32), weights).astype(jnp.bfloat16)
    text_grad = full_grad[:, :TXT]
    image_grad = full_grad[:, TXT:]
    head_group = jnp.arange(HEADS * HEAD, dtype=jnp.int32) // (HEAD * (HEADS // N_SEQ))
    zero_index = jnp.zeros((), jnp.int32)

    def over_groups(group_index, running):
        first_row = (group_index * B_DEV).astype(jnp.int32)
        text_block = lax.dynamic_slice_in_dim(text_input, first_row, B_DEV, 0).astype(jnp.float32)
        text_block_grad = lax.dynamic_slice_in_dim(triple_grad[:, :TXT], first_row, B_DEV, 0).astype(jnp.float32)
        text_part = jnp.einsum('btd,btch->dch', text_block, text_block_grad)

        def over_members(member_index, running_inner):
            image_start = (member_index * IMG_DEV).astype(jnp.int32)
            image_block = lax.dynamic_slice(image_input, (first_row, image_start, zero_index), (B_DEV, IMG_DEV, D)).astype(jnp.float32)
            block_grads = lax.dynamic_slice(triple_grad, (first_row, image_start + TXT, zero_index, zero_index), (B_DEV, IMG_DEV, 3, HEADS * HEAD)).astype(jnp.float32)
            column_mask = (head_group == member_index).astype(jnp.float32)
            partial_value = jnp.einsum('btd,btch->dch', image_block, block_grads) + text_part * column_mask
            rounded = lax.optimization_barrier(partial_value.astype(jnp.bfloat16))
            return running_inner + rounded.astype(jnp.float32)
        return lax.fori_loop(0, N_SEQ, over_members, running)
    weight_grad = lax.fori_loop(0, N_FSDP, over_groups, jnp.zeros((D, 3, HEADS * HEAD), jnp.float32))
    return (image_grad, text_grad, weight_grad, gain_grad)
```

```python
import math

import jax
import jax.numpy as jnp
from jax import lax
from jax.experimental import pallas as pl
from jax.experimental.pallas import tpu as pltpu
from jax.sharding import Mesh
from jax.sharding import PartitionSpec as P

HEADS = 16
HEAD = 128
SEQ = ("seq_0", "seq_1", "seq_2")
FSDP = ("fsdp_0", "fsdp_1")
FSDP_SEQ = ("fsdp_0", "fsdp_1", "seq_0", "seq_1", "seq_2")
EPS = 1e-06
F32 = jnp.float32
BF16 = jnp.bfloat16

Q_ROWS = 256
KEY_ROWS = 136


def dot_nt(a, b):
    return lax.dot_general(a, b, (((1,), (1,)), ((), ())), preferred_element_type=F32)


def dot_nn(a, b):
    return lax.dot_general(a, b, (((1,), (0,)), ((), ())), preferred_element_type=F32)


def folded(values):
    rows, width = values.shape
    return jnp.sum(values.reshape(rows // 8, 8, width), axis=0)


def attention_kernel(
    triple, upstream, qgain, kgain, grads, gains, qn, kn, kn_t, expd, dpd, dsd, dk, dv, gsum
):
    rows = triple.shape[0]
    factor = 1.0 / math.sqrt(HEAD)
    scale = factor * math.log2(math.e)

    def normed(values, gain):
        floated = values.astype(F32)
        inverse = lax.rsqrt(jnp.mean(floated * floated, axis=-1, keepdims=True) + EPS)
        return floated, inverse, (floated * inverse * gain).astype(BF16)

    qn[...] = normed(triple[:, 0:HEAD], qgain[...])[2]
    keys = normed(triple[:, HEAD : 2 * HEAD], kgain[...])[2]
    kn[...] = keys
    kn_t[...] = keys.T
    dk[...] = jnp.zeros_like(dk)
    dv[...] = jnp.zeros_like(dv)
    gsum[...] = jnp.zeros_like(gsum)

    def back(values, gain, incoming):
        floated = values.astype(F32)
        inverse = lax.rsqrt(jnp.mean(floated * floated, axis=-1, keepdims=True) + EPS)
        weighted = incoming * gain
        inner = jnp.mean(weighted * floated, axis=-1, keepdims=True)
        grad = inverse * weighted - floated * (inverse * inverse * inverse * inner)
        return grad, folded(incoming * floated * inverse)

    def block(start, count):
        qb = qn[pl.ds(start, count), :]
        ub = upstream[pl.ds(start, count), :]
        total = jnp.zeros((8, count), F32)
        inner = jnp.zeros((8, count), F32)
        for c in range(0, rows, KEY_ROWS):
            part = pl.ds(c, KEY_ROWS)
            e = jnp.exp2(dot_nt(kn[part, :], qb) * scale)
            d = dot_nt(triple[part, 2 * HEAD : 3 * HEAD], ub)
            expd[part, :count] = e
            dpd[part, :count] = d
            total = total + folded(e)
            inner = inner + folded(e * d)
        recip = 1.0 / jnp.sum(total, axis=0, keepdims=True)
        delta = jnp.sum(inner, axis=0, keepdims=True) * recip
        for c in range(0, rows, KEY_ROWS):
            part = pl.ds(c, KEY_ROWS)
            p = expd[part, :count] * recip
            ds = (p * (dpd[part, :count] - delta)).astype(BF16)
            dsd[part, :count] = ds
            dv[part, :] += dot_nn(p.astype(BF16), ub)
            dk[part, :] += dot_nn(ds, qb)
        dq_t = dot_nn(kn_t[...], dsd[:, :count])
        dq = dq_t.T * factor
        grad, gain_part = back(triple[pl.ds(start, count), 0:HEAD], qgain[...], dq)
        grads[pl.ds(start, count), 0:HEAD] = grad.astype(BF16)
        gsum[0:8, :] += gain_part

    image_rows = rows // Q_ROWS * Q_ROWS

    def step(i, carry):
        block(pl.multiple_of(i * Q_ROWS, Q_ROWS), Q_ROWS)
        return carry

    lax.fori_loop(0, image_rows // Q_ROWS, step, 0)
    if rows > image_rows:
        block(image_rows, rows - image_rows)
    grad, gain_part = back(triple[:, HEAD : 2 * HEAD], kgain[...], dk[...] * factor)
    grads[:, HEAD : 2 * HEAD] = grad.astype(BF16)
    grads[:, 2 * HEAD : 3 * HEAD] = dv[...].astype(BF16)
    gsum[8:16, :] = gain_part
    gains[0:1, :] = jnp.sum(gsum[0:8, :], axis=0, keepdims=True)
    gains[1:2, :] = jnp.sum(gsum[8:16, :], axis=0, keepdims=True)


def attention(triple, upstream, query_gain, key_gain):
    rows = triple.shape[0]
    vmem = pl.BlockSpec(memory_space=pltpu.VMEM)
    return pl.pallas_call(
        attention_kernel,
        out_shape=(
            jax.ShapeDtypeStruct((rows, 3 * HEAD), BF16),
            jax.ShapeDtypeStruct((2, HEAD), F32),
        ),
        in_specs=[vmem] * 4,
        out_specs=(vmem, vmem),
        scratch_shapes=[
            pltpu.VMEM((rows, HEAD), BF16),
            pltpu.VMEM((rows, HEAD), BF16),
            pltpu.VMEM((HEAD, rows), BF16),
            pltpu.VMEM((rows, Q_ROWS), F32),
            pltpu.VMEM((rows, Q_ROWS), F32),
            pltpu.VMEM((rows, Q_ROWS), BF16),
            pltpu.VMEM((rows, HEAD), F32),
            pltpu.VMEM((rows, HEAD), F32),
            pltpu.VMEM((16, HEAD), F32),
        ],
        compiler_params=pltpu.CompilerParams(vmem_limit_bytes=48 * 1024 * 1024),
        cost_estimate=pl.CostEstimate(
            flops=10 * rows * rows * HEAD, bytes_accessed=8 * rows * HEAD, transcendentals=rows * rows
        ),
        name="attention",
    )(triple, upstream, query_gain.reshape(1, HEAD), key_gain.reshape(1, HEAD))


def local(image_input, text_input, w_qkv, query_gain, key_gain, image_cotangent, text_cotangent):
    own_index = lax.axis_index(SEQ)
    offset = own_index * HEAD
    features = image_input.shape[2]
    image_rows_dev = image_input.shape[1]
    text_rows = text_input.shape[1]
    own = lax.dynamic_slice_in_dim(w_qkv, offset, HEAD, 2).reshape(w_qkv.shape[0], 3 * HEAD)
    weights = lax.all_gather(own, FSDP, axis=0, tiled=True)
    whole_image = lax.all_gather(image_input[0], SEQ, axis=0, tiled=True)
    image_rows = whole_image.shape[0]
    arrived = lax.all_to_all(image_cotangent[0], SEQ, split_axis=1, concat_axis=0, tiled=True)
    text_up = lax.dynamic_slice_in_dim(text_cotangent[0], offset, HEAD, 1)
    upstream = jnp.concatenate([arrived, text_up], axis=0)
    tokens = jnp.concatenate([whole_image, text_input[0]], axis=0)
    triple = jnp.dot(tokens, weights, preferred_element_type=F32).astype(BF16)
    grads, gain_part = attention(triple, upstream, query_gain, key_gain)
    gain_total = lax.psum(gain_part, FSDP_SEQ)
    head_total = lax.dot_general(tokens, grads, (((0,), (0,)), ((), ())), preferred_element_type=F32)
    grad_weights = lax.psum_scatter(
        head_total.astype(BF16), FSDP, scatter_dimension=0, tiled=True
    ).astype(F32)
    partial = lax.dot_general(grads, weights, (((1,), (1,)), ((), ())), preferred_element_type=F32)
    partial = partial.astype(BF16)
    image_out = lax.psum_scatter(partial[:image_rows], SEQ, scatter_dimension=0, tiled=True)
    text_out = lax.psum(partial[image_rows:], SEQ)
    return (
        image_out.reshape(1, image_rows_dev, features),
        text_out.reshape(1, text_rows, features),
        grad_weights.reshape(-1, 3, HEAD),
        gain_total,
    )


def solution(mesh):
    finer = Mesh(
        mesh.devices.reshape(2, 4, 2, 4, 2), ("fsdp_0", "fsdp_1", "seq_0", "seq_1", "seq_2")
    )
    return jax.shard_map(
        local,
        mesh=finer,
        in_specs=(
            P(FSDP, SEQ, None),
            P(FSDP, None, None),
            P(FSDP, None, None),
            P(),
            P(),
            P(FSDP, SEQ, None),
            P(FSDP, None, None),
        ),
        out_specs=(P(FSDP, SEQ, None), P(FSDP, None, None), P(FSDP, None, SEQ), P()),
        check_vma=False,
    )
```

```python
import math

import jax
import jax.numpy as jnp
from jax import lax
from jax.experimental import pallas as pl
from jax.experimental.pallas import tpu as pltpu
from jax.sharding import Mesh
from jax.sharding import PartitionSpec as P

HEADS = 16
HEAD = 128
SEQ = ("seq_0", "seq_1", "seq_2")
FSDP = ("fsdp_0", "fsdp_1")
FSDP_SEQ = ("fsdp_0", "fsdp_1", "seq_0", "seq_1", "seq_2")
EPS = 1e-06
F32 = jnp.float32
BF16 = jnp.bfloat16

Q_ROWS = 256
KEY_ROWS = 136


def dot_nt(a, b):
    return lax.dot_general(a, b, (((1,), (1,)), ((), ())), preferred_element_type=F32)


def dot_nn(a, b):
    return lax.dot_general(a, b, (((1,), (0,)), ((), ())), preferred_element_type=F32)


def folded(values):
    rows, width = values.shape
    return jnp.sum(values.reshape(rows // 8, 8, width), axis=0)


def attention_kernel(
    triple, upstream, qgain, kgain, grads, gains, qn, kn, kn_t, expd, dpd, dsd, dk, dv, gsum
):
    rows = triple.shape[0]
    factor = 1.0 / math.sqrt(HEAD)
    scale = factor * math.log2(math.e)

    def normed(values, gain):
        floated = values.astype(F32)
        inverse = lax.rsqrt(jnp.mean(floated * floated, axis=-1, keepdims=True) + EPS)
        return floated, inverse, (floated * inverse * gain).astype(BF16)

    qn[...] = normed(triple[:, 0:HEAD], qgain[...])[2]
    keys = normed(triple[:, HEAD : 2 * HEAD], kgain[...])[2]
    kn[...] = keys
    kn_t[...] = keys.T
    dk[...] = jnp.zeros_like(dk)
    dv[...] = jnp.zeros_like(dv)
    gsum[...] = jnp.zeros_like(gsum)

    def back(values, gain, incoming):
        floated = values.astype(F32)
        inverse = lax.rsqrt(jnp.mean(floated * floated, axis=-1, keepdims=True) + EPS)
        weighted = incoming * gain
        inner = jnp.mean(weighted * floated, axis=-1, keepdims=True)
        grad = inverse * weighted - floated * (inverse * inverse * inverse * inner)
        return grad, folded(incoming * floated * inverse)

    def block(start, count):
        qb = qn[pl.ds(start, count), :]
        ub = upstream[pl.ds(start, count), :]
        total = jnp.zeros((8, count), F32)
        inner = jnp.zeros((8, count), F32)
        for c in range(0, rows, KEY_ROWS):
            part = pl.ds(c, KEY_ROWS)
            e = jnp.exp2(dot_nt(kn[part, :], qb) * scale)
            d = dot_nt(triple[part, 2 * HEAD : 3 * HEAD], ub)
            expd[part, :count] = e
            dpd[part, :count] = d
            total = total + folded(e)
            inner = inner + folded(e * d)
        recip = 1.0 / jnp.sum(total, axis=0, keepdims=True)
        delta = jnp.sum(inner, axis=0, keepdims=True) * recip
        for c in range(0, rows, KEY_ROWS):
            part = pl.ds(c, KEY_ROWS)
            p = expd[part, :count] * recip
            ds = (p * (dpd[part, :count] - delta)).astype(BF16)
            dsd[part, :count] = ds
            dv[part, :] += dot_nn(p.astype(BF16), ub)
            dk[part, :] += dot_nn(ds, qb)
        dq_t = dot_nn(kn_t[...], dsd[:, :count])
        dq = dq_t.T * factor
        grad, gain_part = back(triple[pl.ds(start, count), 0:HEAD], qgain[...], dq)
        grads[pl.ds(start, count), 0:HEAD] = grad.astype(BF16)
        gsum[0:8, :] += gain_part

    image_rows = rows // Q_ROWS * Q_ROWS

    def step(i, carry):
        block(pl.multiple_of(i * Q_ROWS, Q_ROWS), Q_ROWS)
        return carry

    lax.fori_loop(0, image_rows // Q_ROWS, step, 0)
    if rows > image_rows:
        block(image_rows, rows - image_rows)
    grad, gain_part = back(triple[:, HEAD : 2 * HEAD], kgain[...], dk[...] * factor)
    grads[:, HEAD : 2 * HEAD] = grad.astype(BF16)
    grads[:, 2 * HEAD : 3 * HEAD] = dv[...].astype(BF16)
    gsum[8:16, :] = gain_part
    gains[0:1, :] = jnp.sum(gsum[0:8, :], axis=0, keepdims=True)
    gains[1:2, :] = jnp.sum(gsum[8:16, :], axis=0, keepdims=True)


def attention(triple, upstream, query_gain, key_gain):
    rows = triple.shape[0]
    vmem = pl.BlockSpec(memory_space=pltpu.VMEM)
    return pl.pallas_call(
        attention_kernel,
        out_shape=(
            jax.ShapeDtypeStruct((rows, 3 * HEAD), BF16),
            jax.ShapeDtypeStruct((2, HEAD), F32),
        ),
        in_specs=[vmem] * 4,
        out_specs=(vmem, vmem),
        scratch_shapes=[
            pltpu.VMEM((rows, HEAD), BF16),
            pltpu.VMEM((rows, HEAD), BF16),
            pltpu.VMEM((HEAD, rows), BF16),
            pltpu.VMEM((rows, Q_ROWS), F32),
            pltpu.VMEM((rows, Q_ROWS), F32),
            pltpu.VMEM((rows, Q_ROWS), BF16),
            pltpu.VMEM((rows, HEAD), F32),
            pltpu.VMEM((rows, HEAD), F32),
            pltpu.VMEM((16, HEAD), F32),
        ],
        compiler_params=pltpu.CompilerParams(vmem_limit_bytes=48 * 1024 * 1024),
        cost_estimate=pl.CostEstimate(
            flops=10 * rows * rows * HEAD, bytes_accessed=8 * rows * HEAD, transcendentals=rows * rows
        ),
        name="attention",
    )(triple, upstream, query_gain.reshape(1, HEAD), key_gain.reshape(1, HEAD))


MESH = pl.DeviceIdType.MESH


class Copies:
    def __init__(self, send, recv):
        self.send, self.recv, self.made = send, recv, []

    def make(self, src, dst, to):
        i = len(self.made)
        copy = pltpu.make_async_remote_copy(
            src_ref=src,
            dst_ref=dst,
            send_sem=self.send.at[i],
            recv_sem=self.recv.at[i],
            device_id=to,
            device_id_type=MESH,
        )
        self.made.append(copy)
        return copy


def where():
    return (
        lax.axis_index("fsdp_0"),
        lax.axis_index("fsdp_1"),
        lax.axis_index("seq_0"),
        lax.axis_index("seq_1"),
        lax.axis_index("seq_2"),
    )


SEQ_OFFSETS = [(a, b, c) for a in range(2) for b in range(4) for c in range(2) if a + b + c > 0]
FSDP_OFFSETS = [(a, b) for a in range(2) for b in range(4) if a + b > 0]


def seq_peer(offset):
    _, _, xh, z, core = where()
    return (xh + offset[0]) % 2, (z + offset[1]) % 4, (core + offset[2]) % 2


def fsdp_peer(offset):
    xl, y, _, _, _ = where()
    return (xl + offset[0]) % 2, (y + offset[1]) % 4


def seq_id(peer):
    return {"seq_0": peer[0], "seq_1": peer[1], "seq_2": peer[2]}


def fsdp_id(peer):
    return {"fsdp_0": peer[0], "fsdp_1": peer[1]}


class Ring:
    def __init__(self, copies, slot, pair_axis, pair, ring_axis, ring):
        self.planes = (pair, 1 - pair)
        self.ring = ring
        after, before = {ring_axis: (ring + 1) % 4}, {ring_axis: (ring + 3) % 4}
        other = {pair_axis: 1 - pair}

        def same(piece, to):
            return copies.make(piece, piece, to)

        self.cross = [same(slot(pair, ring, h), other) for h in range(2)]
        self.up = [[same(slot(p, ring, h), after) for h in range(2)] for p in self.planes]
        self.down = [[same(slot(p, ring, h), before) for h in range(2)] for p in self.planes]
        self.pass_up = [same(slot(p, (ring + 3) % 4, 0), after) for p in self.planes]
        self.pass_down = [same(slot(p, (ring + 1) % 4, 1), before) for p in self.planes]


IMAGE_CHUNK = 128
IMAGE_ROWS = 2048
WEIGHT_ROWS = 192


def gather_kernel(
    image, text, own_weights, cotangent, text_cotangent,
    tokens_out, weights_out, triple_out, upstream_out,
    tokens, weights, triple, upstream, send, recv, local_sems,
):
    xl, y, xh, z, core = where()
    own = (xh * 4 + z) * 2 + core
    half = IMAGE_CHUNK // 2

    def rows(p, r, c, h):
        return pl.ds(pl.multiple_of(((p * 4 + r) * 2 + c) * IMAGE_CHUNK + h * half, half), half)

    def token_slot(p, r, h):
        return tokens.at[rows(p, r, core, h), :]

    whalf = WEIGHT_ROWS // 2

    def weight_slot(p, r, h):
        return weights.at[
            pl.ds(pl.multiple_of((p * 4 + r) * WEIGHT_ROWS + h * whalf, whalf), whalf), :
        ]

    barrier = pltpu.get_barrier_semaphore()
    greeted = [seq_id(seq_peer(o)) for o in SEQ_OFFSETS] + [
        fsdp_id(fsdp_peer(o)) for o in ((1, 0), (0, 1), (0, 3))
    ]
    for peer in greeted:
        pl.semaphore_signal(barrier, inc=1, device_id=peer, device_id_type=MESH)

    def columns(s):
        return pl.ds(pl.multiple_of(s * HEAD, HEAD), HEAD)

    def chunk(s):
        return pl.ds(pl.multiple_of(s * IMAGE_CHUNK, IMAGE_CHUNK), IMAGE_CHUNK)

    text_rows = pl.ds(IMAGE_ROWS, text.shape[0])
    fills = [
        pltpu.make_async_copy(image, tokens.at[chunk(own), :], local_sems.at[0]),
        pltpu.make_async_copy(
            own_weights,
            weights.at[pl.ds(pl.multiple_of((xl * 4 + y) * WEIGHT_ROWS, WEIGHT_ROWS), WEIGHT_ROWS), :],
            local_sems.at[1],
        ),
        pltpu.make_async_copy(text, tokens.at[text_rows, :], local_sems.at[2]),
        pltpu.make_async_copy(
            cotangent.at[:, columns(own)], upstream.at[chunk(own), :], local_sems.at[3]
        ),
        pltpu.make_async_copy(
            text_cotangent.at[:, columns(own)], upstream.at[text_rows, :], local_sems.at[4]
        ),
    ]
    for fill in fills:
        fill.start()

    copies = Copies(send, recv)
    token_ring = Ring(copies, token_slot, "seq_0", xh, "seq_1", z)
    weight_ring = Ring(copies, weight_slot, "fsdp_0", xl, "fsdp_1", y)
    shared = {}
    for plane in range(2):
        for d in range(4):
            for h in range(2):
                piece = token_slot(token_ring.planes[plane], (z + d) % 4, h)
                shared[plane, d, h] = copies.make(piece, piece, {"seq_2": 1 - core})
    exchanged = []
    for offset in SEQ_OFFSETS:
        peer = seq_peer(offset)
        s = (peer[0] * 4 + peer[1]) * 2 + peer[2]
        exchanged.append(
            copies.make(cotangent.at[:, columns(s)], upstream.at[chunk(own), :], seq_id(peer))
        )

    fills[0].wait()
    fills[1].wait()
    pl.semaphore_wait(barrier, len(greeted))

    t, w = token_ring, weight_ring
    for h in range(2):
        t.cross[h].start()
        t.up[0][h].start()
        t.down[0][1 - h].start()
    for h in range(2):
        w.cross[h].start()
        w.up[0][h].start()
        w.down[0][1 - h].start()
    for h in range(2):
        shared[0, 0, h].start()

    def pass_on(ring, plane, then):
        ring.up[plane][0].wait_recv()
        ring.pass_up[plane].start()
        then(3, 0)
        ring.down[plane][1].wait_recv()
        ring.pass_down[plane].start()
        then(1, 1)

    def nothing(d, h):
        pass

    def share(plane):
        def then(d, h):
            shared[plane, d, h].start()

        return then

    pass_on(t, 0, share(0))
    pass_on(w, 0, nothing)
    for h in range(2):
        w.cross[h].wait_recv()
        w.up[1][h].start()
        w.down[1][h].start()
    for h in range(2):
        t.cross[h].wait_recv()
        t.up[1][h].start()
        t.down[1][h].start()
        shared[1, 0, h].start()
    t.up[0][1].wait_recv()
    shared[0, 3, 1].start()
    t.down[0][0].wait_recv()
    shared[0, 1, 0].start()
    for copy in exchanged:
        copy.start()
    pass_on(w, 1, nothing)
    t.pass_up[0].wait_recv()
    shared[0, 2, 0].start()
    t.pass_down[0].wait_recv()
    shared[0, 2, 1].start()
    for plane in range(2):
        w.up[plane][1].wait_recv()
        w.down[plane][0].wait_recv()
        w.pass_up[plane].wait_recv()
        w.pass_down[plane].wait_recv()
    weights_copy = pltpu.make_async_copy(weights, weights_out, local_sems.at[1])
    weights_copy.start()
    fills[2].wait()

    def project(start, count):
        at = pl.ds(start, count)
        triple[at, :] = dot_nn(tokens[at, :], weights[...]).astype(BF16)

    def project_pair(plane, d):
        for h in range(2):
            shared[plane, d, h].wait_recv()
        p = token_ring.planes[plane]
        project(pl.multiple_of((p * 4 + (z + d) % 4) * 2 * IMAGE_CHUNK, 2 * IMAGE_CHUNK), 2 * IMAGE_CHUNK)

    project(IMAGE_ROWS, text.shape[0])
    pass_on(t, 1, share(1))
    for d in range(4):
        project_pair(0, d)
    t.up[1][1].wait_recv()
    shared[1, 3, 1].start()
    t.down[1][0].wait_recv()
    shared[1, 1, 0].start()
    project_pair(1, 0)
    t.pass_up[1].wait_recv()
    shared[1, 2, 0].start()
    t.pass_down[1].wait_recv()
    shared[1, 2, 1].start()
    project_pair(1, 1)
    project_pair(1, 3)
    project_pair(1, 2)
    tokens_copy = pltpu.make_async_copy(tokens, tokens_out, local_sems.at[0])
    tokens_copy.start()
    triple_copy = pltpu.make_async_copy(triple, triple_out, local_sems.at[2])
    triple_copy.start()
    for copy in exchanged:
        copy.wait_recv()
    fills[3].wait()
    fills[4].wait()
    upstream_copy = pltpu.make_async_copy(upstream, upstream_out, local_sems.at[3])
    upstream_copy.start()
    for copy in copies.made:
        copy.wait_send()
    for copy in (tokens_copy, weights_copy, triple_copy, upstream_copy):
        copy.wait()


def gather(image, text, own_weights, cotangent, text_cotangent):
    features = image.shape[1]
    total = IMAGE_ROWS + text.shape[0]
    depth = 8 * WEIGHT_ROWS
    anywhere = pl.BlockSpec(memory_space=pl.ANY)
    n_copies = 2 * 14 + 16 + len(SEQ_OFFSETS)
    return pl.pallas_call(
        gather_kernel,
        out_shape=(
            jax.ShapeDtypeStruct((total, features), BF16),
            jax.ShapeDtypeStruct((depth, 3 * HEAD), BF16),
            jax.ShapeDtypeStruct((total, 3 * HEAD), BF16),
            jax.ShapeDtypeStruct((total, HEAD), BF16),
        ),
        in_specs=[anywhere] * 5,
        out_specs=(anywhere,) * 4,
        scratch_shapes=[
            pltpu.VMEM((total, features), BF16),
            pltpu.VMEM((depth, 3 * HEAD), BF16),
            pltpu.VMEM((total, 3 * HEAD), BF16),
            pltpu.VMEM((total, HEAD), BF16),
            pltpu.SemaphoreType.DMA((n_copies,)),
            pltpu.SemaphoreType.DMA((n_copies,)),
            pltpu.SemaphoreType.DMA((5,)),
        ],
        compiler_params=pltpu.CompilerParams(
            collective_id=0, has_side_effects=True, vmem_limit_bytes=48 * 1024 * 1024
        ),
        cost_estimate=pl.CostEstimate(
            flops=2 * total * features * 3 * HEAD, bytes_accessed=16 * 2**20, transcendentals=0
        ),
        name="gather",
    )(image, text, own_weights, cotangent, text_cotangent)


def local(image_input, text_input, w_qkv, query_gain, key_gain, image_cotangent, text_cotangent):
    own_index = lax.axis_index(SEQ)
    offset = own_index * HEAD
    features = image_input.shape[2]
    image_rows_dev = image_input.shape[1]
    text_rows = text_input.shape[1]
    own = lax.dynamic_slice_in_dim(w_qkv, offset, HEAD, 2).reshape(w_qkv.shape[0], 3 * HEAD)
    image_rows = IMAGE_ROWS
    tokens, weights, triple, upstream = gather(
        image_input[0], text_input[0], own, image_cotangent[0], text_cotangent[0]
    )
    grads, gain_part = attention(triple, upstream, query_gain, key_gain)
    gain_total = lax.psum(gain_part, FSDP_SEQ)
    head_total = lax.dot_general(tokens, grads, (((0,), (0,)), ((), ())), preferred_element_type=F32)
    grad_weights = lax.psum_scatter(
        head_total.astype(BF16), FSDP, scatter_dimension=0, tiled=True
    ).astype(F32)
    partial = lax.dot_general(grads, weights, (((1,), (1,)), ((), ())), preferred_element_type=F32)
    partial = partial.astype(BF16)
    image_out = lax.psum_scatter(partial[:image_rows], SEQ, scatter_dimension=0, tiled=True)
    text_out = lax.psum(partial[image_rows:], SEQ)
    return (
        image_out.reshape(1, image_rows_dev, features),
        text_out.reshape(1, text_rows, features),
        grad_weights.reshape(-1, 3, HEAD),
        gain_total,
    )


def solution(mesh):
    finer = Mesh(
        mesh.devices.reshape(2, 4, 2, 4, 2), ("fsdp_0", "fsdp_1", "seq_0", "seq_1", "seq_2")
    )
    return jax.shard_map(
        local,
        mesh=finer,
        in_specs=(
            P(FSDP, SEQ, None),
            P(FSDP, None, None),
            P(FSDP, None, None),
            P(),
            P(),
            P(FSDP, SEQ, None),
            P(FSDP, None, None),
        ),
        out_specs=(P(FSDP, SEQ, None), P(FSDP, None, None), P(FSDP, None, SEQ), P()),
        check_vma=False,
    )
```

```python
import math

import jax
import jax.numpy as jnp
from jax import lax
from jax.experimental import pallas as pl
from jax.experimental.pallas import tpu as pltpu
from jax.sharding import Mesh
from jax.sharding import PartitionSpec as P

HEADS = 16
HEAD = 128
SEQ = ("seq_0", "seq_1", "seq_2")
FSDP = ("fsdp_0", "fsdp_1")
FSDP_SEQ = ("fsdp_0", "fsdp_1", "seq_0", "seq_1", "seq_2")
EPS = 1e-06
F32 = jnp.float32
BF16 = jnp.bfloat16

Q_ROWS = 256
KEY_ROWS = 136


def dot_nt(a, b):
    return lax.dot_general(a, b, (((1,), (1,)), ((), ())), preferred_element_type=F32)


def dot_nn(a, b):
    return lax.dot_general(a, b, (((1,), (0,)), ((), ())), preferred_element_type=F32)


def folded(values):
    rows, width = values.shape
    return jnp.sum(values.reshape(rows // 8, 8, width), axis=0)


def attention_kernel(
    triple, upstream, qgain, kgain, grads, gains, qn, kn, kn_t, expd, dpd, dsd, dk, dv, gsum
):
    rows = triple.shape[0]
    factor = 1.0 / math.sqrt(HEAD)
    scale = factor * math.log2(math.e)

    def normed(values, gain):
        floated = values.astype(F32)
        inverse = lax.rsqrt(jnp.mean(floated * floated, axis=-1, keepdims=True) + EPS)
        return floated, inverse, (floated * inverse * gain).astype(BF16)

    qn[...] = normed(triple[:, 0:HEAD], qgain[...])[2]
    keys = normed(triple[:, HEAD : 2 * HEAD], kgain[...])[2]
    kn[...] = keys
    kn_t[...] = keys.T
    dk[...] = jnp.zeros_like(dk)
    dv[...] = jnp.zeros_like(dv)
    gsum[...] = jnp.zeros_like(gsum)

    def back(values, gain, incoming):
        floated = values.astype(F32)
        inverse = lax.rsqrt(jnp.mean(floated * floated, axis=-1, keepdims=True) + EPS)
        weighted = incoming * gain
        inner = jnp.mean(weighted * floated, axis=-1, keepdims=True)
        grad = inverse * weighted - floated * (inverse * inverse * inverse * inner)
        return grad, folded(incoming * floated * inverse)

    def block(start, count):
        qb = qn[pl.ds(start, count), :]
        ub = upstream[pl.ds(start, count), :]
        total = jnp.zeros((8, count), F32)
        inner = jnp.zeros((8, count), F32)
        for c in range(0, rows, KEY_ROWS):
            part = pl.ds(c, KEY_ROWS)
            e = jnp.exp2(dot_nt(kn[part, :], qb) * scale)
            d = dot_nt(triple[part, 2 * HEAD : 3 * HEAD], ub)
            expd[part, :count] = e
            dpd[part, :count] = d
            total = total + folded(e)
            inner = inner + folded(e * d)
        recip = 1.0 / jnp.sum(total, axis=0, keepdims=True)
        delta = jnp.sum(inner, axis=0, keepdims=True) * recip
        for c in range(0, rows, KEY_ROWS):
            part = pl.ds(c, KEY_ROWS)
            p = expd[part, :count] * recip
            ds = (p * (dpd[part, :count] - delta)).astype(BF16)
            dsd[part, :count] = ds
            dv[part, :] += dot_nn(p.astype(BF16), ub)
            dk[part, :] += dot_nn(ds, qb)
        dq_t = dot_nn(kn_t[...], dsd[:, :count])
        dq = dq_t.T * factor
        grad, gain_part = back(triple[pl.ds(start, count), 0:HEAD], qgain[...], dq)
        grads[pl.ds(start, count), 0:HEAD] = grad.astype(BF16)
        gsum[0:8, :] += gain_part

    image_rows = rows // Q_ROWS * Q_ROWS

    def step(i, carry):
        block(pl.multiple_of(i * Q_ROWS, Q_ROWS), Q_ROWS)
        return carry

    lax.fori_loop(0, image_rows // Q_ROWS, step, 0)
    if rows > image_rows:
        block(image_rows, rows - image_rows)
    grad, gain_part = back(triple[:, HEAD : 2 * HEAD], kgain[...], dk[...] * factor)
    grads[:, HEAD : 2 * HEAD] = grad.astype(BF16)
    grads[:, 2 * HEAD : 3 * HEAD] = dv[...].astype(BF16)
    gsum[8:16, :] = gain_part
    gains[0:1, :] = jnp.sum(gsum[0:8, :], axis=0, keepdims=True)
    gains[1:2, :] = jnp.sum(gsum[8:16, :], axis=0, keepdims=True)


def attention(triple, upstream, query_gain, key_gain):
    rows = triple.shape[0]
    vmem = pl.BlockSpec(memory_space=pltpu.VMEM)
    return pl.pallas_call(
        attention_kernel,
        out_shape=(
            jax.ShapeDtypeStruct((rows, 3 * HEAD), BF16),
            jax.ShapeDtypeStruct((2, HEAD), F32),
        ),
        in_specs=[vmem] * 4,
        out_specs=(vmem, vmem),
        scratch_shapes=[
            pltpu.VMEM((rows, HEAD), BF16),
            pltpu.VMEM((rows, HEAD), BF16),
            pltpu.VMEM((HEAD, rows), BF16),
            pltpu.VMEM((rows, Q_ROWS), F32),
            pltpu.VMEM((rows, Q_ROWS), F32),
            pltpu.VMEM((rows, Q_ROWS), BF16),
            pltpu.VMEM((rows, HEAD), F32),
            pltpu.VMEM((rows, HEAD), F32),
            pltpu.VMEM((16, HEAD), F32),
        ],
        compiler_params=pltpu.CompilerParams(vmem_limit_bytes=48 * 1024 * 1024),
        cost_estimate=pl.CostEstimate(
            flops=10 * rows * rows * HEAD, bytes_accessed=8 * rows * HEAD, transcendentals=rows * rows
        ),
        name="attention",
    )(triple, upstream, query_gain.reshape(1, HEAD), key_gain.reshape(1, HEAD))


MESH = pl.DeviceIdType.MESH


class Copies:
    def __init__(self, send, recv):
        self.send, self.recv, self.made = send, recv, []

    def make(self, src, dst, to):
        i = len(self.made)
        copy = pltpu.make_async_remote_copy(
            src_ref=src,
            dst_ref=dst,
            send_sem=self.send.at[i],
            recv_sem=self.recv.at[i],
            device_id=to,
            device_id_type=MESH,
        )
        self.made.append(copy)
        return copy


def where():
    return (
        lax.axis_index("fsdp_0"),
        lax.axis_index("fsdp_1"),
        lax.axis_index("seq_0"),
        lax.axis_index("seq_1"),
        lax.axis_index("seq_2"),
    )


SEQ_OFFSETS = [(a, b, c) for a in range(2) for b in range(4) for c in range(2) if a + b + c > 0]
FSDP_OFFSETS = [(a, b) for a in range(2) for b in range(4) if a + b > 0]


def seq_peer(offset):
    _, _, xh, z, core = where()
    return (xh + offset[0]) % 2, (z + offset[1]) % 4, (core + offset[2]) % 2


def fsdp_peer(offset):
    xl, y, _, _, _ = where()
    return (xl + offset[0]) % 2, (y + offset[1]) % 4


def seq_id(peer):
    return {"seq_0": peer[0], "seq_1": peer[1], "seq_2": peer[2]}


def fsdp_id(peer):
    return {"fsdp_0": peer[0], "fsdp_1": peer[1]}


class Ring:
    def __init__(self, copies, slot, pair_axis, pair, ring_axis, ring):
        self.planes = (pair, 1 - pair)
        self.ring = ring
        after, before = {ring_axis: (ring + 1) % 4}, {ring_axis: (ring + 3) % 4}
        other = {pair_axis: 1 - pair}

        def same(piece, to):
            return copies.make(piece, piece, to)

        self.cross = [same(slot(pair, ring, h), other) for h in range(2)]
        self.up = [[same(slot(p, ring, h), after) for h in range(2)] for p in self.planes]
        self.down = [[same(slot(p, ring, h), before) for h in range(2)] for p in self.planes]
        self.pass_up = [same(slot(p, (ring + 3) % 4, 0), after) for p in self.planes]
        self.pass_down = [same(slot(p, (ring + 1) % 4, 1), before) for p in self.planes]


IMAGE_CHUNK = 128
IMAGE_ROWS = 2048
WEIGHT_ROWS = 192


def gather_kernel(
    image, text, own_weights, cotangent, text_cotangent,
    tokens_out, weights_out, triple_out, upstream_out,
    tokens, weights, triple, upstream, send, recv, local_sems,
):
    xl, y, xh, z, core = where()
    own = (xh * 4 + z) * 2 + core
    half = IMAGE_CHUNK // 2

    def rows(p, r, c, h):
        return pl.ds(pl.multiple_of(((p * 4 + r) * 2 + c) * IMAGE_CHUNK + h * half, half), half)

    def token_slot(p, r, h):
        return tokens.at[rows(p, r, core, h), :]

    whalf = WEIGHT_ROWS // 2

    def weight_slot(p, r, h):
        return weights.at[
            pl.ds(pl.multiple_of((p * 4 + r) * WEIGHT_ROWS + h * whalf, whalf), whalf), :
        ]

    barrier = pltpu.get_barrier_semaphore()
    greeted = [seq_id(seq_peer(o)) for o in SEQ_OFFSETS] + [
        fsdp_id(fsdp_peer(o)) for o in ((1, 0), (0, 1), (0, 3))
    ]
    for peer in greeted:
        pl.semaphore_signal(barrier, inc=1, device_id=peer, device_id_type=MESH)

    def columns(s):
        return pl.ds(pl.multiple_of(s * HEAD, HEAD), HEAD)

    def chunk(s):
        return pl.ds(pl.multiple_of(s * IMAGE_CHUNK, IMAGE_CHUNK), IMAGE_CHUNK)

    text_rows = pl.ds(IMAGE_ROWS, text.shape[0])
    fills = [
        pltpu.make_async_copy(image, tokens.at[chunk(own), :], local_sems.at[0]),
        pltpu.make_async_copy(
            own_weights,
            weights.at[pl.ds(pl.multiple_of((xl * 4 + y) * WEIGHT_ROWS, WEIGHT_ROWS), WEIGHT_ROWS), :],
            local_sems.at[1],
        ),
        pltpu.make_async_copy(text, tokens.at[text_rows, :], local_sems.at[2]),
        pltpu.make_async_copy(
            cotangent.at[:, columns(own)], upstream.at[chunk(own), :], local_sems.at[3]
        ),
        pltpu.make_async_copy(
            text_cotangent.at[:, columns(own)], upstream.at[text_rows, :], local_sems.at[4]
        ),
    ]
    for fill in fills:
        fill.start()

    copies = Copies(send, recv)
    token_ring = Ring(copies, token_slot, "seq_0", xh, "seq_1", z)
    weight_ring = Ring(copies, weight_slot, "fsdp_0", xl, "fsdp_1", y)
    shared = {}
    for plane in range(2):
        for d in range(4):
            for h in range(2):
                piece = token_slot(token_ring.planes[plane], (z + d) % 4, h)
                shared[plane, d, h] = copies.make(piece, piece, {"seq_2": 1 - core})
    exchanged = []
    for offset in SEQ_OFFSETS:
        peer = seq_peer(offset)
        s = (peer[0] * 4 + peer[1]) * 2 + peer[2]
        exchanged.append(
            copies.make(cotangent.at[:, columns(s)], upstream.at[chunk(own), :], seq_id(peer))
        )

    fills[0].wait()
    fills[1].wait()
    pl.semaphore_wait(barrier, len(greeted))

    t, w = token_ring, weight_ring
    for h in range(2):
        t.cross[h].start()
        t.up[0][h].start()
        t.down[0][1 - h].start()
    for h in range(2):
        w.cross[h].start()
        w.up[0][h].start()
        w.down[0][1 - h].start()
    for h in range(2):
        shared[0, 0, h].start()

    def pass_on(ring, plane, then):
        ring.up[plane][0].wait_recv()
        ring.pass_up[plane].start()
        then(3, 0)
        ring.down[plane][1].wait_recv()
        ring.pass_down[plane].start()
        then(1, 1)

    def nothing(d, h):
        pass

    def share(plane):
        def then(d, h):
            shared[plane, d, h].start()

        return then

    pass_on(t, 0, share(0))
    pass_on(w, 0, nothing)
    for h in range(2):
        w.cross[h].wait_recv()
        w.up[1][h].start()
        w.down[1][h].start()
    for h in range(2):
        t.cross[h].wait_recv()
        t.up[1][h].start()
        t.down[1][h].start()
        shared[1, 0, h].start()
    t.up[0][1].wait_recv()
    shared[0, 3, 1].start()
    t.down[0][0].wait_recv()
    shared[0, 1, 0].start()
    for copy in exchanged:
        copy.start()
    pass_on(w, 1, nothing)
    t.pass_up[0].wait_recv()
    shared[0, 2, 0].start()
    t.pass_down[0].wait_recv()
    shared[0, 2, 1].start()
    for plane in range(2):
        w.up[plane][1].wait_recv()
        w.down[plane][0].wait_recv()
        w.pass_up[plane].wait_recv()
        w.pass_down[plane].wait_recv()
    weights_copy = pltpu.make_async_copy(weights, weights_out, local_sems.at[1])
    weights_copy.start()
    fills[2].wait()

    def project(start, count):
        at = pl.ds(start, count)
        triple[at, :] = dot_nn(tokens[at, :], weights[...]).astype(BF16)

    def project_pair(plane, d):
        for h in range(2):
            shared[plane, d, h].wait_recv()
        p = token_ring.planes[plane]
        project(pl.multiple_of((p * 4 + (z + d) % 4) * 2 * IMAGE_CHUNK, 2 * IMAGE_CHUNK), 2 * IMAGE_CHUNK)

    project(IMAGE_ROWS, text.shape[0])
    pass_on(t, 1, share(1))
    for d in range(4):
        project_pair(0, d)
    t.up[1][1].wait_recv()
    shared[1, 3, 1].start()
    t.down[1][0].wait_recv()
    shared[1, 1, 0].start()
    project_pair(1, 0)
    t.pass_up[1].wait_recv()
    shared[1, 2, 0].start()
    t.pass_down[1].wait_recv()
    shared[1, 2, 1].start()
    project_pair(1, 1)
    project_pair(1, 3)
    project_pair(1, 2)
    tokens_copy = pltpu.make_async_copy(tokens, tokens_out, local_sems.at[0])
    tokens_copy.start()
    triple_copy = pltpu.make_async_copy(triple, triple_out, local_sems.at[2])
    triple_copy.start()
    for copy in exchanged:
        copy.wait_recv()
    fills[3].wait()
    fills[4].wait()
    upstream_copy = pltpu.make_async_copy(upstream, upstream_out, local_sems.at[3])
    upstream_copy.start()
    for copy in copies.made:
        copy.wait_send()
    for copy in (tokens_copy, weights_copy, triple_copy, upstream_copy):
        copy.wait()


def gather(image, text, own_weights, cotangent, text_cotangent):
    features = image.shape[1]
    total = IMAGE_ROWS + text.shape[0]
    depth = 8 * WEIGHT_ROWS
    anywhere = pl.BlockSpec(memory_space=pl.ANY)
    n_copies = 2 * 14 + 16 + len(SEQ_OFFSETS)
    return pl.pallas_call(
        gather_kernel,
        out_shape=(
            jax.ShapeDtypeStruct((total, features), BF16),
            jax.ShapeDtypeStruct((depth, 3 * HEAD), BF16),
            jax.ShapeDtypeStruct((total, 3 * HEAD), BF16),
            jax.ShapeDtypeStruct((total, HEAD), BF16),
        ),
        in_specs=[anywhere] * 5,
        out_specs=(anywhere,) * 4,
        scratch_shapes=[
            pltpu.VMEM((total, features), BF16),
            pltpu.VMEM((depth, 3 * HEAD), BF16),
            pltpu.VMEM((total, 3 * HEAD), BF16),
            pltpu.VMEM((total, HEAD), BF16),
            pltpu.SemaphoreType.DMA((n_copies,)),
            pltpu.SemaphoreType.DMA((n_copies,)),
            pltpu.SemaphoreType.DMA((5,)),
        ],
        compiler_params=pltpu.CompilerParams(
            collective_id=0, has_side_effects=True, vmem_limit_bytes=48 * 1024 * 1024
        ),
        cost_estimate=pl.CostEstimate(
            flops=2 * total * features * 3 * HEAD, bytes_accessed=16 * 2**20, transcendentals=0
        ),
        name="gather",
    )(image, text, own_weights, cotangent, text_cotangent)


def dot_tn(a, b):
    return lax.dot_general(a, b, (((0,), (0,)), ((), ())), preferred_element_type=F32)


PAIR_OFFSETS = [(a, b) for a in range(2) for b in range(4) if a + b > 0]


def reduce_kernel(
    tokens_in, weights_in, grads_in, gains_in,
    image_out, text_out, weight_out, gain_out,
    tokens, weights, grads, grads_other, sums, piece_out, piece_in, cross_out, cross_in,
    dw_out, dw_in, text_part, text_in, text_all, gain_seq, gain_fsdp, send, recv, local_sems,
):
    xl, y, xh, z, core = where()
    own = (xh * 4 + z) * 2 + core
    group = xl * 4 + y
    half = IMAGE_CHUNK // 2
    planes = (xh, 1 - xh)
    other_core = {"seq_2": 1 - core}

    barrier = pltpu.get_barrier_semaphore()
    greeted = [seq_id(seq_peer(o)) for o in SEQ_OFFSETS] + [
        fsdp_id(fsdp_peer(o)) for o in FSDP_OFFSETS
    ]
    for peer in greeted:
        pl.semaphore_signal(barrier, inc=1, device_id=peer, device_id_type=MESH)
    fills = [
        pltpu.make_async_copy(grads_in, grads, local_sems.at[0]),
        pltpu.make_async_copy(weights_in, weights.at[0], local_sems.at[1]),
        pltpu.make_async_copy(tokens_in, tokens, local_sems.at[2]),
    ]
    for fill in fills:
        fill.start()

    copies = Copies(send, recv)
    to_other = [copies.make(weights.at[0], weights.at[1], other_core)]
    for plane in (1, 0):
        for d in (2, 1, 3, 0):
            at = planes[plane] * 4 + (z + d) % 4
            to_other.append(
                copies.make(
                    grads.at[pl.ds(pl.multiple_of((at * 2 + 1 - core) * IMAGE_CHUNK, IMAGE_CHUNK), IMAGE_CHUNK), :],
                    grads_other.at[pl.ds(pl.multiple_of(at * IMAGE_CHUNK, IMAGE_CHUNK), IMAGE_CHUNK), :],
                    other_core,
                )
            )
    text_half = text_out.shape[0] // 2
    text_mine = pl.ds(pl.multiple_of(IMAGE_ROWS + core * text_half, text_half), text_half)
    text_theirs = pl.ds(pl.multiple_of(IMAGE_ROWS + (1 - core) * text_half, text_half), text_half)
    text_got = pl.ds(IMAGE_ROWS // 2, text_half)
    to_other.append(copies.make(grads.at[text_theirs, :], grads_other.at[text_got, :], other_core))

    gain_first = [
        copies.make(gain_seq.at[own], gain_seq.at[own], seq_id(seq_peer(o))) for o in SEQ_OFFSETS
    ]
    gain_second = [
        copies.make(gain_fsdp.at[group], gain_fsdp.at[group], fsdp_id(fsdp_peer(o)))
        for o in FSDP_OFFSETS
    ]
    dw_sends = []
    for o in FSDP_OFFSETS:
        peer = fsdp_peer(o)
        dw_sends.append(copies.make(dw_out.at[peer[0] * 4 + peer[1]], dw_in.at[group], fsdp_id(peer)))
    text_first, text_second = [], []
    for o in PAIR_OFFSETS:
        peer = seq_peer((o[0], o[1], 0))
        to = {"seq_0": peer[0], "seq_1": peer[1]}
        text_first.append(copies.make(text_part.at[peer[0], peer[1]], text_in.at[xh, z], to))
        text_second.append(copies.make(text_all.at[core, xh, z], text_all.at[core, xh, z], to))
    text_third = copies.make(text_all.at[core], text_all.at[core], other_core)
    up, down = {"seq_1": (z + 1) % 4}, {"seq_1": (z + 3) % 4}
    pieces = {}
    for plane in range(2):
        for i in range(6):
            pieces[plane, i] = copies.make(
                piece_out.at[plane, i], piece_in.at[plane, i], up if i < 3 else down
            )
    cross = [copies.make(cross_out.at[h], cross_in.at[h], {"seq_0": 1 - xh}) for h in range(2)]

    gain_seq[own] = jnp.zeros(gain_seq.shape[1:], F32)
    gain_seq[own, 0:2, :] = gains_in[...]
    fills[0].wait()
    fills[1].wait()
    pl.semaphore_wait(barrier, len(greeted))
    for copy in to_other + gain_first:
        copy.start()
    fills[2].wait()

    def weight_part(j):
        block = 2 * WEIGHT_ROWS
        part = dot_tn(tokens[:, j * block : (j + 1) * block], grads[...]).astype(BF16)
        dw_out[2 * j] = part[:WEIGHT_ROWS]
        dw_out[2 * j + 1] = part[WEIGHT_ROWS:]

    def input_part(mine, theirs):
        return dot_nt(grads[mine, :], weights[0]) + dot_nt(grads_other[theirs, :], weights[1])

    def add_up(plane, d):
        at = planes[plane] * 4 + (z + d) % 4
        mine = pl.ds(pl.multiple_of((at * 2 + core) * IMAGE_CHUNK, IMAGE_CHUNK), IMAGE_CHUNK)
        theirs = pl.ds(pl.multiple_of(at * IMAGE_CHUNK, IMAGE_CHUNK), IMAGE_CHUNK)
        sums[plane, d] = input_part(mine, theirs)

    halves = (pl.ds(0, half), pl.ds(half, half))

    def put(plane, i, value):
        piece_out[plane, i] = value.astype(BF16)
        pieces[plane, i].start()

    def arrived(plane, i):
        return piece_in[plane, i].astype(F32)

    weight_part(0)
    weight_part(1)
    for copy in to_other:
        copy.wait_recv()

    def first_sends(plane):
        add_up(plane, 2)
        put(plane, 0, sums[plane, 2, halves[0], :])
        put(plane, 3, sums[plane, 2, halves[1], :])
        add_up(plane, 1)
        put(plane, 1, sums[plane, 1, halves[1], :])
        add_up(plane, 3)
        put(plane, 4, sums[plane, 3, halves[0], :])

    def pass_on(plane):
        pieces[plane, 0].wait_recv()
        put(plane, 2, sums[plane, 1, halves[0], :] + arrived(plane, 0))
        pieces[plane, 3].wait_recv()
        put(plane, 5, sums[plane, 3, halves[1], :] + arrived(plane, 3))

    def finish(plane, h):
        first, second = (2, 4) if h == 0 else (1, 5)
        pieces[plane, first].wait_recv()
        pieces[plane, second].wait_recv()
        return sums[plane, 0, halves[h], :] + arrived(plane, first) + arrived(plane, second)

    first_sends(1)
    text_sum = input_part(text_mine, text_got).astype(BF16)
    rows, columns = text_part.shape[2:]
    for a in range(2):
        for b in range(4):
            text_part[a, b] = text_sum[b * rows : (b + 1) * rows, a * columns : (a + 1) * columns]
    for copy in text_first:
        copy.start()
    text_in[xh, z] = text_part[xh, z]
    weight_part(2)
    pass_on(1)
    weight_part(3)
    for copy in dw_sends:
        copy.start()
    dw_in[group] = dw_out[group]
    first_sends(0)
    add_up(1, 0)
    for copy in gain_first:
        copy.wait_recv()
    gain_fsdp[group] = jnp.sum(gain_seq[...], axis=0)
    for copy in gain_second:
        copy.start()
    for copy in text_first:
        copy.wait_recv()
    text_all[core, xh, z] = jnp.sum(text_in[...].astype(F32), axis=(0, 1)).astype(BF16)
    for copy in text_second:
        copy.start()
    for h in (1, 0):
        cross_out[h] = finish(1, h).astype(BF16)
        cross[h].start()
    pass_on(0)
    add_up(0, 0)
    for copy in text_second:
        copy.wait_recv()
    text_third.start()
    for copy in gain_second:
        copy.wait_recv()
    gain_out[...] = jnp.sum(gain_fsdp[...], axis=0)[0:2]
    for copy in dw_sends:
        copy.wait_recv()
    weight_out[...] = jnp.sum(dw_in[...].astype(F32), axis=0)
    text_third.wait_recv()
    for c in range(2):
        for a in range(2):
            for b in range(4):
                text_out[
                    c * text_half + b * rows : c * text_half + (b + 1) * rows,
                    a * columns : (a + 1) * columns,
                ] = text_all[c, a, b]
    for h in (1, 0):
        total = finish(0, h)
        cross[h].wait_recv()
        image_out[halves[h], :] = (total + cross_in[h].astype(F32)).astype(BF16)
    for copy in copies.made:
        copy.wait_send()


def reduce(tokens, weights, grads, gains):
    total, features = tokens.shape
    text_rows = total - IMAGE_ROWS
    anywhere = pl.BlockSpec(memory_space=pl.ANY)
    vmem = pl.BlockSpec(memory_space=pltpu.VMEM)
    half = IMAGE_CHUNK // 2
    n_copies = 10 + len(SEQ_OFFSETS) + 2 * len(FSDP_OFFSETS) + 2 * len(PAIR_OFFSETS) + 1 + 12 + 2
    text_piece = (2, 4, text_rows // 8, features // 2)
    return pl.pallas_call(
        reduce_kernel,
        out_shape=(
            jax.ShapeDtypeStruct((IMAGE_CHUNK, features), BF16),
            jax.ShapeDtypeStruct((text_rows, features), BF16),
            jax.ShapeDtypeStruct((WEIGHT_ROWS, 3 * HEAD), F32),
            jax.ShapeDtypeStruct((2, HEAD), F32),
        ),
        in_specs=[anywhere, anywhere, anywhere, vmem],
        out_specs=(vmem,) * 4,
        scratch_shapes=[
            pltpu.VMEM((total, features), BF16),
            pltpu.VMEM((2, features, 3 * HEAD), BF16),
            pltpu.VMEM((total, 3 * HEAD), BF16),
            pltpu.VMEM((total // 2, 3 * HEAD), BF16),
            pltpu.VMEM((2, 4, IMAGE_CHUNK, features), F32),
            pltpu.VMEM((2, 6, half, features), BF16),
            pltpu.VMEM((2, 6, half, features), BF16),
            pltpu.VMEM((2, half, features), BF16),
            pltpu.VMEM((2, half, features), BF16),
            pltpu.VMEM((8, WEIGHT_ROWS, 3 * HEAD), BF16),
            pltpu.VMEM((8, WEIGHT_ROWS, 3 * HEAD), BF16),
            pltpu.VMEM(text_piece, BF16),
            pltpu.VMEM(text_piece, BF16),
            pltpu.VMEM((2, *text_piece), BF16),
            pltpu.VMEM((16, 8, HEAD), F32),
            pltpu.VMEM((8, 8, HEAD), F32),
            pltpu.SemaphoreType.DMA((n_copies,)),
            pltpu.SemaphoreType.DMA((n_copies,)),
            pltpu.SemaphoreType.DMA((3,)),
        ],
        compiler_params=pltpu.CompilerParams(
            collective_id=1, has_side_effects=True, vmem_limit_bytes=56 * 1024 * 1024
        ),
        cost_estimate=pl.CostEstimate(
            flops=4 * total * features * 3 * HEAD, bytes_accessed=16 * 2**20, transcendentals=0
        ),
        name="reduce",
    )(tokens, weights, grads, gains)


def local(image_input, text_input, w_qkv, query_gain, key_gain, image_cotangent, text_cotangent):
    own_index = lax.axis_index(SEQ)
    offset = own_index * HEAD
    features = image_input.shape[2]
    image_rows_dev = image_input.shape[1]
    text_rows = text_input.shape[1]
    own = lax.dynamic_slice_in_dim(w_qkv, offset, HEAD, 2).reshape(w_qkv.shape[0], 3 * HEAD)
    tokens, weights, triple, upstream = gather(
        image_input[0], text_input[0], own, image_cotangent[0], text_cotangent[0]
    )
    grads, gain_part = attention(triple, upstream, query_gain, key_gain)
    image_out, text_out, grad_weights, gain_total = reduce(tokens, weights, grads, gain_part)
    return (
        image_out.reshape(1, image_rows_dev, features),
        text_out.reshape(1, text_rows, features),
        grad_weights.reshape(-1, 3, HEAD),
        gain_total,
    )


def solution(mesh):
    finer = Mesh(
        mesh.devices.reshape(2, 4, 2, 4, 2), ("fsdp_0", "fsdp_1", "seq_0", "seq_1", "seq_2")
    )
    return jax.shard_map(
        local,
        mesh=finer,
        in_specs=(
            P(FSDP, SEQ, None),
            P(FSDP, None, None),
            P(FSDP, None, None),
            P(),
            P(),
            P(FSDP, SEQ, None),
            P(FSDP, None, None),
        ),
        out_specs=(P(FSDP, SEQ, None), P(FSDP, None, None), P(FSDP, None, SEQ), P()),
        check_vma=False,
    )
```

```python
import math

import jax
import jax.numpy as jnp
from jax import lax
from jax.experimental import pallas as pl
from jax.experimental.pallas import tpu as pltpu
from jax.sharding import Mesh
from jax.sharding import PartitionSpec as P

HEAD = 128
SEQ = ("seq_0", "seq_1", "seq_2")
FSDP = ("fsdp_0", "fsdp_1")
EPS = 1e-06
F32 = jnp.float32
BF16 = jnp.bfloat16
MESH = pl.DeviceIdType.MESH

Q_ROWS = 256
KEY_ROWS = 136
IMAGE_CHUNK = 128
IMAGE_ROWS = 2048
WEIGHT_ROWS = 192
WIDTH = 3 * HEAD


def dot_nt(a, b):
    return lax.dot_general(a, b, (((1,), (1,)), ((), ())), preferred_element_type=F32)


def dot_nn(a, b):
    return lax.dot_general(a, b, (((1,), (0,)), ((), ())), preferred_element_type=F32)


def dot_tn(a, b):
    return lax.dot_general(a, b, (((0,), (0,)), ((), ())), preferred_element_type=F32)


def folded(values):
    rows, width = values.shape
    return jnp.sum(values.reshape(rows // 8, 8, width), axis=0)


class Copies:
    def __init__(self, send, recv):
        self.send, self.recv, self.made = send, recv, []

    def make(self, src, dst, to):
        i = len(self.made)
        copy = pltpu.make_async_remote_copy(
            src_ref=src,
            dst_ref=dst,
            send_sem=self.send.at[i],
            recv_sem=self.recv.at[i],
            device_id=to,
            device_id_type=MESH,
        )
        self.made.append(copy)
        return copy


def where():
    return (
        lax.axis_index("fsdp_0"),
        lax.axis_index("fsdp_1"),
        lax.axis_index("seq_0"),
        lax.axis_index("seq_1"),
        lax.axis_index("seq_2"),
    )


SEQ_OFFSETS = [(a, b, c) for a in range(2) for b in range(4) for c in range(2) if a + b + c > 0]
FSDP_OFFSETS = [(a, b) for a in range(2) for b in range(4) if a + b > 0]
UNITS = [(a, b) for a in range(2) for b in range(4)]


def seq_peer(offset):
    _, _, xh, z, core = where()
    return (xh + offset[0]) % 2, (z + offset[1]) % 4, (core + offset[2]) % 2


def fsdp_peer(offset):
    xl, y, _, _, _ = where()
    return (xl + offset[0]) % 2, (y + offset[1]) % 4


def seq_id(peer):
    return {"seq_0": peer[0], "seq_1": peer[1], "seq_2": peer[2]}


def fsdp_id(peer):
    return {"fsdp_0": peer[0], "fsdp_1": peer[1]}


class GatherRing:
    def __init__(self, copies, slot, pair_axis, pair, ring_axis, ring):
        self.planes = (pair, 1 - pair)
        after, before = {ring_axis: (ring + 1) % 4}, {ring_axis: (ring + 3) % 4}
        other = {pair_axis: 1 - pair}

        def same(piece, to):
            return copies.make(piece, piece, to)

        self.cross = [same(slot(pair, ring, h), other) for h in range(2)]
        self.up = [[same(slot(p, ring, h), after) for h in range(2)] for p in self.planes]
        self.down = [[same(slot(p, ring, h), before) for h in range(2)] for p in self.planes]
        self.pass_up = same(slot(pair, (ring + 3) % 4, 0), after)
        self.pass_down = same(slot(pair, (ring + 1) % 4, 1), before)
        self.far = [same(slot(pair, (ring + 2) % 4, h), other) for h in range(2)]


GATHER_COPIES = 14


class ReduceRing:
    def __init__(self, copies, out, arrived, value, pair_axis, pair, ring_axis, ring):
        up, down = {ring_axis: (ring + 1) % 4}, {ring_axis: (ring + 3) % 4}
        other = {pair_axis: 1 - pair}
        to = [other] * 2 + [up] * 2 + [down] * 2 + [up] * 3 + [down] * 3 + [other] * 2
        self.out, self.arrived, self.value = out, arrived, value
        self.pieces = [copies.make(out.at[i], arrived.at[i], t) for i, t in enumerate(to)]

    def put(self, i, value):
        self.out[i] = value.astype(BF16)
        self.pieces[i].start()

    def got(self, i):
        self.pieces[i].wait_recv()
        return self.arrived[i].astype(F32)

    def send_far(self):
        self.put(0, self.value(1, 2, 0))
        self.put(1, self.value(1, 2, 1))

    def send_up(self):
        self.put(2, self.value(1, 1, 0))
        self.put(3, self.value(1, 1, 1))

    def send_down(self):
        self.put(4, self.value(1, 3, 0))
        self.put(5, self.value(1, 3, 1))

    def own_up(self):
        self.put(7, self.value(0, 1, 1))

    def own_down(self):
        self.put(10, self.value(0, 3, 0))

    def own_far(self):
        self.put(6, self.value(0, 2, 0) + self.got(0))
        self.put(9, self.value(0, 2, 1) + self.got(1))

    def pass_on(self):
        self.put(8, self.value(0, 1, 0) + self.got(6))
        self.put(11, self.value(0, 3, 1) + self.got(9))

    def cross(self):
        self.put(12, self.value(1, 0, 0) + self.got(2) + self.got(4))
        self.put(13, self.value(1, 0, 1) + self.got(3) + self.got(5))

    def total(self, h):
        parts = ((8, 10, 12), (7, 11, 13))[h]
        result = self.value(0, 0, h)
        for i in parts:
            result = result + self.got(i)
        return result


REDUCE_COPIES = 14


def step_kernel(
    image, text, w_qkv, qgain, kgain, cotangent, text_cotangent,
    image_out, text_out, weight_out, gain_out,
    tokens, weights, triple, upstream, qn, kn, kn_t, expd, esum, dsd, dpd, dv, gsum,
    grads, grads_other, dw, dx_out, dx_in, dw_out, dw_in,
    text_part, text_in, text_all, gain_seq, gain_fsdp, send, recv, local_sems,
):
    xl, y, xh, z, core = where()
    own = (xh * 4 + z) * 2 + core
    group = xl * 4 + y
    half = IMAGE_CHUNK // 2
    whalf = WEIGHT_ROWS // 2
    total_rows = tokens.shape[0]
    text_count = text.shape[0]
    text_rows = pl.ds(IMAGE_ROWS, text_count)
    factor = 1.0 / math.sqrt(HEAD)
    scale = factor * math.log2(math.e)
    planes = (xh, 1 - xh)
    other_core = {"seq_2": 1 - core}

    barrier = pltpu.get_barrier_semaphore()
    greeted = [seq_id(seq_peer(o)) for o in SEQ_OFFSETS] + [
        fsdp_id(fsdp_peer(o)) for o in FSDP_OFFSETS
    ]
    for peer in greeted:
        pl.semaphore_signal(barrier, inc=1, device_id=peer, device_id_type=MESH)

    def columns(s):
        return pl.ds(pl.multiple_of(s * HEAD, HEAD), HEAD)

    def chunk(s):
        return pl.ds(pl.multiple_of(s * IMAGE_CHUNK, IMAGE_CHUNK), IMAGE_CHUNK)

    def token_slot(p, r, h):
        start = ((p * 4 + r) * 2 + core) * IMAGE_CHUNK + h * half
        return tokens.at[pl.ds(pl.multiple_of(start, half), half), :]

    def weight_slot(p, r, h):
        start = (p * 4 + r) * WEIGHT_ROWS + h * whalf
        return weights.at[0, pl.ds(pl.multiple_of(start, whalf), whalf), :]

    group_rows = pl.ds(pl.multiple_of(group * WEIGHT_ROWS, WEIGHT_ROWS), WEIGHT_ROWS)
    fill_image = pltpu.make_async_copy(image, tokens.at[chunk(own), :], local_sems.at[0])
    fill_weights = [
        pltpu.make_async_copy(
            w_qkv.at[j, :, columns(own)],
            weights.at[0, group_rows, j * HEAD : (j + 1) * HEAD],
            local_sems.at[1 + j],
        )
        for j in range(3)
    ]
    fill_text = pltpu.make_async_copy(text, tokens.at[text_rows, :], local_sems.at[4])
    fill_upstream = [
        pltpu.make_async_copy(
            cotangent.at[:, columns(own)], upstream.at[chunk(own), :], local_sems.at[5]
        ),
        pltpu.make_async_copy(
            text_cotangent.at[:, columns(own)], upstream.at[text_rows, :], local_sems.at[6]
        ),
    ]
    for fill in (fill_image, *fill_weights, fill_text, *fill_upstream):
        fill.start()

    copies = Copies(send, recv)
    t = GatherRing(copies, token_slot, "seq_0", xh, "seq_1", z)
    w = GatherRing(copies, weight_slot, "fsdp_0", xl, "fsdp_1", y)
    shared = {}
    for plane, d in UNITS:
        for h in range(2):
            piece = token_slot(planes[plane], (z + d) % 4, h)
            shared[plane, d, h] = copies.make(piece, piece, other_core)
    exchanged = []
    for offset in SEQ_OFFSETS:
        peer = seq_peer(offset)
        s = (peer[0] * 4 + peer[1]) * 2 + peer[2]
        exchanged.append(
            copies.make(cotangent.at[:, columns(s)], upstream.at[chunk(own), :], seq_id(peer))
        )
    weights_shared = copies.make(weights.at[0], weights.at[1], other_core)

    def unit_at(plane, d):
        return planes[plane] * 4 + (z + d) % 4

    grads_shared = {}
    for plane, d in UNITS:
        at = unit_at(plane, d)
        grads_shared[plane, d] = copies.make(
            grads.at[chunk(at * 2 + 1 - core), :], grads_other.at[chunk(at), :], other_core
        )
    text_half = text_count // 2

    def text_share(c):
        return pl.ds(pl.multiple_of(IMAGE_ROWS + c * text_half, text_half), text_half)

    text_got = pl.ds(IMAGE_ROWS // 2, text_half)
    text_shared = copies.make(grads.at[text_share(1 - core), :], grads_other.at[text_got, :], other_core)
    gain_first = [
        copies.make(gain_seq.at[own], gain_seq.at[own], seq_id(seq_peer(o))) for o in SEQ_OFFSETS
    ]
    gain_second = [
        copies.make(gain_fsdp.at[group], gain_fsdp.at[group], fsdp_id(fsdp_peer(o)))
        for o in FSDP_OFFSETS
    ]
    text_first, text_second = [], []
    for o in FSDP_OFFSETS:
        peer = seq_peer((o[0], o[1], 0))
        to = {"seq_0": peer[0], "seq_1": peer[1]}
        text_first.append(copies.make(text_part.at[peer[0], peer[1]], text_in.at[xh, z], to))
        text_second.append(copies.make(text_all.at[core, xh, z], text_all.at[core, xh, z], to))
    text_third = copies.make(text_all.at[core], text_all.at[core], other_core)

    def dx_value(plane, d, h):
        start = (plane * 4 + d) * IMAGE_CHUNK + h * half
        return expd[start : start + half, : tokens.shape[1]]

    def dw_value(plane, d, h):
        f = (xl if plane == 0 else 1 - xl) * 4 + (y + d) % 4
        return dw[pl.ds(pl.multiple_of(f * WEIGHT_ROWS + h * whalf, whalf), whalf), :]

    dx_ring = ReduceRing(copies, dx_out, dx_in, dx_value, "seq_0", xh, "seq_1", z)
    dw_ring = ReduceRing(copies, dw_out, dw_in, dw_value, "fsdp_0", xl, "fsdp_1", y)

    fill_image.wait()
    pl.semaphore_wait(barrier, len(greeted))
    for h in range(2):
        t.cross[h].start()
        t.up[0][h].start()
        t.down[0][1 - h].start()
    for fill in fill_weights:
        fill.wait()
    for h in range(2):
        w.cross[h].start()
        w.up[0][h].start()
        w.down[0][1 - h].start()
    for h in range(2):
        shared[0, 0, h].start()

    t.up[0][0].wait_recv()
    t.pass_up.start()
    shared[0, 3, 0].start()
    t.down[0][1].wait_recv()
    t.pass_down.start()
    shared[0, 1, 1].start()
    w.up[0][0].wait_recv()
    w.pass_up.start()
    w.down[0][1].wait_recv()
    w.pass_down.start()
    for h in range(2):
        w.cross[h].wait_recv()
        w.up[1][h].start()
        w.down[1][h].start()
    for h in range(2):
        t.cross[h].wait_recv()
        t.up[1][h].start()
        t.down[1][h].start()
        shared[1, 0, h].start()
    t.up[0][1].wait_recv()
    shared[0, 3, 1].start()
    t.down[0][0].wait_recv()
    shared[0, 1, 0].start()
    w.pass_up.wait_recv()
    w.far[0].start()
    w.pass_down.wait_recv()
    w.far[1].start()
    t.pass_up.wait_recv()
    t.far[0].start()
    shared[0, 2, 0].start()
    t.pass_down.wait_recv()
    t.far[1].start()
    shared[0, 2, 1].start()
    for copy in exchanged:
        copy.start()
    w.up[0][1].wait_recv()
    w.down[0][0].wait_recv()
    for h in range(2):
        w.up[1][h].wait_recv()
        w.down[1][h].wait_recv()
        w.far[h].wait_recv()
    weights_shared.start()

    def normed(values, gain):
        inverse = lax.rsqrt(jnp.mean(values * values, axis=-1, keepdims=True) + EPS)
        return (values * inverse * gain).astype(BF16)

    def project(start, count):
        at = pl.ds(start, count)
        result = dot_nn(tokens[at, :], weights[0]).astype(BF16)
        triple[at, :] = result
        qn[at, :] = normed(result[:, :HEAD].astype(F32), qgain[...])
        keys = normed(result[:, HEAD : 2 * HEAD].astype(F32), kgain[...])
        kn[at, :] = keys
        kn_t[:, at] = keys.T

    def unit_start(plane, d):
        return pl.multiple_of(unit_at(plane, d) * Q_ROWS, Q_ROWS)

    def project_unit(plane, d):
        for h in range(2):
            shared[plane, d, h].wait_recv()
        project(unit_start(plane, d), Q_ROWS)

    fill_text.wait()
    project(IMAGE_ROWS, text_count)
    for d in range(4):
        project_unit(0, d)
    for h in range(2):
        t.up[1][h].wait_recv()
        shared[1, 3, h].start()
        t.down[1][h].wait_recv()
        shared[1, 1, h].start()
    project_unit(1, 0)
    for h in range(2):
        t.far[h].wait_recv()
        shared[1, 2, h].start()
    project_unit(1, 1)
    project_unit(1, 3)
    project_unit(1, 2)

    dv[...] = jnp.zeros_like(dv)
    gsum[...] = jnp.zeros_like(gsum)
    key_parts = [pl.ds(c, KEY_ROWS) for c in range(0, total_rows, KEY_ROWS)]

    def exponentials(start, count):
        at = pl.ds(start, count)
        qb = qn[at, :]
        total = jnp.zeros((8, count), F32)
        for part in key_parts:
            e = jnp.exp2(dot_nt(kn[part, :], qb) * scale)
            expd[part, at] = e
            total = total + folded(e)
        esum[:, at] = total

    def score_grads(start, count):
        at = pl.ds(start, count)
        ub = upstream[at, :]
        inner = jnp.zeros((8, count), F32)
        for part in key_parts:
            d = dot_nt(triple[part, 2 * HEAD :], ub)
            dpd[part, :count] = d
            inner = inner + folded(expd[part, at] * d)
        recip = 1.0 / jnp.sum(esum[:, at], axis=0, keepdims=True)
        delta = jnp.sum(inner, axis=0, keepdims=True) * recip
        for part in key_parts:
            p = expd[part, at] * recip
            dsd[part, at] = (p * (dpd[part, :count] - delta)).astype(BF16)
            dv[part, :] += dot_nn(p.astype(BF16), ub)

    def over_blocks(block):
        def step(i, carry):
            block(pl.multiple_of(i * Q_ROWS, Q_ROWS), Q_ROWS)
            return carry

        lax.fori_loop(0, IMAGE_ROWS // Q_ROWS, step, 0)
        block(IMAGE_ROWS, text_count)

    over_blocks(exponentials)
    for copy in exchanged:
        copy.wait_recv()
    for fill in fill_upstream:
        fill.wait()
    over_blocks(score_grads)

    def back(values, gain, incoming):
        floated = values.astype(F32)
        inverse = lax.rsqrt(jnp.mean(floated * floated, axis=-1, keepdims=True) + EPS)
        weighted = incoming * gain
        inner = jnp.mean(weighted * floated, axis=-1, keepdims=True)
        grad = inverse * weighted - floated * (inverse * inverse * inverse * inner)
        return grad.astype(BF16), folded(incoming * floated * inverse)

    def token_grads(start, count):
        at = pl.ds(start, count)
        dq = dot_nn(kn_t[...], dsd[:, at]).T * factor
        dk = dot_nn(dsd[at, :], qn[...]) * factor
        dq, q_part = back(triple[at, :HEAD], qgain[...], dq)
        dk, k_part = back(triple[at, HEAD : 2 * HEAD], kgain[...], dk)
        grads[at, :HEAD] = dq
        grads[at, HEAD : 2 * HEAD] = dk
        grads[at, 2 * HEAD :] = dv[at, :].astype(BF16)
        gsum[0:8, :] += q_part
        gsum[8:16, :] += k_part

    def unit_grads(plane, d):
        token_grads(unit_start(plane, d), Q_ROWS)
        grads_shared[plane, d].start()

    def input_part(mine, theirs):
        return dot_nt(grads[mine, :], weights[0]) + dot_nt(grads_other[theirs, :], weights[1])

    def input_sum(plane, d):
        at = unit_at(plane, d)
        grads_shared[plane, d].wait_recv()
        start = (plane * 4 + d) * IMAGE_CHUNK
        expd[start : start + IMAGE_CHUNK, : tokens.shape[1]] = input_part(
            chunk(at * 2 + core), chunk(at)
        )

    def weight_part(j):
        block = 2 * WEIGHT_ROWS
        dw[j * block : (j + 1) * block, :] = dot_tn(
            tokens[:, j * block : (j + 1) * block], grads[...]
        )

    unit_grads(1, 2)
    unit_grads(1, 1)
    weights_shared.wait_recv()
    input_sum(1, 2)
    dx_ring.send_far()
    unit_grads(1, 3)
    input_sum(1, 1)
    dx_ring.send_up()
    unit_grads(0, 2)
    input_sum(1, 3)
    dx_ring.send_down()
    unit_grads(0, 1)
    unit_grads(0, 3)
    input_sum(0, 1)
    dx_ring.own_up()
    input_sum(0, 3)
    dx_ring.own_down()
    input_sum(0, 2)
    dx_ring.own_far()
    token_grads(IMAGE_ROWS, text_count)
    text_shared.start()
    unit_grads(1, 0)
    unit_grads(0, 0)
    gain_seq[own] = jnp.zeros(gain_seq.shape[1:], F32)
    gain_seq[own, 0:1, :] = jnp.sum(gsum[0:8, :], axis=0, keepdims=True)
    gain_seq[own, 1:2, :] = jnp.sum(gsum[8:16, :], axis=0, keepdims=True)
    for copy in gain_first:
        copy.start()
    weight_part(0)
    weight_part(1)
    input_sum(1, 0)
    dx_ring.cross()
    dx_ring.pass_on()
    weight_part(2)
    weight_part(3)
    dw_ring.send_far()
    dw_ring.send_up()
    dw_ring.send_down()
    dw_ring.own_up()
    dw_ring.own_down()
    text_shared.wait_recv()
    text_sum = input_part(text_share(core), text_got).astype(BF16)
    rows, width = text_part.shape[2:]
    for a, b in UNITS:
        text_part[a, b] = text_sum[b * rows : (b + 1) * rows, a * width : (a + 1) * width]
    for copy in text_first:
        copy.start()
    text_in[xh, z] = text_part[xh, z]
    dw_ring.own_far()
    input_sum(0, 0)
    for copy in gain_first:
        copy.wait_recv()
    gain_fsdp[group] = jnp.sum(gain_seq[...], axis=0)
    for copy in gain_second:
        copy.start()
    dw_ring.cross()
    dw_ring.pass_on()
    for copy in text_first:
        copy.wait_recv()
    text_all[core, xh, z] = jnp.sum(text_in[...].astype(F32), axis=(0, 1)).astype(BF16)
    for copy in text_second:
        copy.start()
    for copy in gain_second:
        copy.wait_recv()
    gain_out[...] = jnp.sum(gain_fsdp[...], axis=0)[0:2]
    for copy in text_second:
        copy.wait_recv()
    text_third.start()
    for h in range(2):
        image_out[h * half : (h + 1) * half, :] = dx_ring.total(h).astype(BF16)
    for h in range(2):
        total = dw_ring.total(h)
        for j in range(3):
            weight_out[j, h * whalf : (h + 1) * whalf, :] = total[:, j * HEAD : (j + 1) * HEAD]
    text_third.wait_recv()
    for c in range(2):
        for a, b in UNITS:
            text_out[
                c * text_half + b * rows : c * text_half + (b + 1) * rows,
                a * width : (a + 1) * width,
            ] = text_all[c, a, b]
    for copy in copies.made:
        copy.wait_send()


def step(image, text, w_qkv, query_gain, key_gain, cotangent, text_cotangent):
    features = image.shape[1]
    text_count = text.shape[0]
    total = IMAGE_ROWS + text_count
    depth = w_qkv.shape[1] * 8
    hbm = pl.BlockSpec(memory_space=pltpu.HBM)
    vmem = pl.BlockSpec(memory_space=pltpu.VMEM)
    half, whalf = IMAGE_CHUNK // 2, WEIGHT_ROWS // 2
    text_piece = (2, 4, text_count // 8, features // 2)
    n_copies = (
        2 * GATHER_COPIES + 16 + len(SEQ_OFFSETS) + 1 + 9
        + len(SEQ_OFFSETS) + len(FSDP_OFFSETS) + 2 * len(FSDP_OFFSETS) + 1 + 2 * REDUCE_COPIES
    )
    return pl.pallas_call(
        step_kernel,
        out_shape=(
            jax.ShapeDtypeStruct((IMAGE_CHUNK, features), BF16),
            jax.ShapeDtypeStruct((text_count, features), BF16),
            jax.ShapeDtypeStruct((3, WEIGHT_ROWS, HEAD), F32),
            jax.ShapeDtypeStruct((2, HEAD), F32),
        ),
        in_specs=[hbm, hbm, hbm, vmem, vmem, hbm, hbm],
        out_specs=(vmem,) * 4,
        scratch_shapes=[
            pltpu.VMEM((total, features), BF16),
            pltpu.VMEM((2, depth, WIDTH), BF16),
            pltpu.VMEM((total, WIDTH), BF16),
            pltpu.VMEM((total, HEAD), BF16),
            pltpu.VMEM((total, HEAD), BF16),
            pltpu.VMEM((total, HEAD), BF16),
            pltpu.VMEM((HEAD, total), BF16),
            pltpu.VMEM((total, total), F32),
            pltpu.VMEM((8, total), F32),
            pltpu.VMEM((total, total), BF16),
            pltpu.VMEM((total, Q_ROWS), F32),
            pltpu.VMEM((total, HEAD), F32),
            pltpu.VMEM((16, HEAD), F32),
            pltpu.VMEM((total, WIDTH), BF16),
            pltpu.VMEM((total // 2, WIDTH), BF16),
            pltpu.VMEM((depth, WIDTH), F32),
            pltpu.VMEM((REDUCE_COPIES, half, features), BF16),
            pltpu.VMEM((REDUCE_COPIES, half, features), BF16),
            pltpu.VMEM((REDUCE_COPIES, whalf, WIDTH), BF16),
            pltpu.VMEM((REDUCE_COPIES, whalf, WIDTH), BF16),
            pltpu.VMEM(text_piece, BF16),
            pltpu.VMEM(text_piece, BF16),
            pltpu.VMEM((2, *text_piece), BF16),
            pltpu.VMEM((16, 8, HEAD), F32),
            pltpu.VMEM((8, 8, HEAD), F32),
            pltpu.SemaphoreType.DMA((n_copies,)),
            pltpu.SemaphoreType.DMA((n_copies,)),
            pltpu.SemaphoreType.DMA((7,)),
        ],
        compiler_params=pltpu.CompilerParams(
            collective_id=0, has_side_effects=True, vmem_limit_bytes=62 * 1024 * 1024
        ),
        name="step",
    )(image, text, w_qkv, query_gain, key_gain, cotangent, text_cotangent)


def store_kernel(*refs):
    count = (len(refs) - 1) // 2
    sems = refs[-1]
    moves = [
        pltpu.make_async_copy(refs[i], refs[count + i], sems.at[i]) for i in range(count)
    ]
    for move in moves:
        move.start()
    for move in moves:
        move.wait()


def store(*arrays):
    hbm = pl.BlockSpec(memory_space=pltpu.HBM)
    vmem = pl.BlockSpec(memory_space=pltpu.VMEM)
    return pl.pallas_call(
        store_kernel,
        out_shape=tuple(jax.ShapeDtypeStruct(a.shape, a.dtype) for a in arrays),
        in_specs=[vmem] * len(arrays),
        out_specs=(hbm,) * len(arrays),
        scratch_shapes=[pltpu.SemaphoreType.DMA((len(arrays),))],
        compiler_params=pltpu.CompilerParams(vmem_limit_bytes=4 * 1024 * 1024),
        name="store",
    )(*arrays)


def local(image_input, text_input, w_qkv, query_gain, key_gain, image_cotangent, text_cotangent):
    image_out, text_out, grad_weights, gain_total = store(
        *step(
            image_input[0],
            text_input[0],
            w_qkv.transpose(1, 0, 2),
            query_gain.reshape(1, HEAD),
            key_gain.reshape(1, HEAD),
            image_cotangent[0],
            text_cotangent[0],
        )
    )
    return image_out[None], text_out[None], grad_weights.transpose(1, 0, 2), gain_total


def solution(mesh):
    finer = Mesh(
        mesh.devices.reshape(2, 4, 2, 4, 2), ("fsdp_0", "fsdp_1", "seq_0", "seq_1", "seq_2")
    )
    return jax.shard_map(
        local,
        mesh=finer,
        in_specs=(
            P(FSDP, SEQ, None),
            P(FSDP, None, None),
            P(FSDP, None, None),
            P(),
            P(),
            P(FSDP, SEQ, None),
            P(FSDP, None, None),
        ),
        out_specs=(P(FSDP, SEQ, None), P(FSDP, None, None), P(FSDP, None, SEQ), P()),
        check_vma=False,
    )
```

```python
import math

import jax
import jax.numpy as jnp
from jax import lax
from jax.experimental import pallas as pl
from jax.experimental.pallas import tpu as pltpu
from jax.sharding import Mesh
from jax.sharding import PartitionSpec as P

HEAD = 128
SEQ = ("seq_0", "seq_1", "seq_2")
FSDP = ("fsdp_0", "fsdp_1")
EPS = 1e-06
F32 = jnp.float32
BF16 = jnp.bfloat16
MESH = pl.DeviceIdType.MESH

Q_ROWS = 256
KEY_ROWS = 136
IMAGE_CHUNK = 128
IMAGE_ROWS = 2048
WEIGHT_ROWS = 192
WIDTH = 3 * HEAD


def dot_nt(a, b):
    return lax.dot_general(a, b, (((1,), (1,)), ((), ())), preferred_element_type=F32)


def dot_nn(a, b):
    return lax.dot_general(a, b, (((1,), (0,)), ((), ())), preferred_element_type=F32)


def dot_tn(a, b):
    return lax.dot_general(a, b, (((0,), (0,)), ((), ())), preferred_element_type=F32)


def folded(values):
    rows, width = values.shape
    return jnp.sum(values.reshape(rows // 8, 8, width), axis=0)


class Copies:
    def __init__(self, send, recv):
        self.send, self.recv, self.made = send, recv, []

    def make(self, src, dst, to):
        i = len(self.made)
        copy = pltpu.make_async_remote_copy(
            src_ref=src,
            dst_ref=dst,
            send_sem=self.send.at[i],
            recv_sem=self.recv.at[i],
            device_id=to,
            device_id_type=MESH,
        )
        self.made.append(copy)
        return copy


def where():
    return (
        lax.axis_index("fsdp_0"),
        lax.axis_index("fsdp_1"),
        lax.axis_index("seq_0"),
        lax.axis_index("seq_1"),
        lax.axis_index("seq_2"),
    )


SEQ_OFFSETS = [(a, b, c) for a in range(2) for b in range(4) for c in range(2) if a + b + c > 0]
FSDP_OFFSETS = [(a, b) for a in range(2) for b in range(4) if a + b > 0]
UNITS = [(a, b) for a in range(2) for b in range(4)]


def seq_peer(offset):
    _, _, xh, z, core = where()
    return (xh + offset[0]) % 2, (z + offset[1]) % 4, (core + offset[2]) % 2


def fsdp_peer(offset):
    xl, y, _, _, _ = where()
    return (xl + offset[0]) % 2, (y + offset[1]) % 4


def seq_id(peer):
    return {"seq_0": peer[0], "seq_1": peer[1], "seq_2": peer[2]}


def fsdp_id(peer):
    return {"fsdp_0": peer[0], "fsdp_1": peer[1]}


class GatherRing:
    def __init__(self, copies, slot, pair_axis, pair, ring_axis, ring):
        self.planes = (pair, 1 - pair)
        after, before = {ring_axis: (ring + 1) % 4}, {ring_axis: (ring + 3) % 4}
        other = {pair_axis: 1 - pair}

        def same(piece, to):
            return copies.make(piece, piece, to)

        self.cross = [same(slot(pair, ring, h), other) for h in range(2)]
        self.up = [[same(slot(p, ring, h), after) for h in range(2)] for p in self.planes]
        self.down = [[same(slot(p, ring, h), before) for h in range(2)] for p in self.planes]
        self.pass_up = same(slot(pair, (ring + 3) % 4, 0), after)
        self.pass_down = same(slot(pair, (ring + 1) % 4, 1), before)
        self.far = [same(slot(pair, (ring + 2) % 4, h), other) for h in range(2)]


GATHER_COPIES = 14


class ReduceRing:
    def __init__(self, copies, out, arrived, value, pair_axis, pair, ring_axis, ring):
        up, down = {ring_axis: (ring + 1) % 4}, {ring_axis: (ring + 3) % 4}
        other = {pair_axis: 1 - pair}
        to = [other] * 2 + [up] * 2 + [down] * 2 + [up] * 3 + [down] * 3 + [other] * 2
        self.out, self.arrived, self.value = out, arrived, value
        self.pieces = [copies.make(out.at[i], arrived.at[i], t) for i, t in enumerate(to)]

    def put(self, i, value):
        self.out[i] = value.astype(BF16)
        self.pieces[i].start()

    def got(self, i):
        self.pieces[i].wait_recv()
        return self.arrived[i].astype(F32)

    def send_far(self):
        self.put(0, self.value(1, 2, 0))
        self.put(1, self.value(1, 2, 1))

    def send_up(self):
        self.put(2, self.value(1, 1, 0))
        self.put(3, self.value(1, 1, 1))

    def send_down(self):
        self.put(4, self.value(1, 3, 0))
        self.put(5, self.value(1, 3, 1))

    def own_up(self):
        self.put(7, self.value(0, 1, 1))

    def own_down(self):
        self.put(10, self.value(0, 3, 0))

    def own_far(self, h):
        self.put((6, 9)[h], self.value(0, 2, h) + self.got(h))

    def pass_on(self, h):
        self.put((8, 11)[h], self.value(0, (1, 3)[h], h) + self.got((6, 9)[h]))

    def cross(self):
        self.put(12, self.value(1, 0, 0) + self.got(2) + self.got(4))
        self.put(13, self.value(1, 0, 1) + self.got(3) + self.got(5))

    def total(self, h):
        parts = ((8, 10, 12), (7, 11, 13))[h]
        result = self.value(0, 0, h)
        for i in parts:
            result = result + self.got(i)
        return result


REDUCE_COPIES = 14


def step_kernel(
    image, text, w_qkv, qgain, kgain, cotangent, text_cotangent,
    image_out, text_out, weight_out, gain_out,
    tokens, weights, triple, upstream, qn, kn, kn_t, expd, esum, dsd, dpd, dv, gsum,
    grads, grads_other, dw, dx_out, dx_in, dw_out, dw_in,
    text_part, text_in, text_all, gain_seq, gain_fsdp, send, recv, local_sems,
):
    xl, y, xh, z, core = where()
    own = (xh * 4 + z) * 2 + core
    group = xl * 4 + y
    half = IMAGE_CHUNK // 2
    whalf = WEIGHT_ROWS // 2
    total_rows = tokens.shape[0]
    text_count = text.shape[0]
    text_rows = pl.ds(IMAGE_ROWS, text_count)
    factor = 1.0 / math.sqrt(HEAD)
    scale = factor * math.log2(math.e)
    planes = (xh, 1 - xh)
    other_core = {"seq_2": 1 - core}

    barrier = pltpu.get_barrier_semaphore()
    greeted = [seq_id(seq_peer(o)) for o in SEQ_OFFSETS] + [
        fsdp_id(fsdp_peer(o)) for o in FSDP_OFFSETS
    ]
    for peer in greeted:
        pl.semaphore_signal(barrier, inc=1, device_id=peer, device_id_type=MESH)

    def columns(s):
        return pl.ds(pl.multiple_of(s * HEAD, HEAD), HEAD)

    def chunk(s):
        return pl.ds(pl.multiple_of(s * IMAGE_CHUNK, IMAGE_CHUNK), IMAGE_CHUNK)

    def token_slot(p, r, h):
        start = ((p * 4 + r) * 2 + core) * IMAGE_CHUNK + h * half
        return tokens.at[pl.ds(pl.multiple_of(start, half), half), :]

    def weight_slot(p, r, h):
        start = (p * 4 + r) * WEIGHT_ROWS + h * whalf
        return weights.at[0, pl.ds(pl.multiple_of(start, whalf), whalf), :]

    group_rows = pl.ds(pl.multiple_of(group * WEIGHT_ROWS, WEIGHT_ROWS), WEIGHT_ROWS)
    fill_image = pltpu.make_async_copy(image, tokens.at[chunk(own), :], local_sems.at[0])
    fill_weights = [
        pltpu.make_async_copy(
            w_qkv.at[j, :, columns(own)],
            weights.at[0, group_rows, j * HEAD : (j + 1) * HEAD],
            local_sems.at[1 + j],
        )
        for j in range(3)
    ]
    fill_text = pltpu.make_async_copy(text, tokens.at[text_rows, :], local_sems.at[4])
    fill_upstream = [
        pltpu.make_async_copy(
            cotangent.at[:, columns(own)], upstream.at[chunk(own), :], local_sems.at[5]
        ),
        pltpu.make_async_copy(
            text_cotangent.at[:, columns(own)], upstream.at[text_rows, :], local_sems.at[6]
        ),
    ]
    for fill in (fill_image, *fill_weights, fill_text, *fill_upstream):
        fill.start()

    copies = Copies(send, recv)
    t = GatherRing(copies, token_slot, "seq_0", xh, "seq_1", z)
    w = GatherRing(copies, weight_slot, "fsdp_0", xl, "fsdp_1", y)
    shared = {}
    for plane, d in UNITS:
        for h in range(2):
            piece = token_slot(planes[plane], (z + d) % 4, h)
            shared[plane, d, h] = copies.make(piece, piece, other_core)
    exchanged = []
    for offset in SEQ_OFFSETS:
        peer = seq_peer(offset)
        s = (peer[0] * 4 + peer[1]) * 2 + peer[2]
        exchanged.append(
            copies.make(cotangent.at[:, columns(s)], upstream.at[chunk(own), :], seq_id(peer))
        )
    weights_shared = copies.make(weights.at[0], weights.at[1], other_core)

    def unit_at(plane, d):
        return planes[plane] * 4 + (z + d) % 4

    grads_shared = {}
    for plane, d in UNITS:
        at = unit_at(plane, d)
        grads_shared[plane, d] = copies.make(
            grads.at[chunk(at * 2 + 1 - core), :], grads_other.at[chunk(at), :], other_core
        )
    text_half = text_count // 2

    def text_share(c):
        return pl.ds(pl.multiple_of(IMAGE_ROWS + c * text_half, text_half), text_half)

    text_got = pl.ds(IMAGE_ROWS // 2, text_half)
    text_shared = copies.make(grads.at[text_share(1 - core), :], grads_other.at[text_got, :], other_core)
    gain_first = [
        copies.make(gain_seq.at[own], gain_seq.at[own], seq_id(seq_peer(o))) for o in SEQ_OFFSETS
    ]
    gain_second = [
        copies.make(gain_fsdp.at[group], gain_fsdp.at[group], fsdp_id(fsdp_peer(o)))
        for o in FSDP_OFFSETS
    ]
    text_first, text_second = [], []
    for o in FSDP_OFFSETS:
        peer = seq_peer((o[0], o[1], 0))
        to = {"seq_0": peer[0], "seq_1": peer[1]}
        text_first.append(copies.make(text_part.at[peer[0], peer[1]], text_in.at[xh, z], to))
        text_second.append(copies.make(text_all.at[core, xh, z], text_all.at[core, xh, z], to))
    text_third = copies.make(text_all.at[core], text_all.at[core], other_core)

    def dx_value(plane, d, h):
        start = (plane * 4 + d) * IMAGE_CHUNK + h * half
        return expd[start : start + half, : tokens.shape[1]]

    def dw_value(plane, d, h):
        f = (xl if plane == 0 else 1 - xl) * 4 + (y + d) % 4
        return dw[pl.ds(pl.multiple_of(f * WEIGHT_ROWS + h * whalf, whalf), whalf), :]

    dx_ring = ReduceRing(copies, dx_out, dx_in, dx_value, "seq_0", xh, "seq_1", z)
    dw_ring = ReduceRing(copies, dw_out, dw_in, dw_value, "fsdp_0", xl, "fsdp_1", y)

    fill_image.wait()
    pl.semaphore_wait(barrier, len(greeted))
    for h in range(2):
        t.cross[h].start()
        t.up[0][h].start()
        t.down[0][1 - h].start()
    for fill in fill_weights:
        fill.wait()
    for h in range(2):
        w.cross[h].start()
        w.up[0][h].start()
        w.down[0][1 - h].start()
    for h in range(2):
        shared[0, 0, h].start()

    t.up[0][0].wait_recv()
    t.pass_up.start()
    shared[0, 3, 0].start()
    t.down[0][1].wait_recv()
    t.pass_down.start()
    shared[0, 1, 1].start()
    w.up[0][0].wait_recv()
    w.pass_up.start()
    w.down[0][1].wait_recv()
    w.pass_down.start()
    for h in range(2):
        w.cross[h].wait_recv()
        w.up[1][h].start()
        w.down[1][h].start()
    for h in range(2):
        t.cross[h].wait_recv()
        t.up[1][h].start()
        t.down[1][h].start()
        shared[1, 0, h].start()
    t.up[0][1].wait_recv()
    shared[0, 3, 1].start()
    t.down[0][0].wait_recv()
    shared[0, 1, 0].start()
    w.pass_up.wait_recv()
    w.far[0].start()
    w.pass_down.wait_recv()
    w.far[1].start()
    t.pass_up.wait_recv()
    t.far[0].start()
    shared[0, 2, 0].start()
    t.pass_down.wait_recv()
    t.far[1].start()
    shared[0, 2, 1].start()
    for copy in exchanged:
        copy.start()
    w.up[0][1].wait_recv()
    w.down[0][0].wait_recv()
    for h in range(2):
        w.up[1][h].wait_recv()
        w.down[1][h].wait_recv()
        w.far[h].wait_recv()
    weights_shared.start()

    def normed(values, gain):
        inverse = lax.rsqrt(jnp.mean(values * values, axis=-1, keepdims=True) + EPS)
        return (values * inverse * gain).astype(BF16)

    def project(start, count):
        at = pl.ds(start, count)
        result = dot_nn(tokens[at, :], weights[0]).astype(BF16)
        triple[at, :] = result
        qn[at, :] = normed(result[:, :HEAD].astype(F32), qgain[...])
        keys = normed(result[:, HEAD : 2 * HEAD].astype(F32), kgain[...])
        kn[at, :] = keys
        kn_t[:, at] = keys.T

    def unit_start(plane, d):
        return pl.multiple_of(unit_at(plane, d) * Q_ROWS, Q_ROWS)

    def project_unit(plane, d):
        for h in range(2):
            shared[plane, d, h].wait_recv()
        project(unit_start(plane, d), Q_ROWS)

    fill_text.wait()
    project(IMAGE_ROWS, text_count)
    for d in range(4):
        project_unit(0, d)
    for h in range(2):
        t.up[1][h].wait_recv()
        shared[1, 3, h].start()
        t.down[1][h].wait_recv()
        shared[1, 1, h].start()
    project_unit(1, 0)
    for h in range(2):
        t.far[h].wait_recv()
        shared[1, 2, h].start()
    project_unit(1, 1)
    project_unit(1, 3)
    project_unit(1, 2)

    dv[...] = jnp.zeros_like(dv)
    gsum[...] = jnp.zeros_like(gsum)
    key_parts = [pl.ds(c, KEY_ROWS) for c in range(0, total_rows, KEY_ROWS)]

    def exponentials(start, count):
        at = pl.ds(start, count)
        qb = qn[at, :]
        total = jnp.zeros((8, count), F32)
        for part in key_parts:
            e = jnp.exp2(dot_nt(kn[part, :], qb) * scale)
            expd[part, at] = e
            total = total + folded(e)
        esum[:, at] = total

    def score_grads(start, count):
        at = pl.ds(start, count)
        ub = upstream[at, :]
        inner = jnp.zeros((8, count), F32)
        for part in key_parts:
            d = dot_nt(triple[part, 2 * HEAD :], ub)
            dpd[part, :count] = d
            inner = inner + folded(expd[part, at] * d)
        recip = 1.0 / jnp.sum(esum[:, at], axis=0, keepdims=True)
        delta = jnp.sum(inner, axis=0, keepdims=True) * recip
        for part in key_parts:
            p = expd[part, at] * recip
            dsd[part, at] = (p * (dpd[part, :count] - delta)).astype(BF16)
            dv[part, :] += dot_nn(p.astype(BF16), ub)

    def exponential_block(i, carry):
        exponentials(pl.multiple_of(i * Q_ROWS, Q_ROWS), Q_ROWS)
        return carry

    blocks = IMAGE_ROWS // Q_ROWS
    lax.fori_loop(0, blocks, exponential_block, 0)
    exponentials(IMAGE_ROWS, text_count)
    for fill in fill_upstream:
        fill.wait()
    score_grads(IMAGE_ROWS, text_count)

    def score_block(i, carry):
        for plane in range(2):

            @pl.when(i == 4 * plane)
            def _():
                for offset, copy in zip(SEQ_OFFSETS, exchanged):
                    if offset[0] == plane:
                        copy.wait_recv()

        at = (xh + i // 4) % 2 * 4 + (z + i) % 4
        score_grads(pl.multiple_of(at * Q_ROWS, Q_ROWS), Q_ROWS)
        return carry

    lax.fori_loop(0, blocks, score_block, 0)

    def back(values, gain, incoming):
        floated = values.astype(F32)
        inverse = lax.rsqrt(jnp.mean(floated * floated, axis=-1, keepdims=True) + EPS)
        weighted = incoming * gain
        inner = jnp.mean(weighted * floated, axis=-1, keepdims=True)
        grad = inverse * weighted - floated * (inverse * inverse * inverse * inner)
        return grad.astype(BF16), folded(incoming * floated * inverse)

    def token_grads(start, count):
        at = pl.ds(start, count)
        dq = dot_nn(kn_t[...], dsd[:, at]).T * factor
        dk = dot_nn(dsd[at, :], qn[...]) * factor
        dq, q_part = back(triple[at, :HEAD], qgain[...], dq)
        dk, k_part = back(triple[at, HEAD : 2 * HEAD], kgain[...], dk)
        grads[at, :HEAD] = dq
        grads[at, HEAD : 2 * HEAD] = dk
        grads[at, 2 * HEAD :] = dv[at, :].astype(BF16)
        gsum[0:8, :] += q_part
        gsum[8:16, :] += k_part

    def unit_grads(plane, d):
        token_grads(unit_start(plane, d), Q_ROWS)
        grads_shared[plane, d].start()

    def input_part(mine, theirs):
        return dot_nt(grads[mine, :], weights[0]) + dot_nt(grads_other[theirs, :], weights[1])

    def input_sum(plane, d):
        at = unit_at(plane, d)
        grads_shared[plane, d].wait_recv()
        start = (plane * 4 + d) * IMAGE_CHUNK
        expd[start : start + IMAGE_CHUNK, : tokens.shape[1]] = input_part(
            chunk(at * 2 + core), chunk(at)
        )

    def weight_part(j):
        block = 2 * WEIGHT_ROWS
        dw[j * block : (j + 1) * block, :] = dot_tn(
            tokens[:, j * block : (j + 1) * block], grads[...]
        )

    unit_grads(1, 1)
    unit_grads(1, 2)
    unit_grads(1, 3)
    weights_shared.wait_recv()
    input_sum(1, 1)
    dx_ring.send_up()
    input_sum(1, 2)
    dx_ring.send_far()
    input_sum(1, 3)
    dx_ring.send_down()
    for unit in ((0, 2), (0, 1), (0, 3), (1, 0), (0, 0)):
        unit_grads(*unit)
    token_grads(IMAGE_ROWS, text_count)
    text_shared.start()
    gain_seq[own] = jnp.zeros(gain_seq.shape[1:], F32)
    gain_seq[own, 0:1, :] = jnp.sum(gsum[0:8, :], axis=0, keepdims=True)
    gain_seq[own, 1:2, :] = jnp.sum(gsum[8:16, :], axis=0, keepdims=True)
    for copy in gain_first:
        copy.start()
    input_sum(0, 2)
    dx_ring.own_far(0)
    weight_part(0)
    weight_part(1)
    input_sum(0, 1)
    dx_ring.own_up()
    dx_ring.own_far(1)
    input_sum(0, 3)
    dx_ring.own_down()
    weight_part(2)
    weight_part(3)
    dw_ring.send_far()
    dw_ring.send_up()
    dw_ring.send_down()
    dw_ring.own_up()
    dw_ring.own_down()
    input_sum(1, 0)
    dx_ring.cross()
    text_shared.wait_recv()
    text_sum = input_part(text_share(core), text_got).astype(BF16)
    rows, width = text_part.shape[2:]
    for a, b in UNITS:
        text_part[a, b] = text_sum[b * rows : (b + 1) * rows, a * width : (a + 1) * width]
    for copy in text_first:
        copy.start()
    text_in[xh, z] = text_part[xh, z]
    dx_ring.pass_on(0)
    input_sum(0, 0)
    for copy in gain_first:
        copy.wait_recv()
    gain_fsdp[group] = jnp.sum(gain_seq[...], axis=0)
    for copy in gain_second:
        copy.start()
    for h in range(2):
        dw_ring.own_far(h)
    dx_ring.pass_on(1)
    dw_ring.cross()
    for copy in text_first:
        copy.wait_recv()
    text_all[core, xh, z] = jnp.sum(text_in[...].astype(F32), axis=(0, 1)).astype(BF16)
    for copy in text_second:
        copy.start()
    for h in range(2):
        dw_ring.pass_on(h)
    for copy in gain_second:
        copy.wait_recv()
    gain_out[...] = jnp.sum(gain_fsdp[...], axis=0)[0:2]
    for copy in text_second:
        copy.wait_recv()
    text_third.start()
    for h in range(2):
        image_out[h * half : (h + 1) * half, :] = dx_ring.total(h).astype(BF16)
    for h in range(2):
        total = dw_ring.total(h)
        for j in range(3):
            weight_out[j, h * whalf : (h + 1) * whalf, :] = total[:, j * HEAD : (j + 1) * HEAD]
    text_third.wait_recv()
    for c in range(2):
        for a, b in UNITS:
            text_out[
                c * text_half + b * rows : c * text_half + (b + 1) * rows,
                a * width : (a + 1) * width,
            ] = text_all[c, a, b]
    for copy in copies.made:
        copy.wait_send()


def step(image, text, w_qkv, query_gain, key_gain, cotangent, text_cotangent):
    features = image.shape[1]
    text_count = text.shape[0]
    total = IMAGE_ROWS + text_count
    depth = w_qkv.shape[1] * 8
    hbm = pl.BlockSpec(memory_space=pltpu.HBM)
    vmem = pl.BlockSpec(memory_space=pltpu.VMEM)
    half, whalf = IMAGE_CHUNK // 2, WEIGHT_ROWS // 2
    text_piece = (2, 4, text_count // 8, features // 2)
    n_copies = (
        2 * GATHER_COPIES + 16 + len(SEQ_OFFSETS) + 1 + 9
        + len(SEQ_OFFSETS) + len(FSDP_OFFSETS) + 2 * len(FSDP_OFFSETS) + 1 + 2 * REDUCE_COPIES
    )
    return pl.pallas_call(
        step_kernel,
        out_shape=(
            jax.ShapeDtypeStruct((IMAGE_CHUNK, features), BF16),
            jax.ShapeDtypeStruct((text_count, features), BF16),
            jax.ShapeDtypeStruct((3, WEIGHT_ROWS, HEAD), F32),
            jax.ShapeDtypeStruct((2, HEAD), F32),
        ),
        in_specs=[hbm, hbm, hbm, vmem, vmem, hbm, hbm],
        out_specs=(vmem,) * 4,
        scratch_shapes=[
            pltpu.VMEM((total, features), BF16),
            pltpu.VMEM((2, depth, WIDTH), BF16),
            pltpu.VMEM((total, WIDTH), BF16),
            pltpu.VMEM((total, HEAD), BF16),
            pltpu.VMEM((total, HEAD), BF16),
            pltpu.VMEM((total, HEAD), BF16),
            pltpu.VMEM((HEAD, total), BF16),
            pltpu.VMEM((total, total), F32),
            pltpu.VMEM((8, total), F32),
            pltpu.VMEM((total, total), BF16),
            pltpu.VMEM((total, Q_ROWS), F32),
            pltpu.VMEM((total, HEAD), F32),
            pltpu.VMEM((16, HEAD), F32),
            pltpu.VMEM((total, WIDTH), BF16),
            pltpu.VMEM((total // 2, WIDTH), BF16),
            pltpu.VMEM((depth, WIDTH), F32),
            pltpu.VMEM((REDUCE_COPIES, half, features), BF16),
            pltpu.VMEM((REDUCE_COPIES, half, features), BF16),
            pltpu.VMEM((REDUCE_COPIES, whalf, WIDTH), BF16),
            pltpu.VMEM((REDUCE_COPIES, whalf, WIDTH), BF16),
            pltpu.VMEM(text_piece, BF16),
            pltpu.VMEM(text_piece, BF16),
            pltpu.VMEM((2, *text_piece), BF16),
            pltpu.VMEM((16, 8, HEAD), F32),
            pltpu.VMEM((8, 8, HEAD), F32),
            pltpu.SemaphoreType.DMA((n_copies,)),
            pltpu.SemaphoreType.DMA((n_copies,)),
            pltpu.SemaphoreType.DMA((7,)),
        ],
        compiler_params=pltpu.CompilerParams(
            collective_id=0, has_side_effects=True, vmem_limit_bytes=62 * 1024 * 1024
        ),
        name="step",
    )(image, text, w_qkv, query_gain, key_gain, cotangent, text_cotangent)


def store_kernel(*refs):
    count = (len(refs) - 2) // 3
    taken, kept, held = refs[:count], refs[count : 2 * count], refs[2 * count : 3 * count]
    loads, stores = refs[-2:]
    ins = [pltpu.make_async_copy(taken[i], held[i], loads.at[i]) for i in range(count)]
    outs = [pltpu.make_async_copy(held[i], kept[i], stores.at[i]) for i in range(count)]
    for copy in ins:
        copy.start()
    for i in range(count):
        ins[i].wait()
        outs[i].start()
    for copy in outs:
        copy.wait()


def store(*arrays):
    hbm = pl.BlockSpec(memory_space=pltpu.HBM)
    return pl.pallas_call(
        store_kernel,
        out_shape=tuple(jax.ShapeDtypeStruct(a.shape, a.dtype) for a in arrays),
        in_specs=[hbm] * len(arrays),
        out_specs=(hbm,) * len(arrays),
        scratch_shapes=[pltpu.VMEM(a.shape, a.dtype) for a in arrays]
        + [pltpu.SemaphoreType.DMA((len(arrays),))] * 2,
        compiler_params=pltpu.CompilerParams(vmem_limit_bytes=67043328),
        name="store",
    )(*arrays)


def local(image_input, text_input, w_qkv, query_gain, key_gain, image_cotangent, text_cotangent):
    image_out, text_out, grad_weights, gain_total = store(
        *step(
            image_input[0],
            text_input[0],
            w_qkv.transpose(1, 0, 2),
            query_gain.reshape(1, HEAD),
            key_gain.reshape(1, HEAD),
            image_cotangent[0],
            text_cotangent[0],
        )
    )
    return image_out[None], text_out[None], grad_weights.transpose(1, 0, 2), gain_total


def solution(mesh):
    finer = Mesh(
        mesh.devices.reshape(2, 4, 2, 4, 2), ("fsdp_0", "fsdp_1", "seq_0", "seq_1", "seq_2")
    )
    return jax.shard_map(
        local,
        mesh=finer,
        in_specs=(
            P(FSDP, SEQ, None),
            P(FSDP, None, None),
            P(FSDP, None, None),
            P(),
            P(),
            P(FSDP, SEQ, None),
            P(FSDP, None, None),
        ),
        out_specs=(P(FSDP, SEQ, None), P(FSDP, None, None), P(FSDP, None, SEQ), P()),
        check_vma=False,
    )
```

```python
import math

import jax
import jax.numpy as jnp
from jax import lax
from jax.experimental import pallas as pl
from jax.experimental.pallas import tpu as pltpu
from jax.sharding import Mesh
from jax.sharding import PartitionSpec as P

HEAD = 128
SEQ = ("seq_0", "seq_1", "seq_2")
FSDP = ("fsdp_0", "fsdp_1")
EPS = 1e-06
F32 = jnp.float32
BF16 = jnp.bfloat16
MESH = pl.DeviceIdType.MESH

Q_ROWS = 256
KEY_ROWS = 136
IMAGE_CHUNK = 128
IMAGE_ROWS = 2048
WEIGHT_ROWS = 192
WIDTH = 3 * HEAD


def dot_nt(a, b):
    return lax.dot_general(a, b, (((1,), (1,)), ((), ())), preferred_element_type=F32)


def dot_nn(a, b):
    return lax.dot_general(a, b, (((1,), (0,)), ((), ())), preferred_element_type=F32)


def dot_tn(a, b):
    return lax.dot_general(a, b, (((0,), (0,)), ((), ())), preferred_element_type=F32)


def folded(values):
    rows, width = values.shape
    return jnp.sum(values.reshape(rows // 8, 8, width), axis=0)


class Copies:
    def __init__(self, send, recv):
        self.send, self.recv, self.made = send, recv, []

    def make(self, src, dst, to):
        i = len(self.made)
        copy = pltpu.make_async_remote_copy(
            src_ref=src,
            dst_ref=dst,
            send_sem=self.send.at[i],
            recv_sem=self.recv.at[i],
            device_id=to,
            device_id_type=MESH,
        )
        self.made.append(copy)
        return copy


def where():
    return (
        lax.axis_index("fsdp_0"),
        lax.axis_index("fsdp_1"),
        lax.axis_index("seq_0"),
        lax.axis_index("seq_1"),
        lax.axis_index("seq_2"),
    )


SEQ_OFFSETS = [(a, b, c) for a in range(2) for b in range(4) for c in range(2) if a + b + c > 0]
FSDP_OFFSETS = [(a, b) for a in range(2) for b in range(4) if a + b > 0]
UNITS = [(a, b) for a in range(2) for b in range(4)]


def seq_peer(offset):
    _, _, xh, z, core = where()
    return (xh + offset[0]) % 2, (z + offset[1]) % 4, (core + offset[2]) % 2


def fsdp_peer(offset):
    xl, y, _, _, _ = where()
    return (xl + offset[0]) % 2, (y + offset[1]) % 4


def seq_id(peer):
    return {"seq_0": peer[0], "seq_1": peer[1], "seq_2": peer[2]}


def fsdp_id(peer):
    return {"fsdp_0": peer[0], "fsdp_1": peer[1]}


class GatherRing:
    def __init__(self, copies, slot, pair_axis, pair, ring_axis, ring, far):
        self.planes = (pair, 1 - pair)
        after, before = {ring_axis: (ring + 1) % 4}, {ring_axis: (ring + 3) % 4}
        other = {pair_axis: 1 - pair}

        def same(piece, to):
            return copies.make(piece, piece, to)

        self.cross = [same(slot(pair, ring, h), other) for h in range(2)]
        self.up = [[same(slot(p, ring, h), after) for h in range(2)] for p in self.planes]
        self.down = [[same(slot(p, ring, h), before) for h in range(2)] for p in self.planes]
        passed = self.planes[:1] if far else self.planes
        self.pass_up = [same(slot(p, (ring + 3) % 4, 0), after) for p in passed]
        self.pass_down = [same(slot(p, (ring + 1) % 4, 1), before) for p in passed]
        if far:
            self.far = [same(slot(pair, (ring + 2) % 4, h), other) for h in range(2)]


GATHER_COPIES = 14


class ReduceRing:
    def __init__(self, copies, out, arrived, value, pair_axis, pair, ring_axis, ring):
        up, down = {ring_axis: (ring + 1) % 4}, {ring_axis: (ring + 3) % 4}
        other = {pair_axis: 1 - pair}
        to = [other] * 2 + [up] * 2 + [down] * 2 + [up] * 3 + [down] * 3 + [other] * 2
        self.out, self.arrived, self.value = out, arrived, value
        self.pieces = [copies.make(out.at[i], arrived.at[i], t) for i, t in enumerate(to)]

    def put(self, i, value):
        self.out[i] = value.astype(BF16)
        self.pieces[i].start()

    def got(self, i):
        self.pieces[i].wait_recv()
        return self.arrived[i].astype(F32)

    def send_far(self):
        self.put(0, self.value(1, 2, 0))
        self.put(1, self.value(1, 2, 1))

    def send_up(self):
        self.put(2, self.value(1, 1, 0))
        self.put(3, self.value(1, 1, 1))

    def send_down(self):
        self.put(4, self.value(1, 3, 0))
        self.put(5, self.value(1, 3, 1))

    def own_up(self):
        self.put(7, self.value(0, 1, 1))

    def own_down(self):
        self.put(10, self.value(0, 3, 0))

    def own_far(self, h):
        self.put((6, 9)[h], self.value(0, 2, h) + self.got(h))

    def pass_on(self, h):
        self.put((8, 11)[h], self.value(0, (1, 3)[h], h) + self.got((6, 9)[h]))

    def cross(self):
        self.put(12, self.value(1, 0, 0) + self.got(2) + self.got(4))
        self.put(13, self.value(1, 0, 1) + self.got(3) + self.got(5))

    def total(self, h):
        parts = ((8, 10, 12), (7, 11, 13))[h]
        result = self.value(0, 0, h)
        for i in parts:
            result = result + self.got(i)
        return result


class PlainReduceRing(ReduceRing):
    def __init__(self, copies, out, arrived, value, pair_axis, pair, ring_axis, ring):
        up, down = {ring_axis: (ring + 1) % 4}, {ring_axis: (ring + 3) % 4}
        to = ([up] * 3 + [down] * 3) * 2 + [{pair_axis: 1 - pair}] * 2
        self.out, self.arrived, self.value = out, arrived, value
        self.pieces = [copies.make(out.at[i], arrived.at[i], t) for i, t in enumerate(to)]

    def first(self, plane):
        base = 6 * (1 - plane)
        self.put(base, self.value(plane, 2, 0))
        self.put(base + 3, self.value(plane, 2, 1))
        self.put(base + 1, self.value(plane, 1, 1))
        self.put(base + 4, self.value(plane, 3, 0))

    def pass_on(self, plane):
        base = 6 * (1 - plane)
        self.put(base + 2, self.value(plane, 1, 0) + self.got(base))
        self.put(base + 5, self.value(plane, 3, 1) + self.got(base + 3))

    def own(self, plane, h):
        base = 6 * (1 - plane)
        near = self.got(base + (2, 1)[h]) + self.got(base + (4, 5)[h])
        return self.value(plane, 0, h) + near

    def cross(self):
        for h in range(2):
            self.put(12 + h, self.own(1, h))

    def total(self, h):
        return self.own(0, h) + self.got(12 + h)


REDUCE_COPIES = 14


def step_kernel(
    image, text, w_qkv, qgain, kgain, cotangent, text_cotangent,
    image_out, text_out, weight_out, gain_out,
    tokens, weights, triple, upstream, qn, kn, kn_t, expd, esum, dsd, dpd, dv, gsum,
    grads, grads_other, dw, dx_out, dx_in, dw_out, dw_in,
    text_part, text_in, text_all, gain_seq, gain_fsdp, send, recv, local_sems,
):
    xl, y, xh, z, core = where()
    own = (xh * 4 + z) * 2 + core
    group = xl * 4 + y
    half = IMAGE_CHUNK // 2
    whalf = WEIGHT_ROWS // 2
    total_rows = tokens.shape[0]
    text_count = text.shape[0]
    text_rows = pl.ds(IMAGE_ROWS, text_count)
    factor = 1.0 / math.sqrt(HEAD)
    scale = factor * math.log2(math.e)
    planes = (xh, 1 - xh)
    other_core = {"seq_2": 1 - core}

    barrier = pltpu.get_barrier_semaphore()
    greeted = [seq_id(seq_peer(o)) for o in SEQ_OFFSETS] + [
        fsdp_id(fsdp_peer(o)) for o in FSDP_OFFSETS
    ]
    for peer in greeted:
        pl.semaphore_signal(barrier, inc=1, device_id=peer, device_id_type=MESH)

    def columns(s):
        return pl.ds(pl.multiple_of(s * HEAD, HEAD), HEAD)

    def chunk(s):
        return pl.ds(pl.multiple_of(s * IMAGE_CHUNK, IMAGE_CHUNK), IMAGE_CHUNK)

    def token_slot(p, r, h):
        start = ((p * 4 + r) * 2 + core) * IMAGE_CHUNK + h * half
        return tokens.at[pl.ds(pl.multiple_of(start, half), half), :]

    def weight_slot(p, r, h):
        start = (p * 4 + r) * WEIGHT_ROWS + h * whalf
        return weights.at[0, pl.ds(pl.multiple_of(start, whalf), whalf), :]

    group_rows = pl.ds(pl.multiple_of(group * WEIGHT_ROWS, WEIGHT_ROWS), WEIGHT_ROWS)
    fill_image = pltpu.make_async_copy(image, tokens.at[chunk(own), :], local_sems.at[0])
    fill_weights = [
        pltpu.make_async_copy(
            w_qkv.at[j, :, columns(own)],
            weights.at[0, group_rows, j * HEAD : (j + 1) * HEAD],
            local_sems.at[1 + j],
        )
        for j in range(3)
    ]
    fill_text = pltpu.make_async_copy(text, tokens.at[text_rows, :], local_sems.at[4])
    fill_upstream = [
        pltpu.make_async_copy(
            cotangent.at[:, columns(own)], upstream.at[chunk(own), :], local_sems.at[5]
        ),
        pltpu.make_async_copy(
            text_cotangent.at[:, columns(own)], upstream.at[text_rows, :], local_sems.at[6]
        ),
    ]
    for fill in (fill_image, *fill_weights, fill_text, *fill_upstream):
        fill.start()

    copies = Copies(send, recv)
    t = GatherRing(copies, token_slot, "seq_0", xh, "seq_1", z, True)
    w = GatherRing(copies, weight_slot, "fsdp_0", xl, "fsdp_1", y, False)
    shared = {}
    for plane, d in UNITS:
        for h in range(2):
            piece = token_slot(planes[plane], (z + d) % 4, h)
            shared[plane, d, h] = copies.make(piece, piece, other_core)
    exchanged = []
    for offset in SEQ_OFFSETS:
        peer = seq_peer(offset)
        s = (peer[0] * 4 + peer[1]) * 2 + peer[2]
        exchanged.append(
            copies.make(cotangent.at[:, columns(s)], upstream.at[chunk(own), :], seq_id(peer))
        )
    weights_shared = copies.make(weights.at[0], weights.at[1], other_core)

    def unit_at(plane, d):
        return planes[plane] * 4 + (z + d) % 4

    grads_shared = {}
    for plane, d in UNITS:
        at = unit_at(plane, d)
        grads_shared[plane, d] = copies.make(
            grads.at[chunk(at * 2 + 1 - core), :], grads_other.at[chunk(at), :], other_core
        )
    text_half = text_count // 2

    def text_share(c):
        return pl.ds(pl.multiple_of(IMAGE_ROWS + c * text_half, text_half), text_half)

    text_got = pl.ds(IMAGE_ROWS // 2, text_half)
    text_shared = copies.make(grads.at[text_share(1 - core), :], grads_other.at[text_got, :], other_core)
    gain_first = [
        copies.make(gain_seq.at[own], gain_seq.at[own], seq_id(seq_peer(o))) for o in SEQ_OFFSETS
    ]
    gain_second = [
        copies.make(gain_fsdp.at[group], gain_fsdp.at[group], fsdp_id(fsdp_peer(o)))
        for o in FSDP_OFFSETS
    ]
    text_first, text_second = [], []
    for o in FSDP_OFFSETS:
        peer = seq_peer((o[0], o[1], 0))
        to = {"seq_0": peer[0], "seq_1": peer[1]}
        text_first.append(copies.make(text_part.at[peer[0], peer[1]], text_in.at[xh, z], to))
        text_second.append(copies.make(text_all.at[core, xh, z], text_all.at[core, xh, z], to))
    text_third = copies.make(text_all.at[core], text_all.at[core], other_core)

    def dx_value(plane, d, h):
        start = (plane * 4 + d) * IMAGE_CHUNK + h * half
        return expd[start : start + half, : tokens.shape[1]]

    def dw_value(plane, d, h):
        f = (xl if plane == 0 else 1 - xl) * 4 + (y + d) % 4
        return dw[pl.ds(pl.multiple_of(f * WEIGHT_ROWS + h * whalf, whalf), whalf), :]

    dx_ring = ReduceRing(copies, dx_out, dx_in, dx_value, "seq_0", xh, "seq_1", z)
    dw_ring = PlainReduceRing(copies, dw_out, dw_in, dw_value, "fsdp_0", xl, "fsdp_1", y)

    fill_image.wait()
    pl.semaphore_wait(barrier, len(greeted))
    for h in range(2):
        t.cross[h].start()
        t.up[0][h].start()
        t.down[0][1 - h].start()
    for fill in fill_weights:
        fill.wait()
    for h in range(2):
        w.cross[h].start()
        w.up[0][h].start()
        w.down[0][1 - h].start()
    for h in range(2):
        shared[0, 0, h].start()

    def pass_weights(plane):
        w.up[plane][0].wait_recv()
        w.pass_up[plane].start()
        w.down[plane][1].wait_recv()
        w.pass_down[plane].start()

    t.up[0][0].wait_recv()
    t.pass_up[0].start()
    shared[0, 3, 0].start()
    t.down[0][1].wait_recv()
    t.pass_down[0].start()
    shared[0, 1, 1].start()
    pass_weights(0)
    for h in range(2):
        w.cross[h].wait_recv()
        w.up[1][h].start()
        w.down[1][h].start()
    for h in range(2):
        t.cross[h].wait_recv()
        t.up[1][h].start()
        t.down[1][h].start()
        shared[1, 0, h].start()
    t.up[0][1].wait_recv()
    shared[0, 3, 1].start()
    t.down[0][0].wait_recv()
    shared[0, 1, 0].start()
    pass_weights(1)
    t.pass_up[0].wait_recv()
    t.far[0].start()
    shared[0, 2, 0].start()
    t.pass_down[0].wait_recv()
    t.far[1].start()
    shared[0, 2, 1].start()
    for copy in exchanged:
        copy.start()
    for plane in range(2):
        w.up[plane][1].wait_recv()
        w.down[plane][0].wait_recv()
        w.pass_up[plane].wait_recv()
        w.pass_down[plane].wait_recv()
    weights_shared.start()

    def normed(values, gain):
        inverse = lax.rsqrt(jnp.mean(values * values, axis=-1, keepdims=True) + EPS)
        return (values * inverse * gain).astype(BF16)

    def project(start, count):
        at = pl.ds(start, count)
        result = dot_nn(tokens[at, :], weights[0]).astype(BF16)
        triple[at, :] = result
        qn[at, :] = normed(result[:, :HEAD].astype(F32), qgain[...])
        keys = normed(result[:, HEAD : 2 * HEAD].astype(F32), kgain[...])
        kn[at, :] = keys
        kn_t[:, at] = keys.T

    def unit_start(plane, d):
        return pl.multiple_of(unit_at(plane, d) * Q_ROWS, Q_ROWS)

    def project_unit(plane, d):
        for h in range(2):
            shared[plane, d, h].wait_recv()
        project(unit_start(plane, d), Q_ROWS)

    blocks = IMAGE_ROWS // Q_ROWS

    def exponentials(start, count, keys):
        at = pl.ds(start, count)
        qb = qn[at, :]
        total = jnp.zeros((8, count), F32)
        for key in keys:
            part = pl.ds(key, HEAD)
            e = jnp.exp2(dot_nt(kn[part, :], qb) * scale)
            expd[part, at] = e
            total = total + folded(e)
        esum[:, at] += total

    def plane_keys(plane):
        base = planes[plane] * (IMAGE_ROWS // 2)
        return [pl.multiple_of(base + c, HEAD) for c in range(0, IMAGE_ROWS // 2, HEAD)]

    def exponential_blocks(plane, keys):
        def block(i, carry):
            at = planes[plane] * (blocks // 2) + i
            exponentials(pl.multiple_of(at * Q_ROWS, Q_ROWS), Q_ROWS, keys)
            return carry

        lax.fori_loop(0, blocks // 2, block, 0)

    esum[...] = jnp.zeros_like(esum)
    fill_text.wait()
    project(IMAGE_ROWS, text_count)
    for d in range(4):
        project_unit(0, d)
    own_keys = plane_keys(0) + [IMAGE_ROWS]
    exponential_blocks(0, own_keys)
    exponentials(IMAGE_ROWS, text_count, own_keys)
    for h in range(2):
        t.up[1][h].wait_recv()
        shared[1, 3, h].start()
        t.down[1][h].wait_recv()
        shared[1, 1, h].start()
    project_unit(1, 0)
    for h in range(2):
        t.far[h].wait_recv()
        shared[1, 2, h].start()
    project_unit(1, 1)
    project_unit(1, 3)
    project_unit(1, 2)

    exponential_blocks(1, plane_keys(0) + plane_keys(1) + [IMAGE_ROWS])
    exponential_blocks(0, plane_keys(1))
    exponentials(IMAGE_ROWS, text_count, plane_keys(1))

    dv[...] = jnp.zeros_like(dv)
    gsum[...] = jnp.zeros_like(gsum)
    key_parts = [pl.ds(c, KEY_ROWS) for c in range(0, total_rows, KEY_ROWS)]

    def score_grads(start, count):
        at = pl.ds(start, count)
        ub = upstream[at, :]
        inner = jnp.zeros((8, count), F32)
        for part in key_parts:
            d = dot_nt(triple[part, 2 * HEAD :], ub)
            dpd[part, :count] = d
            inner = inner + folded(expd[part, at] * d)
        recip = 1.0 / jnp.sum(esum[:, at], axis=0, keepdims=True)
        delta = jnp.sum(inner, axis=0, keepdims=True) * recip
        for part in key_parts:
            p = expd[part, at] * recip
            dsd[part, at] = (p * (dpd[part, :count] - delta)).astype(BF16)
            dv[part, :] += dot_nn(p.astype(BF16), ub)

    for fill in fill_upstream:
        fill.wait()
    score_grads(IMAGE_ROWS, text_count)

    def score_block(i, carry):
        for plane in range(2):

            @pl.when(i == 4 * plane)
            def _():
                for offset, copy in zip(SEQ_OFFSETS, exchanged):
                    if offset[0] == plane:
                        copy.wait_recv()

        at = (xh + i // 4) % 2 * 4 + (z + i) % 4
        score_grads(pl.multiple_of(at * Q_ROWS, Q_ROWS), Q_ROWS)
        return carry

    lax.fori_loop(0, blocks, score_block, 0)

    def back(values, gain, incoming):
        floated = values.astype(F32)
        inverse = lax.rsqrt(jnp.mean(floated * floated, axis=-1, keepdims=True) + EPS)
        weighted = incoming * gain
        inner = jnp.mean(weighted * floated, axis=-1, keepdims=True)
        grad = inverse * weighted - floated * (inverse * inverse * inverse * inner)
        return grad.astype(BF16), folded(incoming * floated * inverse)

    def token_grads(start, count):
        at = pl.ds(start, count)
        dq = dot_nn(kn_t[...], dsd[:, at]).T * factor
        dk = dot_nn(dsd[at, :], qn[...]) * factor
        dq, q_part = back(triple[at, :HEAD], qgain[...], dq)
        dk, k_part = back(triple[at, HEAD : 2 * HEAD], kgain[...], dk)
        grads[at, :HEAD] = dq
        grads[at, HEAD : 2 * HEAD] = dk
        grads[at, 2 * HEAD :] = dv[at, :].astype(BF16)
        gsum[0:8, :] += q_part
        gsum[8:16, :] += k_part

    def unit_grads(plane, d):
        token_grads(unit_start(plane, d), Q_ROWS)
        grads_shared[plane, d].start()

    def input_part(mine, theirs):
        return dot_nt(grads[mine, :], weights[0]) + dot_nt(grads_other[theirs, :], weights[1])

    def input_sum(plane, d):
        at = unit_at(plane, d)
        grads_shared[plane, d].wait_recv()
        start = (plane * 4 + d) * IMAGE_CHUNK
        expd[start : start + IMAGE_CHUNK, : tokens.shape[1]] = input_part(
            chunk(at * 2 + core), chunk(at)
        )

    def weight_part(j):
        block = 2 * WEIGHT_ROWS
        dw[j * block : (j + 1) * block, :] = dot_tn(
            tokens[:, j * block : (j + 1) * block], grads[...]
        )

    unit_grads(1, 1)
    unit_grads(1, 2)
    token_grads(IMAGE_ROWS, text_count)
    text_shared.start()
    unit_grads(1, 3)
    weights_shared.wait_recv()
    input_sum(1, 1)
    dx_ring.send_up()
    input_sum(1, 2)
    dx_ring.send_far()
    input_sum(1, 3)
    dx_ring.send_down()
    text_shared.wait_recv()
    text_sum = input_part(text_share(core), text_got).astype(BF16)
    rows, width = text_part.shape[2:]
    for a, b in UNITS:
        text_part[a, b] = text_sum[b * rows : (b + 1) * rows, a * width : (a + 1) * width]
    for copy in text_first:
        copy.start()
    text_in[xh, z] = text_part[xh, z]
    for unit in ((0, 2), (0, 1), (0, 3), (1, 0), (0, 0)):
        unit_grads(*unit)
    gain_seq[own] = jnp.zeros(gain_seq.shape[1:], F32)
    gain_seq[own, 0:1, :] = jnp.sum(gsum[0:8, :], axis=0, keepdims=True)
    gain_seq[own, 1:2, :] = jnp.sum(gsum[8:16, :], axis=0, keepdims=True)
    for copy in gain_first:
        copy.start()
    input_sum(0, 2)
    dx_ring.own_far(0)
    weight_part(0)
    weight_part(1)
    input_sum(0, 1)
    dx_ring.own_up()
    dx_ring.own_far(1)
    input_sum(0, 3)
    dx_ring.own_down()
    weight_part(2)
    weight_part(3)
    dw_ring.first(1)
    input_sum(1, 0)
    dx_ring.cross()
    dw_ring.first(0)
    dx_ring.pass_on(0)
    for copy in text_first:
        copy.wait_recv()
    text_all[core, xh, z] = jnp.sum(text_in[...].astype(F32), axis=(0, 1)).astype(BF16)
    for copy in text_second:
        copy.start()
    dw_ring.pass_on(1)
    for copy in gain_first:
        copy.wait_recv()
    gain_fsdp[group] = jnp.sum(gain_seq[...], axis=0)
    for copy in gain_second:
        copy.start()
    dx_ring.pass_on(1)
    dw_ring.pass_on(0)
    dw_ring.cross()
    input_sum(0, 0)
    for copy in gain_second:
        copy.wait_recv()
    gain_out[...] = jnp.sum(gain_fsdp[...], axis=0)[0:2]
    for copy in text_second:
        copy.wait_recv()
    text_third.start()
    for h in range(2):
        image_out[h * half : (h + 1) * half, :] = dx_ring.total(h).astype(BF16)
    for h in range(2):
        total = dw_ring.total(h)
        for j in range(3):
            weight_out[j, h * whalf : (h + 1) * whalf, :] = total[:, j * HEAD : (j + 1) * HEAD]
    text_third.wait_recv()
    for c in range(2):
        for a, b in UNITS:
            text_out[
                c * text_half + b * rows : c * text_half + (b + 1) * rows,
                a * width : (a + 1) * width,
            ] = text_all[c, a, b]
    for copy in copies.made:
        copy.wait_send()


def step(image, text, w_qkv, query_gain, key_gain, cotangent, text_cotangent):
    features = image.shape[1]
    text_count = text.shape[0]
    total = IMAGE_ROWS + text_count
    depth = w_qkv.shape[1] * 8
    hbm = pl.BlockSpec(memory_space=pltpu.HBM)
    vmem = pl.BlockSpec(memory_space=pltpu.VMEM)
    half, whalf = IMAGE_CHUNK // 2, WEIGHT_ROWS // 2
    text_piece = (2, 4, text_count // 8, features // 2)
    n_copies = (
        2 * GATHER_COPIES + 16 + len(SEQ_OFFSETS) + 1 + 9
        + len(SEQ_OFFSETS) + len(FSDP_OFFSETS) + 2 * len(FSDP_OFFSETS) + 1 + 2 * REDUCE_COPIES
    )
    return pl.pallas_call(
        step_kernel,
        out_shape=(
            jax.ShapeDtypeStruct((IMAGE_CHUNK, features), BF16),
            jax.ShapeDtypeStruct((text_count, features), BF16),
            jax.ShapeDtypeStruct((3, WEIGHT_ROWS, HEAD), F32),
            jax.ShapeDtypeStruct((2, HEAD), F32),
        ),
        in_specs=[hbm, hbm, hbm, vmem, vmem, hbm, hbm],
        out_specs=(vmem,) * 4,
        scratch_shapes=[
            pltpu.VMEM((total, features), BF16),
            pltpu.VMEM((2, depth, WIDTH), BF16),
            pltpu.VMEM((total, WIDTH), BF16),
            pltpu.VMEM((total, HEAD), BF16),
            pltpu.VMEM((total, HEAD), BF16),
            pltpu.VMEM((total, HEAD), BF16),
            pltpu.VMEM((HEAD, total), BF16),
            pltpu.VMEM((total, total), F32),
            pltpu.VMEM((8, total), F32),
            pltpu.VMEM((total, total), BF16),
            pltpu.VMEM((total, Q_ROWS), F32),
            pltpu.VMEM((total, HEAD), F32),
            pltpu.VMEM((16, HEAD), F32),
            pltpu.VMEM((total, WIDTH), BF16),
            pltpu.VMEM((total // 2, WIDTH), BF16),
            pltpu.VMEM((depth, WIDTH), F32),
            pltpu.VMEM((REDUCE_COPIES, half, features), BF16),
            pltpu.VMEM((REDUCE_COPIES, half, features), BF16),
            pltpu.VMEM((REDUCE_COPIES, whalf, WIDTH), BF16),
            pltpu.VMEM((REDUCE_COPIES, whalf, WIDTH), BF16),
            pltpu.VMEM(text_piece, BF16),
            pltpu.VMEM(text_piece, BF16),
            pltpu.VMEM((2, *text_piece), BF16),
            pltpu.VMEM((16, 8, HEAD), F32),
            pltpu.VMEM((8, 8, HEAD), F32),
            pltpu.SemaphoreType.DMA((n_copies,)),
            pltpu.SemaphoreType.DMA((n_copies,)),
            pltpu.SemaphoreType.DMA((7,)),
        ],
        compiler_params=pltpu.CompilerParams(
            collective_id=0, has_side_effects=True, vmem_limit_bytes=62 * 1024 * 1024
        ),
        name="step",
    )(image, text, w_qkv, query_gain, key_gain, cotangent, text_cotangent)


def store_kernel(*refs):
    count = (len(refs) - 2) // 3
    taken, kept, held = refs[:count], refs[count : 2 * count], refs[2 * count : 3 * count]
    loads, stores = refs[-2:]
    ins = [pltpu.make_async_copy(taken[i], held[i], loads.at[i]) for i in range(count)]
    outs = [pltpu.make_async_copy(held[i], kept[i], stores.at[i]) for i in range(count)]
    for copy in ins:
        copy.start()
    for i in range(count):
        ins[i].wait()
        outs[i].start()
    for copy in outs:
        copy.wait()


def store(*arrays):
    hbm = pl.BlockSpec(memory_space=pltpu.HBM)
    return pl.pallas_call(
        store_kernel,
        out_shape=tuple(jax.ShapeDtypeStruct(a.shape, a.dtype) for a in arrays),
        in_specs=[hbm] * len(arrays),
        out_specs=(hbm,) * len(arrays),
        scratch_shapes=[pltpu.VMEM(a.shape, a.dtype) for a in arrays]
        + [pltpu.SemaphoreType.DMA((len(arrays),))] * 2,
        compiler_params=pltpu.CompilerParams(vmem_limit_bytes=67043328),
        name="store",
    )(*arrays)


def local(image_input, text_input, w_qkv, query_gain, key_gain, image_cotangent, text_cotangent):
    image_out, text_out, grad_weights, gain_total = store(
        *step(
            image_input[0],
            text_input[0],
            w_qkv.transpose(1, 0, 2),
            query_gain.reshape(1, HEAD),
            key_gain.reshape(1, HEAD),
            image_cotangent[0],
            text_cotangent[0],
        )
    )
    return image_out[None], text_out[None], grad_weights.transpose(1, 0, 2), gain_total


def solution(mesh):
    finer = Mesh(
        mesh.devices.reshape(2, 4, 2, 4, 2), ("fsdp_0", "fsdp_1", "seq_0", "seq_1", "seq_2")
    )
    return jax.shard_map(
        local,
        mesh=finer,
        in_specs=(
            P(FSDP, SEQ, None),
            P(FSDP, None, None),
            P(FSDP, None, None),
            P(),
            P(),
            P(FSDP, SEQ, None),
            P(FSDP, None, None),
        ),
        out_specs=(P(FSDP, SEQ, None), P(FSDP, None, None), P(FSDP, None, SEQ), P()),
        check_vma=False,
    )
```

```python
import math

import jax
import jax.numpy as jnp
from jax import lax
from jax.experimental import pallas as pl
from jax.experimental.pallas import tpu as pltpu
from jax.sharding import Mesh
from jax.sharding import PartitionSpec as P

HEAD = 128
SEQ = ("seq_0", "seq_1", "seq_2")
FSDP = ("fsdp_0", "fsdp_1")
EPS = 1e-06
F32 = jnp.float32
BF16 = jnp.bfloat16
MESH = pl.DeviceIdType.MESH

Q_ROWS = 256
KEY_ROWS = 544
IMAGE_CHUNK = 128
IMAGE_ROWS = 2048
WEIGHT_ROWS = 192
WIDTH = 3 * HEAD


def dot_nt(a, b):
    return lax.dot_general(a, b, (((1,), (1,)), ((), ())), preferred_element_type=F32)


def dot_nn(a, b):
    return lax.dot_general(a, b, (((1,), (0,)), ((), ())), preferred_element_type=F32)


def dot_tn(a, b):
    return lax.dot_general(a, b, (((0,), (0,)), ((), ())), preferred_element_type=F32)


def folded(values):
    rows, width = values.shape
    return jnp.sum(values.reshape(rows // 8, 8, width), axis=0)


class Copies:
    def __init__(self, send, recv):
        self.send, self.recv, self.made = send, recv, []

    def make(self, src, dst, to):
        i = len(self.made)
        copy = pltpu.make_async_remote_copy(
            src_ref=src,
            dst_ref=dst,
            send_sem=self.send.at[i],
            recv_sem=self.recv.at[i],
            device_id=to,
            device_id_type=MESH,
        )
        self.made.append(copy)
        return copy


def where():
    return (
        lax.axis_index("fsdp_0"),
        lax.axis_index("fsdp_1"),
        lax.axis_index("seq_0"),
        lax.axis_index("seq_1"),
        lax.axis_index("seq_2"),
    )


SEQ_OFFSETS = [(a, b, c) for a in range(2) for b in range(4) for c in range(2) if a + b + c > 0]
FSDP_OFFSETS = [(a, b) for a in range(2) for b in range(4) if a + b > 0]
UNITS = [(a, b) for a in range(2) for b in range(4)]


def seq_peer(offset):
    _, _, xh, z, core = where()
    return (xh + offset[0]) % 2, (z + offset[1]) % 4, (core + offset[2]) % 2


def fsdp_peer(offset):
    xl, y, _, _, _ = where()
    return (xl + offset[0]) % 2, (y + offset[1]) % 4


def seq_id(peer):
    return {"seq_0": peer[0], "seq_1": peer[1], "seq_2": peer[2]}


def fsdp_id(peer):
    return {"fsdp_0": peer[0], "fsdp_1": peer[1]}


class GatherRing:
    def __init__(self, copies, slot, pair_axis, pair, ring_axis, ring, far):
        self.planes = (pair, 1 - pair)
        after, before = {ring_axis: (ring + 1) % 4}, {ring_axis: (ring + 3) % 4}
        other = {pair_axis: 1 - pair}

        def same(piece, to):
            return copies.make(piece, piece, to)

        self.cross = [same(slot(pair, ring, h), other) for h in range(2)]
        self.up = [[same(slot(p, ring, h), after) for h in range(2)] for p in self.planes]
        self.down = [[same(slot(p, ring, h), before) for h in range(2)] for p in self.planes]
        passed = self.planes[:1] if far else self.planes
        self.pass_up = [same(slot(p, (ring + 3) % 4, 0), after) for p in passed]
        self.pass_down = [same(slot(p, (ring + 1) % 4, 1), before) for p in passed]
        if far:
            self.far = [same(slot(pair, (ring + 2) % 4, h), other) for h in range(2)]


GATHER_COPIES = 14


class ReduceRing:
    def __init__(self, copies, out, arrived, value, pair_axis, pair, ring_axis, ring):
        up, down = {ring_axis: (ring + 1) % 4}, {ring_axis: (ring + 3) % 4}
        other = {pair_axis: 1 - pair}
        to = [other] * 2 + [up] * 2 + [down] * 2 + [up] * 3 + [down] * 3 + [other] * 2
        self.out, self.arrived, self.value = out, arrived, value
        self.pieces = [copies.make(out.at[i], arrived.at[i], t) for i, t in enumerate(to)]

    def put(self, i, value):
        self.out[i] = value.astype(BF16)
        self.pieces[i].start()

    def got(self, i):
        self.pieces[i].wait_recv()
        return self.arrived[i].astype(F32)

    def send_far(self):
        self.put(0, self.value(1, 2, 0))
        self.put(1, self.value(1, 2, 1))

    def send_up(self):
        self.put(2, self.value(1, 1, 0))
        self.put(3, self.value(1, 1, 1))

    def send_down(self):
        self.put(4, self.value(1, 3, 0))
        self.put(5, self.value(1, 3, 1))

    def own_up(self):
        self.put(7, self.value(0, 1, 1))

    def own_down(self):
        self.put(10, self.value(0, 3, 0))

    def own_far(self, h):
        self.put((6, 9)[h], self.value(0, 2, h) + self.got(h))

    def pass_on(self, h):
        self.put((8, 11)[h], self.value(0, (1, 3)[h], h) + self.got((6, 9)[h]))

    def cross(self):
        self.put(12, self.value(1, 0, 0) + self.got(2) + self.got(4))
        self.put(13, self.value(1, 0, 1) + self.got(3) + self.got(5))

    def total(self, h):
        parts = ((8, 10, 12), (7, 11, 13))[h]
        result = self.value(0, 0, h)
        for i in parts:
            result = result + self.got(i)
        return result


class PlainReduceRing(ReduceRing):
    def __init__(self, copies, out, arrived, value, pair_axis, pair, ring_axis, ring):
        up, down = {ring_axis: (ring + 1) % 4}, {ring_axis: (ring + 3) % 4}
        to = ([up] * 3 + [down] * 3) * 2 + [{pair_axis: 1 - pair}] * 2
        self.out, self.arrived, self.value = out, arrived, value
        self.pieces = [copies.make(out.at[i], arrived.at[i], t) for i, t in enumerate(to)]

    def first(self, plane):
        base = 6 * (1 - plane)
        self.put(base, self.value(plane, 2, 0))
        self.put(base + 3, self.value(plane, 2, 1))
        self.put(base + 1, self.value(plane, 1, 1))
        self.put(base + 4, self.value(plane, 3, 0))

    def pass_on(self, plane):
        base = 6 * (1 - plane)
        self.put(base + 2, self.value(plane, 1, 0) + self.got(base))
        self.put(base + 5, self.value(plane, 3, 1) + self.got(base + 3))

    def own(self, plane, h):
        base = 6 * (1 - plane)
        near = self.got(base + (2, 1)[h]) + self.got(base + (4, 5)[h])
        return self.value(plane, 0, h) + near

    def cross(self):
        for h in range(2):
            self.put(12 + h, self.own(1, h))

    def total(self, h):
        return self.own(0, h) + self.got(12 + h)


REDUCE_COPIES = 14


def step_kernel(
    image, text, w_qkv, qgain, kgain, cotangent, text_cotangent,
    image_out, text_out, weight_out, gain_out,
    tokens, weights, triple, upstream, qn, kn, kn_t, expd, esum, dsd, dpd, dv, gsum,
    grads, grads_other, dw, dx_out, dx_in, dw_out, dw_in,
    text_part, text_pair, text_sum, text_in, text_all, gain_seq, gain_fsdp, send, recv, local_sems,
):
    xl, y, xh, z, core = where()
    own = (xh * 4 + z) * 2 + core
    group = xl * 4 + y
    half = IMAGE_CHUNK // 2
    whalf = WEIGHT_ROWS // 2
    total_rows = tokens.shape[0]
    text_count = text.shape[0]
    text_rows = pl.ds(IMAGE_ROWS, text_count)
    factor = 1.0 / math.sqrt(HEAD)
    scale = factor * math.log2(math.e)
    planes = (xh, 1 - xh)
    other_core = {"seq_2": 1 - core}

    barrier = pltpu.get_barrier_semaphore()
    greeted = [seq_id(seq_peer(o)) for o in SEQ_OFFSETS] + [
        fsdp_id(fsdp_peer(o)) for o in FSDP_OFFSETS
    ]
    for peer in greeted:
        pl.semaphore_signal(barrier, inc=1, device_id=peer, device_id_type=MESH)

    def columns(s):
        return pl.ds(pl.multiple_of(s * HEAD, HEAD), HEAD)

    def chunk(s):
        return pl.ds(pl.multiple_of(s * IMAGE_CHUNK, IMAGE_CHUNK), IMAGE_CHUNK)

    def token_slot(p, r, h):
        start = ((p * 4 + r) * 2 + core) * IMAGE_CHUNK + h * half
        return tokens.at[pl.ds(pl.multiple_of(start, half), half), :]

    def weight_slot(p, r, h):
        start = (p * 4 + r) * WEIGHT_ROWS + h * whalf
        return weights.at[0, pl.ds(pl.multiple_of(start, whalf), whalf), :]

    group_rows = pl.ds(pl.multiple_of(group * WEIGHT_ROWS, WEIGHT_ROWS), WEIGHT_ROWS)
    fill_image = pltpu.make_async_copy(image, tokens.at[chunk(own), :], local_sems.at[0])
    fill_weights = [
        pltpu.make_async_copy(
            w_qkv.at[j, :, columns(own)],
            weights.at[0, group_rows, j * HEAD : (j + 1) * HEAD],
            local_sems.at[1 + j],
        )
        for j in range(3)
    ]
    fill_text = pltpu.make_async_copy(text, tokens.at[text_rows, :], local_sems.at[4])
    fill_upstream = [
        pltpu.make_async_copy(
            cotangent.at[:, columns(own)], upstream.at[chunk(own), :], local_sems.at[5]
        ),
        pltpu.make_async_copy(
            text_cotangent.at[:, columns(own)], upstream.at[text_rows, :], local_sems.at[6]
        ),
    ]
    for fill in (fill_image, *fill_weights, fill_text, *fill_upstream):
        fill.start()

    copies = Copies(send, recv)
    t = GatherRing(copies, token_slot, "seq_0", xh, "seq_1", z, True)
    w = GatherRing(copies, weight_slot, "fsdp_0", xl, "fsdp_1", y, False)
    shared = {}
    for plane, d in UNITS:
        for h in range(2):
            piece = token_slot(planes[plane], (z + d) % 4, h)
            shared[plane, d, h] = copies.make(piece, piece, other_core)
    exchanged = []
    for offset in SEQ_OFFSETS:
        peer = seq_peer(offset)
        s = (peer[0] * 4 + peer[1]) * 2 + peer[2]
        exchanged.append(
            copies.make(cotangent.at[:, columns(s)], upstream.at[chunk(own), :], seq_id(peer))
        )
    weights_shared = copies.make(weights.at[0], weights.at[1], other_core)

    def unit_at(plane, d):
        return planes[plane] * 4 + (z + d) % 4

    grads_shared = {}
    for plane, d in UNITS:
        at = unit_at(plane, d)
        grads_shared[plane, d] = copies.make(
            grads.at[chunk(at * 2 + 1 - core), :], grads_other.at[chunk(at), :], other_core
        )
    text_half = text_count // 2

    def text_share(c):
        return pl.ds(pl.multiple_of(IMAGE_ROWS + c * text_half, text_half), text_half)

    text_got = pl.ds(IMAGE_ROWS // 2, text_half)
    text_shared = copies.make(grads.at[text_share(1 - core), :], grads_other.at[text_got, :], other_core)
    gain_first = [
        copies.make(gain_seq.at[own], gain_seq.at[own], seq_id(seq_peer(o))) for o in SEQ_OFFSETS
    ]
    gain_second = [
        copies.make(gain_fsdp.at[group], gain_fsdp.at[group], fsdp_id(fsdp_peer(o)))
        for o in FSDP_OFFSETS
    ]
    other_pair = {"seq_0": 1 - xh}
    text_cross = copies.make(text_part.at[1 - xh], text_pair, other_pair)
    text_first, text_second = [], []
    for d in range(1, 4):
        at = (z + d) % 4
        text_first.append(copies.make(text_sum.at[at], text_in.at[z], {"seq_1": at}))
        text_second.append(
            copies.make(text_all.at[core, xh, z], text_all.at[core, xh, z], {"seq_1": at})
        )
    text_third = copies.make(text_all.at[core, xh], text_all.at[core, xh], other_pair)
    text_fourth = copies.make(text_all.at[core], text_all.at[core], other_core)

    def dx_value(plane, d, h):
        start = (plane * 4 + d) * IMAGE_CHUNK + h * half
        return expd[start : start + half, : tokens.shape[1]]

    def dw_value(plane, d, h):
        f = (xl if plane == 0 else 1 - xl) * 4 + (y + d) % 4
        return dw[pl.ds(pl.multiple_of(f * WEIGHT_ROWS + h * whalf, whalf), whalf), :]

    dx_ring = ReduceRing(copies, dx_out, dx_in, dx_value, "seq_0", xh, "seq_1", z)
    dw_ring = PlainReduceRing(copies, dw_out, dw_in, dw_value, "fsdp_0", xl, "fsdp_1", y)

    fill_image.wait()
    pl.semaphore_wait(barrier, len(greeted))
    for h in range(2):
        t.cross[h].start()
        t.up[0][h].start()
        t.down[0][1 - h].start()
    for fill in fill_weights:
        fill.wait()
    for h in range(2):
        w.cross[h].start()
        w.up[0][h].start()
        w.down[0][1 - h].start()
    for h in range(2):
        shared[0, 0, h].start()

    def pass_weights(plane):
        w.up[plane][0].wait_recv()
        w.pass_up[plane].start()
        w.down[plane][1].wait_recv()
        w.pass_down[plane].start()

    t.up[0][0].wait_recv()
    t.pass_up[0].start()
    shared[0, 3, 0].start()
    t.down[0][1].wait_recv()
    t.pass_down[0].start()
    shared[0, 1, 1].start()
    pass_weights(0)
    for h in range(2):
        w.cross[h].wait_recv()
        w.up[1][h].start()
        w.down[1][h].start()
    for h in range(2):
        t.cross[h].wait_recv()
        t.up[1][h].start()
        t.down[1][h].start()
        shared[1, 0, h].start()
    t.up[0][1].wait_recv()
    shared[0, 3, 1].start()
    t.down[0][0].wait_recv()
    shared[0, 1, 0].start()
    pass_weights(1)
    t.pass_up[0].wait_recv()
    t.far[0].start()
    shared[0, 2, 0].start()
    t.pass_down[0].wait_recv()
    t.far[1].start()
    shared[0, 2, 1].start()
    for copy in exchanged:
        copy.start()
    for plane in range(2):
        w.up[plane][1].wait_recv()
        w.down[plane][0].wait_recv()
        w.pass_up[plane].wait_recv()
        w.pass_down[plane].wait_recv()
    weights_shared.start()

    def normed(values, gain):
        inverse = lax.rsqrt(jnp.mean(values * values, axis=-1, keepdims=True) + EPS)
        return (values * inverse * gain).astype(BF16)

    def project(start, count):
        at = pl.ds(start, count)
        result = dot_nn(tokens[at, :], weights[0]).astype(BF16)
        triple[at, :] = result
        qn[at, :] = normed(result[:, :HEAD].astype(F32), qgain[...])
        keys = normed(result[:, HEAD : 2 * HEAD].astype(F32), kgain[...])
        kn[at, :] = keys
        kn_t[:, at] = keys.T

    def unit_start(plane, d):
        return pl.multiple_of(unit_at(plane, d) * Q_ROWS, Q_ROWS)

    def project_unit(plane, d):
        for h in range(2):
            shared[plane, d, h].wait_recv()
        project(unit_start(plane, d), Q_ROWS)

    blocks = IMAGE_ROWS // Q_ROWS

    def exponentials(start, count, keys):
        at = pl.ds(start, count)
        qb = qn[at, :]
        total = jnp.zeros((8, count), F32)
        for key in keys:
            part = pl.ds(key, HEAD)
            e = jnp.exp2(dot_nt(kn[part, :], qb) * scale)
            expd[part, at] = e
            total = total + folded(e)
        esum[:, at] += total

    def plane_keys(plane):
        base = planes[plane] * (IMAGE_ROWS // 2)
        return [pl.multiple_of(base + c, HEAD) for c in range(0, IMAGE_ROWS // 2, HEAD)]

    def exponential_blocks(plane, keys):
        def block(i, carry):
            at = planes[plane] * (blocks // 2) + i
            exponentials(pl.multiple_of(at * Q_ROWS, Q_ROWS), Q_ROWS, keys)
            return carry

        lax.fori_loop(0, blocks // 2, block, 0)

    esum[...] = jnp.zeros_like(esum)
    fill_text.wait()
    project(IMAGE_ROWS, text_count)
    for d in range(4):
        project_unit(0, d)
    own_keys = plane_keys(0) + [IMAGE_ROWS]
    exponential_blocks(0, own_keys)
    exponentials(IMAGE_ROWS, text_count, own_keys)
    for h in range(2):
        t.up[1][h].wait_recv()
        shared[1, 3, h].start()
        t.down[1][h].wait_recv()
        shared[1, 1, h].start()
    project_unit(1, 0)
    project_unit(1, 1)
    project_unit(1, 3)
    for h in range(2):
        t.far[h].wait_recv()
        shared[1, 2, h].start()
    project_unit(1, 2)

    exponential_blocks(1, plane_keys(0) + plane_keys(1) + [IMAGE_ROWS])
    exponential_blocks(0, plane_keys(1))
    exponentials(IMAGE_ROWS, text_count, plane_keys(1))

    dv[...] = jnp.zeros_like(dv)
    gsum[...] = jnp.zeros_like(gsum)
    key_parts = [pl.ds(c, KEY_ROWS) for c in range(0, total_rows, KEY_ROWS)]

    def score_grads(start, count):
        at = pl.ds(start, count)
        ub = upstream[at, :]
        inner = jnp.zeros((8, count), F32)
        for part in key_parts:
            d = dot_nt(triple[part, 2 * HEAD :], ub)
            dpd[part, :count] = d
            inner = inner + folded(expd[part, at] * d)
        recip = 1.0 / jnp.sum(esum[:, at], axis=0, keepdims=True)
        delta = jnp.sum(inner, axis=0, keepdims=True) * recip
        for part in key_parts:
            p = expd[part, at] * recip
            dsd[part, at] = (p * (dpd[part, :count] - delta)).astype(BF16)
            dv[part, :] += dot_nn(p.astype(BF16), ub)

    for fill in fill_upstream:
        fill.wait()
    score_grads(IMAGE_ROWS, text_count)

    def score_block(i, carry):
        for plane in range(2):

            @pl.when(i == 4 * plane)
            def _():
                for offset, copy in zip(SEQ_OFFSETS, exchanged):
                    if offset[0] == plane:
                        copy.wait_recv()

        at = (xh + i // 4) % 2 * 4 + (z + i) % 4
        score_grads(pl.multiple_of(at * Q_ROWS, Q_ROWS), Q_ROWS)
        return carry

    lax.fori_loop(0, blocks, score_block, 0)

    def back(values, gain, incoming):
        floated = values.astype(F32)
        inverse = lax.rsqrt(jnp.mean(floated * floated, axis=-1, keepdims=True) + EPS)
        weighted = incoming * gain
        inner = jnp.mean(weighted * floated, axis=-1, keepdims=True)
        grad = inverse * weighted - floated * (inverse * inverse * inverse * inner)
        return grad.astype(BF16), folded(incoming * floated * inverse)

    def token_grads(start, count):
        at = pl.ds(start, count)
        dq = dot_nn(kn_t[...], dsd[:, at]).T * factor
        dk = dot_nn(dsd[at, :], qn[...]) * factor
        dq, q_part = back(triple[at, :HEAD], qgain[...], dq)
        dk, k_part = back(triple[at, HEAD : 2 * HEAD], kgain[...], dk)
        grads[at, :HEAD] = dq
        grads[at, HEAD : 2 * HEAD] = dk
        grads[at, 2 * HEAD :] = dv[at, :].astype(BF16)
        gsum[0:8, :] += q_part
        gsum[8:16, :] += k_part

    def unit_grads(plane, d):
        token_grads(unit_start(plane, d), Q_ROWS)
        grads_shared[plane, d].start()

    def input_part(mine, theirs):
        return dot_nt(grads[mine, :], weights[0]) + dot_nt(grads_other[theirs, :], weights[1])

    def input_sum(plane, d):
        at = unit_at(plane, d)
        grads_shared[plane, d].wait_recv()
        start = (plane * 4 + d) * IMAGE_CHUNK
        expd[start : start + IMAGE_CHUNK, : tokens.shape[1]] = input_part(
            chunk(at * 2 + core), chunk(at)
        )

    def weight_parts(plane):
        block = 2 * WEIGHT_ROWS
        pair = xl if plane == 0 else 1 - xl
        for j in range(2):
            at = pl.ds(pl.multiple_of((pair * 2 + j) * block, block), block)
            dw[at, :] = dot_tn(tokens[:, at], grads[...])

    token_grads(IMAGE_ROWS, text_count)
    text_shared.start()
    unit_grads(1, 1)
    unit_grads(1, 2)
    weights_shared.wait_recv()
    text_shared.wait_recv()
    text_terms = input_part(text_share(core), text_got).astype(BF16)
    rows, width = text_part.shape[2:]
    for a, b in UNITS:
        text_part[a, b] = text_terms[b * rows : (b + 1) * rows, a * width : (a + 1) * width]
    text_cross.start()
    input_sum(1, 1)
    dx_ring.send_up()
    unit_grads(1, 3)
    input_sum(1, 2)
    dx_ring.send_far()
    unit_grads(0, 2)
    input_sum(1, 3)
    dx_ring.send_down()
    text_cross.wait_recv()
    text_sum[...] = (text_part[xh].astype(F32) + text_pair[...].astype(F32)).astype(BF16)
    for copy in text_first:
        copy.start()
    text_in[z] = text_sum[z]
    for unit in ((0, 1), (0, 3), (1, 0), (0, 0)):
        unit_grads(*unit)
    gain_seq[own] = jnp.zeros(gain_seq.shape[1:], F32)
    gain_seq[own, 0:1, :] = jnp.sum(gsum[0:8, :], axis=0, keepdims=True)
    gain_seq[own, 1:2, :] = jnp.sum(gsum[8:16, :], axis=0, keepdims=True)
    for copy in gain_first:
        copy.start()
    input_sum(0, 2)
    dx_ring.own_far(0)
    weight_parts(1)
    dw_ring.first(1)
    input_sum(0, 1)
    dx_ring.own_up()
    dx_ring.own_far(1)
    input_sum(0, 3)
    dx_ring.own_down()
    for copy in text_first:
        copy.wait_recv()
    text_all[core, xh, z] = jnp.sum(text_in[...].astype(F32), axis=0).astype(BF16)
    for copy in text_second:
        copy.start()
    input_sum(1, 0)
    dx_ring.cross()
    weight_parts(0)
    dw_ring.pass_on(1)
    dw_ring.first(0)
    dx_ring.pass_on(0)
    for copy in gain_first:
        copy.wait_recv()
    gain_fsdp[group] = jnp.sum(gain_seq[...], axis=0)
    for copy in gain_second:
        copy.start()
    dw_ring.cross()
    dx_ring.pass_on(1)
    for copy in text_second:
        copy.wait_recv()
    text_third.start()
    input_sum(0, 0)
    dw_ring.pass_on(0)
    for copy in gain_second:
        copy.wait_recv()
    gain_out[...] = jnp.sum(gain_fsdp[...], axis=0)[0:2]
    text_third.wait_recv()
    text_fourth.start()
    for h in range(2):
        image_out[h * half : (h + 1) * half, :] = dx_ring.total(h).astype(BF16)
    for h in range(2):
        total = dw_ring.total(h)
        for j in range(3):
            weight_out[j, h * whalf : (h + 1) * whalf, :] = total[:, j * HEAD : (j + 1) * HEAD]
    text_fourth.wait_recv()
    for c in range(2):
        for a, b in UNITS:
            text_out[
                c * text_half + b * rows : c * text_half + (b + 1) * rows,
                a * width : (a + 1) * width,
            ] = text_all[c, a, b]
    for copy in copies.made:
        copy.wait_send()


def step(image, text, w_qkv, query_gain, key_gain, cotangent, text_cotangent):
    features = image.shape[1]
    text_count = text.shape[0]
    total = IMAGE_ROWS + text_count
    depth = w_qkv.shape[1] * 8
    hbm = pl.BlockSpec(memory_space=pltpu.HBM)
    vmem = pl.BlockSpec(memory_space=pltpu.VMEM)
    half, whalf = IMAGE_CHUNK // 2, WEIGHT_ROWS // 2
    text_piece = (2, 4, text_count // 8, features // 2)
    n_copies = (
        2 * GATHER_COPIES + 16 + len(SEQ_OFFSETS) + 1 + 9
        + len(SEQ_OFFSETS) + len(FSDP_OFFSETS) + 1 + 2 * 3 + 2 + 2 * REDUCE_COPIES
    )
    return pl.pallas_call(
        step_kernel,
        out_shape=(
            jax.ShapeDtypeStruct((IMAGE_CHUNK, features), BF16),
            jax.ShapeDtypeStruct((text_count, features), BF16),
            jax.ShapeDtypeStruct((3, WEIGHT_ROWS, HEAD), F32),
            jax.ShapeDtypeStruct((2, HEAD), F32),
        ),
        in_specs=[hbm, hbm, hbm, vmem, vmem, hbm, hbm],
        out_specs=(vmem,) * 4,
        scratch_shapes=[
            pltpu.VMEM((total, features), BF16),
            pltpu.VMEM((2, depth, WIDTH), BF16),
            pltpu.VMEM((total, WIDTH), BF16),
            pltpu.VMEM((total, HEAD), BF16),
            pltpu.VMEM((total, HEAD), BF16),
            pltpu.VMEM((total, HEAD), BF16),
            pltpu.VMEM((HEAD, total), BF16),
            pltpu.VMEM((total, total), F32),
            pltpu.VMEM((8, total), F32),
            pltpu.VMEM((total, total), BF16),
            pltpu.VMEM((total, Q_ROWS), F32),
            pltpu.VMEM((total, HEAD), F32),
            pltpu.VMEM((16, HEAD), F32),
            pltpu.VMEM((total, WIDTH), BF16),
            pltpu.VMEM((total // 2, WIDTH), BF16),
            pltpu.VMEM((depth, WIDTH), F32),
            pltpu.VMEM((REDUCE_COPIES, half, features), BF16),
            pltpu.VMEM((REDUCE_COPIES, half, features), BF16),
            pltpu.VMEM((REDUCE_COPIES, whalf, WIDTH), BF16),
            pltpu.VMEM((REDUCE_COPIES, whalf, WIDTH), BF16),
            pltpu.VMEM(text_piece, BF16),
            pltpu.VMEM(text_piece[1:], BF16),
            pltpu.VMEM(text_piece[1:], BF16),
            pltpu.VMEM(text_piece[1:], BF16),
            pltpu.VMEM((2, *text_piece), BF16),
            pltpu.VMEM((16, 8, HEAD), F32),
            pltpu.VMEM((8, 8, HEAD), F32),
            pltpu.SemaphoreType.DMA((n_copies,)),
            pltpu.SemaphoreType.DMA((n_copies,)),
            pltpu.SemaphoreType.DMA((7,)),
        ],
        compiler_params=pltpu.CompilerParams(
            collective_id=0, has_side_effects=True, vmem_limit_bytes=62 * 1024 * 1024
        ),
        name="step",
    )(image, text, w_qkv, query_gain, key_gain, cotangent, text_cotangent)


def store_kernel(*refs):
    count = (len(refs) - 2) // 3
    taken, kept, held = refs[:count], refs[count : 2 * count], refs[2 * count : 3 * count]
    loads, stores = refs[-2:]
    ins = [pltpu.make_async_copy(taken[i], held[i], loads.at[i]) for i in range(count)]
    outs = [pltpu.make_async_copy(held[i], kept[i], stores.at[i]) for i in range(count)]
    for copy in ins:
        copy.start()
    for i in range(count):
        ins[i].wait()
        outs[i].start()
    for copy in outs:
        copy.wait()


def store(*arrays):
    hbm = pl.BlockSpec(memory_space=pltpu.HBM)
    return pl.pallas_call(
        store_kernel,
        out_shape=tuple(jax.ShapeDtypeStruct(a.shape, a.dtype) for a in arrays),
        in_specs=[hbm] * len(arrays),
        out_specs=(hbm,) * len(arrays),
        scratch_shapes=[pltpu.VMEM(a.shape, a.dtype) for a in arrays]
        + [pltpu.SemaphoreType.DMA((len(arrays),))] * 2,
        compiler_params=pltpu.CompilerParams(vmem_limit_bytes=67043328),
        name="store",
    )(*arrays)


def local(image_input, text_input, w_qkv, query_gain, key_gain, image_cotangent, text_cotangent):
    image_out, text_out, grad_weights, gain_total = store(
        *step(
            image_input[0],
            text_input[0],
            w_qkv.transpose(1, 0, 2),
            query_gain.reshape(1, HEAD),
            key_gain.reshape(1, HEAD),
            image_cotangent[0],
            text_cotangent[0],
        )
    )
    return image_out[None], text_out[None], grad_weights.transpose(1, 0, 2), gain_total


def solution(mesh):
    finer = Mesh(
        mesh.devices.reshape(2, 4, 2, 4, 2), ("fsdp_0", "fsdp_1", "seq_0", "seq_1", "seq_2")
    )
    return jax.shard_map(
        local,
        mesh=finer,
        in_specs=(
            P(FSDP, SEQ, None),
            P(FSDP, None, None),
            P(FSDP, None, None),
            P(),
            P(),
            P(FSDP, SEQ, None),
            P(FSDP, None, None),
        ),
        out_specs=(P(FSDP, SEQ, None), P(FSDP, None, None), P(FSDP, None, SEQ), P()),
        check_vma=False,
    )
```

```python
import math

import jax
import jax.numpy as jnp
from jax import lax
from jax.experimental import pallas as pl
from jax.experimental.pallas import tpu as pltpu
from jax.sharding import Mesh
from jax.sharding import PartitionSpec as P

HEAD = 128
SEQ = ("seq_0", "seq_1", "seq_2")
FSDP = ("fsdp_0", "fsdp_1")
EPS = 1e-06
F32 = jnp.float32
BF16 = jnp.bfloat16
MESH = pl.DeviceIdType.MESH

Q_ROWS = 256
KEY_ROWS = 544
IMAGE_CHUNK = 128
IMAGE_ROWS = 2048
WEIGHT_ROWS = 192
WIDTH = 3 * HEAD


def dot_nt(a, b):
    return lax.dot_general(a, b, (((1,), (1,)), ((), ())), preferred_element_type=F32)


def dot_nn(a, b):
    return lax.dot_general(a, b, (((1,), (0,)), ((), ())), preferred_element_type=F32)


def dot_tn(a, b):
    return lax.dot_general(a, b, (((0,), (0,)), ((), ())), preferred_element_type=F32)


def folded(values):
    rows, width = values.shape
    return jnp.sum(values.reshape(rows // 8, 8, width), axis=0)


class Copies:
    def __init__(self, send, recv):
        self.send, self.recv, self.made = send, recv, []

    def make(self, src, dst, to):
        i = len(self.made)
        copy = pltpu.make_async_remote_copy(
            src_ref=src,
            dst_ref=dst,
            send_sem=self.send.at[i],
            recv_sem=self.recv.at[i],
            device_id=to,
            device_id_type=MESH,
        )
        self.made.append(copy)
        return copy


def where():
    return (
        lax.axis_index("fsdp_0"),
        lax.axis_index("fsdp_1"),
        lax.axis_index("seq_0"),
        lax.axis_index("seq_1"),
        lax.axis_index("seq_2"),
    )


SEQ_OFFSETS = [(a, b, c) for a in range(2) for b in range(4) for c in range(2) if a + b + c > 0]
FSDP_OFFSETS = [(a, b) for a in range(2) for b in range(4) if a + b > 0]
UNITS = [(a, b) for a in range(2) for b in range(4)]


def seq_peer(offset):
    _, _, xh, z, core = where()
    return (xh + offset[0]) % 2, (z + offset[1]) % 4, (core + offset[2]) % 2


def fsdp_peer(offset):
    xl, y, _, _, _ = where()
    return (xl + offset[0]) % 2, (y + offset[1]) % 4


def seq_id(peer):
    return {"seq_0": peer[0], "seq_1": peer[1], "seq_2": peer[2]}


def fsdp_id(peer):
    return {"fsdp_0": peer[0], "fsdp_1": peer[1]}


class GatherRing:
    def __init__(self, copies, slot, pair_axis, pair, ring_axis, ring, far):
        self.planes = (pair, 1 - pair)
        after, before = {ring_axis: (ring + 1) % 4}, {ring_axis: (ring + 3) % 4}
        other = {pair_axis: 1 - pair}

        def same(piece, to):
            return copies.make(piece, piece, to)

        self.cross = [same(slot(pair, ring, h), other) for h in range(2)]
        self.up = [[same(slot(p, ring, h), after) for h in range(2)] for p in self.planes]
        self.down = [[same(slot(p, ring, h), before) for h in range(2)] for p in self.planes]
        passed = self.planes[:1] if far else self.planes
        self.pass_up = [same(slot(p, (ring + 3) % 4, 0), after) for p in passed]
        self.pass_down = [same(slot(p, (ring + 1) % 4, 1), before) for p in passed]
        if far:
            self.far = [same(slot(pair, (ring + 2) % 4, h), other) for h in range(2)]


GATHER_COPIES = 14


class ReduceRing:
    def __init__(self, copies, out, arrived, value, pair_axis, pair, ring_axis, ring):
        up, down = {ring_axis: (ring + 1) % 4}, {ring_axis: (ring + 3) % 4}
        other = {pair_axis: 1 - pair}
        to = [other] * 2 + [up] * 2 + [down] * 2 + [up] * 3 + [down] * 3 + [other] * 2
        self.out, self.arrived, self.value = out, arrived, value
        self.pieces = [copies.make(out.at[i], arrived.at[i], t) for i, t in enumerate(to)]

    def put(self, i, value):
        self.out[i] = value.astype(BF16)
        self.pieces[i].start()

    def got(self, i):
        self.pieces[i].wait_recv()
        return self.arrived[i].astype(F32)

    def send_far(self, h):
        self.put(h, self.value(1, 2, h))

    def send_up(self):
        self.put(2, self.value(1, 1, 0))
        self.put(3, self.value(1, 1, 1))

    def send_down(self):
        self.put(4, self.value(1, 3, 0))
        self.put(5, self.value(1, 3, 1))

    def own_up(self):
        self.put(7, self.value(0, 1, 1))

    def own_down(self):
        self.put(10, self.value(0, 3, 0))

    def own_far(self, h):
        self.put((6, 9)[h], self.value(0, 2, h) + self.got(h))

    def pass_on(self, h):
        self.put((8, 11)[h], self.value(0, (1, 3)[h], h) + self.got((6, 9)[h]))

    def cross(self):
        self.put(12, self.value(1, 0, 0) + self.got(2) + self.got(4))
        self.put(13, self.value(1, 0, 1) + self.got(3) + self.got(5))

    def total(self, h):
        parts = ((8, 10, 12), (7, 11, 13))[h]
        result = self.value(0, 0, h)
        for i in parts:
            result = result + self.got(i)
        return result


class PlainReduceRing(ReduceRing):
    def __init__(self, copies, out, arrived, value, pair_axis, pair, ring_axis, ring):
        up, down = {ring_axis: (ring + 1) % 4}, {ring_axis: (ring + 3) % 4}
        to = ([up] * 3 + [down] * 3) * 2 + [{pair_axis: 1 - pair}] * 2
        self.out, self.arrived, self.value = out, arrived, value
        self.pieces = [copies.make(out.at[i], arrived.at[i], t) for i, t in enumerate(to)]

    def first(self, plane):
        base = 6 * (1 - plane)
        self.put(base, self.value(plane, 2, 0))
        self.put(base + 3, self.value(plane, 2, 1))
        self.put(base + 1, self.value(plane, 1, 1))
        self.put(base + 4, self.value(plane, 3, 0))

    def pass_on(self, plane):
        base = 6 * (1 - plane)
        self.put(base + 2, self.value(plane, 1, 0) + self.got(base))
        self.put(base + 5, self.value(plane, 3, 1) + self.got(base + 3))

    def own(self, plane, h):
        base = 6 * (1 - plane)
        near = self.got(base + (2, 1)[h]) + self.got(base + (4, 5)[h])
        return self.value(plane, 0, h) + near

    def cross(self):
        for h in range(2):
            self.put(12 + h, self.own(1, h))

    def total(self, h):
        return self.own(0, h) + self.got(12 + h)


REDUCE_COPIES = 14


def step_kernel(
    image, text, w_qkv, qgain, kgain, cotangent, text_cotangent,
    image_out, text_out, weight_out, gain_out,
    tokens, weights, triple, upstream, qn, kn, kn_t, expd, esum, dsd, dpd, dv, gsum,
    grads, grads_other, dw, dx_out, dx_in, dw_out, dw_in,
    text_part, text_pair, text_sum, text_in, text_all, gain_seq, gain_fsdp, send, recv, local_sems,
):
    xl, y, xh, z, core = where()
    own = (xh * 4 + z) * 2 + core
    group = xl * 4 + y
    half = IMAGE_CHUNK // 2
    whalf = WEIGHT_ROWS // 2
    total_rows = tokens.shape[0]
    text_count = text.shape[0]
    text_rows = pl.ds(IMAGE_ROWS, text_count)
    factor = 1.0 / math.sqrt(HEAD)
    scale = factor * math.log2(math.e)
    planes = (xh, 1 - xh)
    other_core = {"seq_2": 1 - core}

    barrier = pltpu.get_barrier_semaphore()
    greeted = [seq_id(seq_peer(o)) for o in SEQ_OFFSETS] + [
        fsdp_id(fsdp_peer(o)) for o in FSDP_OFFSETS
    ]
    for peer in greeted:
        pl.semaphore_signal(barrier, inc=1, device_id=peer, device_id_type=MESH)

    def columns(s):
        return pl.ds(pl.multiple_of(s * HEAD, HEAD), HEAD)

    def chunk(s):
        return pl.ds(pl.multiple_of(s * IMAGE_CHUNK, IMAGE_CHUNK), IMAGE_CHUNK)

    def token_slot(p, r, h):
        start = ((p * 4 + r) * 2 + core) * IMAGE_CHUNK + h * half
        return tokens.at[pl.ds(pl.multiple_of(start, half), half), :]

    def weight_slot(p, r, h):
        start = (p * 4 + r) * WEIGHT_ROWS + h * whalf
        return weights.at[0, pl.ds(pl.multiple_of(start, whalf), whalf), :]

    group_rows = pl.ds(pl.multiple_of(group * WEIGHT_ROWS, WEIGHT_ROWS), WEIGHT_ROWS)
    fill_image = pltpu.make_async_copy(image, tokens.at[chunk(own), :], local_sems.at[0])
    fill_weights = [
        pltpu.make_async_copy(
            w_qkv.at[j, :, columns(own)],
            weights.at[0, group_rows, j * HEAD : (j + 1) * HEAD],
            local_sems.at[1 + j],
        )
        for j in range(3)
    ]
    fill_text = pltpu.make_async_copy(text, tokens.at[text_rows, :], local_sems.at[4])
    fill_upstream = [
        pltpu.make_async_copy(
            cotangent.at[:, columns(own)], upstream.at[chunk(own), :], local_sems.at[5]
        ),
        pltpu.make_async_copy(
            text_cotangent.at[:, columns(own)], upstream.at[text_rows, :], local_sems.at[6]
        ),
    ]
    for fill in (fill_image, *fill_weights, fill_text, *fill_upstream):
        fill.start()

    copies = Copies(send, recv)
    t = GatherRing(copies, token_slot, "seq_0", xh, "seq_1", z, True)
    w = GatherRing(copies, weight_slot, "fsdp_0", xl, "fsdp_1", y, False)
    shared = {}
    for plane, d in UNITS:
        for h in range(2):
            piece = token_slot(planes[plane], (z + d) % 4, h)
            shared[plane, d, h] = copies.make(piece, piece, other_core)
    exchanged = []
    for offset in SEQ_OFFSETS:
        peer = seq_peer(offset)
        s = (peer[0] * 4 + peer[1]) * 2 + peer[2]
        exchanged.append(
            copies.make(cotangent.at[:, columns(s)], upstream.at[chunk(own), :], seq_id(peer))
        )
    weights_shared = copies.make(weights.at[0], weights.at[1], other_core)

    def unit_at(plane, d):
        return planes[plane] * 4 + (z + d) % 4

    grads_shared = {}
    for plane, d in UNITS:
        at = unit_at(plane, d)
        grads_shared[plane, d] = copies.make(
            grads.at[chunk(at * 2 + 1 - core), :], grads_other.at[chunk(at), :], other_core
        )
    text_half = text_count // 2

    def text_share(c):
        return pl.ds(pl.multiple_of(IMAGE_ROWS + c * text_half, text_half), text_half)

    text_got = pl.ds(IMAGE_ROWS // 2, text_half)
    text_shared = copies.make(grads.at[text_share(1 - core), :], grads_other.at[text_got, :], other_core)
    gain_first = [
        copies.make(gain_seq.at[own], gain_seq.at[own], seq_id(seq_peer(o))) for o in SEQ_OFFSETS
    ]
    gain_second = [
        copies.make(gain_fsdp.at[group], gain_fsdp.at[group], fsdp_id(fsdp_peer(o)))
        for o in FSDP_OFFSETS
    ]
    other_pair = {"seq_0": 1 - xh}
    text_cross = copies.make(text_part.at[1 - xh], text_pair, other_pair)
    text_first, text_second = [], []
    for d in range(1, 4):
        at = (z + d) % 4
        text_first.append(copies.make(text_sum.at[at], text_in.at[z], {"seq_1": at}))
    for o in FSDP_OFFSETS:
        peer = seq_peer((o[0], o[1], 0))
        text_second.append(
            copies.make(
                text_all.at[core, xh, z],
                text_all.at[core, xh, z],
                {"seq_0": peer[0], "seq_1": peer[1]},
            )
        )
    text_third = copies.make(text_all.at[core], text_all.at[core], other_core)

    def dx_value(plane, d, h):
        start = (plane * 4 + d) * IMAGE_CHUNK + h * half
        return expd[start : start + half, : tokens.shape[1]]

    def dw_value(plane, d, h):
        f = (xl if plane == 0 else 1 - xl) * 4 + (y + d) % 4
        return dw[pl.ds(pl.multiple_of(f * WEIGHT_ROWS + h * whalf, whalf), whalf), :]

    dx_ring = ReduceRing(copies, dx_out, dx_in, dx_value, "seq_0", xh, "seq_1", z)
    dw_ring = PlainReduceRing(copies, dw_out, dw_in, dw_value, "fsdp_0", xl, "fsdp_1", y)

    fill_image.wait()
    pl.semaphore_wait(barrier, len(greeted))
    for h in range(2):
        t.cross[h].start()
        t.up[0][h].start()
        t.down[0][1 - h].start()
    for fill in fill_weights:
        fill.wait()
    for h in range(2):
        w.cross[h].start()
        w.up[0][h].start()
        w.down[0][1 - h].start()
    for h in range(2):
        shared[0, 0, h].start()

    def pass_weights(plane):
        w.up[plane][0].wait_recv()
        w.pass_up[plane].start()
        w.down[plane][1].wait_recv()
        w.pass_down[plane].start()

    t.up[0][0].wait_recv()
    t.pass_up[0].start()
    shared[0, 3, 0].start()
    t.down[0][1].wait_recv()
    t.pass_down[0].start()
    shared[0, 1, 1].start()
    pass_weights(0)
    for h in range(2):
        w.cross[h].wait_recv()
        w.up[1][h].start()
        w.down[1][h].start()
    for h in range(2):
        t.cross[h].wait_recv()
        t.up[1][h].start()
        t.down[1][h].start()
        shared[1, 0, h].start()
    t.up[0][1].wait_recv()
    shared[0, 3, 1].start()
    t.down[0][0].wait_recv()
    shared[0, 1, 0].start()
    pass_weights(1)
    t.pass_up[0].wait_recv()
    t.far[0].start()
    shared[0, 2, 0].start()
    t.pass_down[0].wait_recv()
    t.far[1].start()
    shared[0, 2, 1].start()
    for copy in exchanged:
        copy.start()
    for plane in range(2):
        w.up[plane][1].wait_recv()
        w.down[plane][0].wait_recv()
        w.pass_up[plane].wait_recv()
        w.pass_down[plane].wait_recv()
    weights_shared.start()

    def normed(values, gain):
        inverse = lax.rsqrt(jnp.mean(values * values, axis=-1, keepdims=True) + EPS)
        return (values * inverse * gain).astype(BF16)

    def project(start, count):
        at = pl.ds(start, count)
        result = dot_nn(tokens[at, :], weights[0]).astype(BF16)
        triple[at, :] = result
        qn[at, :] = normed(result[:, :HEAD].astype(F32), qgain[...])
        keys = normed(result[:, HEAD : 2 * HEAD].astype(F32), kgain[...])
        kn[at, :] = keys
        kn_t[:, at] = keys.T

    def unit_start(plane, d):
        return pl.multiple_of(unit_at(plane, d) * Q_ROWS, Q_ROWS)

    def project_unit(plane, d):
        for h in range(2):
            shared[plane, d, h].wait_recv()
        project(unit_start(plane, d), Q_ROWS)

    blocks = IMAGE_ROWS // Q_ROWS

    def exponentials(start, count, keys):
        at = pl.ds(start, count)
        qb = qn[at, :]
        total = jnp.zeros((8, count), F32)
        for key in keys:
            part = pl.ds(key, HEAD)
            e = jnp.exp2(dot_nt(kn[part, :], qb) * scale)
            expd[part, at] = e
            total = total + folded(e)
        esum[:, at] += total

    def plane_keys(plane):
        base = planes[plane] * (IMAGE_ROWS // 2)
        return [pl.multiple_of(base + c, HEAD) for c in range(0, IMAGE_ROWS // 2, HEAD)]

    def exponential_blocks(plane, keys):
        def block(i, carry):
            at = planes[plane] * (blocks // 2) + i
            exponentials(pl.multiple_of(at * Q_ROWS, Q_ROWS), Q_ROWS, keys)
            return carry

        lax.fori_loop(0, blocks // 2, block, 0)

    esum[...] = jnp.zeros_like(esum)
    fill_text.wait()
    project(IMAGE_ROWS, text_count)
    for d in range(4):
        project_unit(0, d)
    own_keys = plane_keys(0) + [IMAGE_ROWS]
    exponential_blocks(0, own_keys)
    exponentials(IMAGE_ROWS, text_count, own_keys)
    for h in range(2):
        t.up[1][h].wait_recv()
        shared[1, 3, h].start()
        t.down[1][h].wait_recv()
        shared[1, 1, h].start()
    project_unit(1, 0)
    project_unit(1, 1)
    project_unit(1, 3)
    for h in range(2):
        t.far[h].wait_recv()
        shared[1, 2, h].start()
    project_unit(1, 2)

    exponential_blocks(1, plane_keys(0) + plane_keys(1) + [IMAGE_ROWS])
    exponential_blocks(0, plane_keys(1))
    exponentials(IMAGE_ROWS, text_count, plane_keys(1))

    dv[...] = jnp.zeros_like(dv)
    gsum[...] = jnp.zeros_like(gsum)
    key_parts = [pl.ds(c, KEY_ROWS) for c in range(0, total_rows, KEY_ROWS)]

    def score_grads(start, count):
        at = pl.ds(start, count)
        ub = upstream[at, :]
        inner = jnp.zeros((8, count), F32)
        for part in key_parts:
            d = dot_nt(triple[part, 2 * HEAD :], ub)
            dpd[part, :count] = d
            inner = inner + folded(expd[part, at] * d)
        recip = 1.0 / jnp.sum(esum[:, at], axis=0, keepdims=True)
        delta = jnp.sum(inner, axis=0, keepdims=True) * recip
        for part in key_parts:
            p = expd[part, at] * recip
            dsd[part, at] = (p * (dpd[part, :count] - delta)).astype(BF16)
            dv[part, :] += dot_nn(p.astype(BF16), ub)

    for fill in fill_upstream:
        fill.wait()
    score_grads(IMAGE_ROWS, text_count)

    def score_block(i, carry):
        for plane in range(2):

            @pl.when(i == 4 * plane)
            def _():
                for offset, copy in zip(SEQ_OFFSETS, exchanged):
                    if offset[0] == plane:
                        copy.wait_recv()

        at = (xh + i // 4) % 2 * 4 + (z + i) % 4
        score_grads(pl.multiple_of(at * Q_ROWS, Q_ROWS), Q_ROWS)
        return carry

    lax.fori_loop(0, blocks, score_block, 0)

    def back(values, gain, incoming):
        floated = values.astype(F32)
        inverse = lax.rsqrt(jnp.mean(floated * floated, axis=-1, keepdims=True) + EPS)
        weighted = incoming * gain
        inner = jnp.mean(weighted * floated, axis=-1, keepdims=True)
        grad = inverse * weighted - floated * (inverse * inverse * inverse * inner)
        return grad.astype(BF16), folded(incoming * floated * inverse)

    def token_grads(start, count):
        at = pl.ds(start, count)
        dq = dot_nn(kn_t[...], dsd[:, at]).T * factor
        dk = dot_nn(dsd[at, :], qn[...]) * factor
        dq, q_part = back(triple[at, :HEAD], qgain[...], dq)
        dk, k_part = back(triple[at, HEAD : 2 * HEAD], kgain[...], dk)
        grads[at, :HEAD] = dq
        grads[at, HEAD : 2 * HEAD] = dk
        grads[at, 2 * HEAD :] = dv[at, :].astype(BF16)
        gsum[0:8, :] += q_part
        gsum[8:16, :] += k_part

    def unit_grads(plane, d):
        token_grads(unit_start(plane, d), Q_ROWS)
        grads_shared[plane, d].start()

    def input_part(mine, theirs):
        return dot_nt(grads[mine, :], weights[0]) + dot_nt(grads_other[theirs, :], weights[1])

    def input_sum(plane, d):
        at = unit_at(plane, d)
        grads_shared[plane, d].wait_recv()
        start = (plane * 4 + d) * IMAGE_CHUNK
        expd[start : start + IMAGE_CHUNK, : tokens.shape[1]] = input_part(
            chunk(at * 2 + core), chunk(at)
        )

    def weight_parts(plane):
        block = 2 * WEIGHT_ROWS
        pair = xl if plane == 0 else 1 - xl
        for j in range(2):
            at = pl.ds(pl.multiple_of((pair * 2 + j) * block, block), block)
            dw[at, :] = dot_tn(tokens[:, at], grads[...])

    unit_grads(1, 1)
    unit_grads(1, 2)
    weights_shared.wait_recv()
    input_sum(1, 1)
    dx_ring.send_up()
    input_sum(1, 2)
    dx_ring.send_far(0)
    unit_grads(1, 3)
    token_grads(IMAGE_ROWS, text_count)
    text_shared.start()
    input_sum(1, 3)
    dx_ring.send_down()
    text_shared.wait_recv()
    text_terms = input_part(text_share(core), text_got).astype(BF16)
    rows, width = text_part.shape[2:]
    for a, b in UNITS:
        text_part[a, b] = text_terms[b * rows : (b + 1) * rows, a * width : (a + 1) * width]
    text_cross.start()
    dx_ring.send_far(1)
    unit_grads(0, 2)
    unit_grads(0, 1)
    unit_grads(0, 3)
    text_cross.wait_recv()
    text_sum[...] = (text_part[xh].astype(F32) + text_pair[...].astype(F32)).astype(BF16)
    for copy in text_first:
        copy.start()
    text_in[z] = text_sum[z]
    unit_grads(1, 0)
    unit_grads(0, 0)
    gain_seq[own] = jnp.zeros(gain_seq.shape[1:], F32)
    gain_seq[own, 0:1, :] = jnp.sum(gsum[0:8, :], axis=0, keepdims=True)
    gain_seq[own, 1:2, :] = jnp.sum(gsum[8:16, :], axis=0, keepdims=True)
    for copy in gain_first:
        copy.start()
    input_sum(0, 2)
    dx_ring.own_far(0)
    weight_parts(1)
    dw_ring.first(1)
    input_sum(0, 1)
    dx_ring.own_up()
    dx_ring.own_far(1)
    input_sum(0, 3)
    dx_ring.own_down()
    for copy in text_first:
        copy.wait_recv()
    text_all[core, xh, z] = jnp.sum(text_in[...].astype(F32), axis=0).astype(BF16)
    for copy in text_second:
        copy.start()
    input_sum(1, 0)
    dx_ring.cross()
    weight_parts(0)
    dw_ring.pass_on(1)
    dw_ring.first(0)
    dx_ring.pass_on(0)
    for copy in gain_first:
        copy.wait_recv()
    gain_fsdp[group] = jnp.sum(gain_seq[...], axis=0)
    for copy in gain_second:
        copy.start()
    dw_ring.cross()
    dx_ring.pass_on(1)
    input_sum(0, 0)
    for copy in text_second:
        copy.wait_recv()
    text_third.start()
    dw_ring.pass_on(0)
    for copy in gain_second:
        copy.wait_recv()
    gain_out[...] = jnp.sum(gain_fsdp[...], axis=0)[0:2]
    for h in range(2):
        image_out[h * half : (h + 1) * half, :] = dx_ring.total(h).astype(BF16)
    for h in range(2):
        total = dw_ring.total(h)
        for j in range(3):
            weight_out[j, h * whalf : (h + 1) * whalf, :] = total[:, j * HEAD : (j + 1) * HEAD]
    text_third.wait_recv()
    for c in range(2):
        for a, b in UNITS:
            text_out[
                c * text_half + b * rows : c * text_half + (b + 1) * rows,
                a * width : (a + 1) * width,
            ] = text_all[c, a, b]
    for copy in copies.made:
        copy.wait_send()


def step(image, text, w_qkv, query_gain, key_gain, cotangent, text_cotangent):
    features = image.shape[1]
    text_count = text.shape[0]
    total = IMAGE_ROWS + text_count
    depth = w_qkv.shape[1] * 8
    hbm = pl.BlockSpec(memory_space=pltpu.HBM)
    vmem = pl.BlockSpec(memory_space=pltpu.VMEM)
    half, whalf = IMAGE_CHUNK // 2, WEIGHT_ROWS // 2
    text_piece = (2, 4, text_count // 8, features // 2)
    n_copies = (
        2 * GATHER_COPIES + 16 + len(SEQ_OFFSETS) + 1 + 9
        + len(SEQ_OFFSETS) + len(FSDP_OFFSETS) + 1 + 3 + len(FSDP_OFFSETS) + 1 + 2 * REDUCE_COPIES
    )
    return pl.pallas_call(
        step_kernel,
        out_shape=(
            jax.ShapeDtypeStruct((IMAGE_CHUNK, features), BF16),
            jax.ShapeDtypeStruct((text_count, features), BF16),
            jax.ShapeDtypeStruct((3, WEIGHT_ROWS, HEAD), F32),
            jax.ShapeDtypeStruct((2, HEAD), F32),
        ),
        in_specs=[hbm, hbm, hbm, vmem, vmem, hbm, hbm],
        out_specs=(vmem,) * 4,
        scratch_shapes=[
            pltpu.VMEM((total, features), BF16),
            pltpu.VMEM((2, depth, WIDTH), BF16),
            pltpu.VMEM((total, WIDTH), BF16),
            pltpu.VMEM((total, HEAD), BF16),
            pltpu.VMEM((total, HEAD), BF16),
            pltpu.VMEM((total, HEAD), BF16),
            pltpu.VMEM((HEAD, total), BF16),
            pltpu.VMEM((total, total), F32),
            pltpu.VMEM((8, total), F32),
            pltpu.VMEM((total, total), BF16),
            pltpu.VMEM((total, Q_ROWS), F32),
            pltpu.VMEM((total, HEAD), F32),
            pltpu.VMEM((16, HEAD), F32),
            pltpu.VMEM((total, WIDTH), BF16),
            pltpu.VMEM((total // 2, WIDTH), BF16),
            pltpu.VMEM((depth, WIDTH), F32),
            pltpu.VMEM((REDUCE_COPIES, half, features), BF16),
            pltpu.VMEM((REDUCE_COPIES, half, features), BF16),
            pltpu.VMEM((REDUCE_COPIES, whalf, WIDTH), BF16),
            pltpu.VMEM((REDUCE_COPIES, whalf, WIDTH), BF16),
            pltpu.VMEM(text_piece, BF16),
            pltpu.VMEM(text_piece[1:], BF16),
            pltpu.VMEM(text_piece[1:], BF16),
            pltpu.VMEM(text_piece[1:], BF16),
            pltpu.VMEM((2, *text_piece), BF16),
            pltpu.VMEM((16, 8, HEAD), F32),
            pltpu.VMEM((8, 8, HEAD), F32),
            pltpu.SemaphoreType.DMA((n_copies,)),
            pltpu.SemaphoreType.DMA((n_copies,)),
            pltpu.SemaphoreType.DMA((7,)),
        ],
        compiler_params=pltpu.CompilerParams(
            collective_id=0, has_side_effects=True, vmem_limit_bytes=62 * 1024 * 1024
        ),
        name="step",
    )(image, text, w_qkv, query_gain, key_gain, cotangent, text_cotangent)


def store_kernel(*refs):
    count = (len(refs) - 2) // 3
    taken, kept, held = refs[:count], refs[count : 2 * count], refs[2 * count : 3 * count]
    loads, stores = refs[-2:]
    ins = [pltpu.make_async_copy(taken[i], held[i], loads.at[i]) for i in range(count)]
    outs = [pltpu.make_async_copy(held[i], kept[i], stores.at[i]) for i in range(count)]
    for copy in ins:
        copy.start()
    for i in range(count):
        ins[i].wait()
        outs[i].start()
    for copy in outs:
        copy.wait()


def store(*arrays):
    hbm = pl.BlockSpec(memory_space=pltpu.HBM)
    return pl.pallas_call(
        store_kernel,
        out_shape=tuple(jax.ShapeDtypeStruct(a.shape, a.dtype) for a in arrays),
        in_specs=[hbm] * len(arrays),
        out_specs=(hbm,) * len(arrays),
        scratch_shapes=[pltpu.VMEM(a.shape, a.dtype) for a in arrays]
        + [pltpu.SemaphoreType.DMA((len(arrays),))] * 2,
        compiler_params=pltpu.CompilerParams(vmem_limit_bytes=67043328),
        name="store",
    )(*arrays)


def local(image_input, text_input, w_qkv, query_gain, key_gain, image_cotangent, text_cotangent):
    image_out, text_out, grad_weights, gain_total = store(
        *step(
            image_input[0],
            text_input[0],
            w_qkv.transpose(1, 0, 2),
            query_gain.reshape(1, HEAD),
            key_gain.reshape(1, HEAD),
            image_cotangent[0],
            text_cotangent[0],
        )
    )
    return image_out[None], text_out[None], grad_weights.transpose(1, 0, 2), gain_total


def solution(mesh):
    finer = Mesh(
        mesh.devices.reshape(2, 4, 2, 4, 2), ("fsdp_0", "fsdp_1", "seq_0", "seq_1", "seq_2")
    )
    return jax.shard_map(
        local,
        mesh=finer,
        in_specs=(
            P(FSDP, SEQ, None),
            P(FSDP, None, None),
            P(FSDP, None, None),
            P(),
            P(),
            P(FSDP, SEQ, None),
            P(FSDP, None, None),
        ),
        out_specs=(P(FSDP, SEQ, None), P(FSDP, None, None), P(FSDP, None, SEQ), P()),
        check_vma=False,
    )
```

```python
import math

import jax
import jax.numpy as jnp
from jax import lax
from jax.experimental import pallas as pl
from jax.experimental.pallas import tpu as pltpu
from jax.sharding import Mesh
from jax.sharding import PartitionSpec as P

HEAD = 128
SEQ = ("seq_0", "seq_1", "seq_2")
FSDP = ("fsdp_0", "fsdp_1")
EPS = 1e-06
F32 = jnp.float32
BF16 = jnp.bfloat16
MESH = pl.DeviceIdType.MESH

Q_ROWS = 256
KEY_ROWS = 544
IMAGE_CHUNK = 128
IMAGE_ROWS = 2048
WEIGHT_ROWS = 192
WIDTH = 3 * HEAD


def dot_nt(a, b):
    return lax.dot_general(a, b, (((1,), (1,)), ((), ())), preferred_element_type=F32)


def dot_nn(a, b):
    return lax.dot_general(a, b, (((1,), (0,)), ((), ())), preferred_element_type=F32)


def dot_tn(a, b):
    return lax.dot_general(a, b, (((0,), (0,)), ((), ())), preferred_element_type=F32)


def folded(values):
    rows, width = values.shape
    return jnp.sum(values.reshape(rows // 8, 8, width), axis=0)


class Copies:
    def __init__(self, send, recv):
        self.send, self.recv, self.made = send, recv, []

    def make(self, src, dst, to):
        i = len(self.made)
        copy = pltpu.make_async_remote_copy(
            src_ref=src,
            dst_ref=dst,
            send_sem=self.send.at[i],
            recv_sem=self.recv.at[i],
            device_id=to,
            device_id_type=MESH,
        )
        self.made.append(copy)
        return copy


def where():
    return (
        lax.axis_index("fsdp_0"),
        lax.axis_index("fsdp_1"),
        lax.axis_index("seq_0"),
        lax.axis_index("seq_1"),
        lax.axis_index("seq_2"),
    )


SEQ_OFFSETS = [(a, b, c) for a in range(2) for b in range(4) for c in range(2) if a + b + c > 0]
FSDP_OFFSETS = [(a, b) for a in range(2) for b in range(4) if a + b > 0]
UNITS = [(a, b) for a in range(2) for b in range(4)]


def seq_peer(offset):
    _, _, xh, z, core = where()
    return (xh + offset[0]) % 2, (z + offset[1]) % 4, (core + offset[2]) % 2


def fsdp_peer(offset):
    xl, y, _, _, _ = where()
    return (xl + offset[0]) % 2, (y + offset[1]) % 4


def seq_id(peer):
    return {"seq_0": peer[0], "seq_1": peer[1], "seq_2": peer[2]}


def fsdp_id(peer):
    return {"fsdp_0": peer[0], "fsdp_1": peer[1]}


class GatherRing:
    def __init__(self, copies, slot, pair_axis, pair, ring_axis, ring, far):
        self.planes = (pair, 1 - pair)
        after, before = {ring_axis: (ring + 1) % 4}, {ring_axis: (ring + 3) % 4}
        other = {pair_axis: 1 - pair}

        def same(piece, to):
            return copies.make(piece, piece, to)

        self.cross = [same(slot(pair, ring, h), other) for h in range(2)]
        self.up = [[same(slot(p, ring, h), after) for h in range(2)] for p in self.planes]
        self.down = [[same(slot(p, ring, h), before) for h in range(2)] for p in self.planes]
        passed = self.planes[:1] if far else self.planes
        self.pass_up = [same(slot(p, (ring + 3) % 4, 0), after) for p in passed]
        self.pass_down = [same(slot(p, (ring + 1) % 4, 1), before) for p in passed]
        if far:
            self.far = [same(slot(pair, (ring + 2) % 4, h), other) for h in range(2)]


GATHER_COPIES = 14


class ReduceRing:
    def __init__(self, copies, out, arrived, value, pair_axis, pair, ring_axis, ring):
        up, down = {ring_axis: (ring + 1) % 4}, {ring_axis: (ring + 3) % 4}
        other = {pair_axis: 1 - pair}
        to = [other] * 2 + [up] * 2 + [down] * 2 + [up] * 3 + [down] * 3 + [other] * 2
        self.out, self.arrived, self.value = out, arrived, value
        self.pieces = [copies.make(out.at[i], arrived.at[i], t) for i, t in enumerate(to)]

    def put(self, i, value):
        self.out[i] = value.astype(BF16)
        self.pieces[i].start()

    def got(self, i):
        self.pieces[i].wait_recv()
        return self.arrived[i].astype(F32)

    def send_far(self):
        self.put(0, self.value(1, 2, 0))
        self.put(1, self.value(1, 2, 1))

    def send_up(self):
        self.put(2, self.value(1, 1, 0))
        self.put(3, self.value(1, 1, 1))

    def send_down(self):
        self.put(4, self.value(1, 3, 0))
        self.put(5, self.value(1, 3, 1))

    def own_up(self):
        self.put(7, self.value(0, 1, 1))

    def own_down(self):
        self.put(10, self.value(0, 3, 0))

    def own_far(self, h):
        self.put((6, 9)[h], self.value(0, 2, h) + self.got(h))

    def pass_on(self, h):
        self.put((8, 11)[h], self.value(0, (1, 3)[h], h) + self.got((6, 9)[h]))

    def cross(self):
        self.put(12, self.value(1, 0, 0) + self.got(2) + self.got(4))
        self.put(13, self.value(1, 0, 1) + self.got(3) + self.got(5))

    def total(self, h):
        parts = ((8, 10, 12), (7, 11, 13))[h]
        result = self.value(0, 0, h)
        for i in parts:
            result = result + self.got(i)
        return result


class PlainReduceRing(ReduceRing):
    def __init__(self, copies, out, arrived, value, pair_axis, pair, ring_axis, ring):
        up, down = {ring_axis: (ring + 1) % 4}, {ring_axis: (ring + 3) % 4}
        to = ([up] * 3 + [down] * 3) * 2 + [{pair_axis: 1 - pair}] * 2
        self.out, self.arrived, self.value = out, arrived, value
        self.pieces = [copies.make(out.at[i], arrived.at[i], t) for i, t in enumerate(to)]

    def first(self, plane):
        base = 6 * (1 - plane)
        self.put(base, self.value(plane, 2, 0))
        self.put(base + 3, self.value(plane, 2, 1))
        self.put(base + 1, self.value(plane, 1, 1))
        self.put(base + 4, self.value(plane, 3, 0))

    def pass_on(self, plane):
        base = 6 * (1 - plane)
        self.put(base + 2, self.value(plane, 1, 0) + self.got(base))
        self.put(base + 5, self.value(plane, 3, 1) + self.got(base + 3))

    def own(self, plane, h):
        base = 6 * (1 - plane)
        near = self.got(base + (2, 1)[h]) + self.got(base + (4, 5)[h])
        return self.value(plane, 0, h) + near

    def cross(self):
        for h in range(2):
            self.put(12 + h, self.own(1, h))

    def total(self, h):
        return self.own(0, h) + self.got(12 + h)


REDUCE_COPIES = 14


def step_kernel(
    image, text, w_qkv, qgain, kgain, cotangent, text_cotangent,
    image_out, text_out, weight_out, gain_out,
    tokens, weights, triple, upstream, qn, kn, kn_t, expd, esum, dsd, dpd, dv, gsum,
    grads, grads_other, dw, dx_out, dx_in, dw_out, dw_in,
    text_part, text_pair, text_sum, text_in, text_all, gain_seq, gain_fsdp, send, recv, local_sems,
):
    xl, y, xh, z, core = where()
    own = (xh * 4 + z) * 2 + core
    group = xl * 4 + y
    half = IMAGE_CHUNK // 2
    whalf = WEIGHT_ROWS // 2
    total_rows = tokens.shape[0]
    text_count = text.shape[0]
    text_rows = pl.ds(IMAGE_ROWS, text_count)
    factor = 1.0 / math.sqrt(HEAD)
    scale = factor * math.log2(math.e)
    planes = (xh, 1 - xh)
    other_core = {"seq_2": 1 - core}

    barrier = pltpu.get_barrier_semaphore()
    greeted = [seq_id(seq_peer(o)) for o in SEQ_OFFSETS] + [
        fsdp_id(fsdp_peer(o)) for o in FSDP_OFFSETS
    ]
    for peer in greeted:
        pl.semaphore_signal(barrier, inc=1, device_id=peer, device_id_type=MESH)

    def columns(s):
        return pl.ds(pl.multiple_of(s * HEAD, HEAD), HEAD)

    def chunk(s):
        return pl.ds(pl.multiple_of(s * IMAGE_CHUNK, IMAGE_CHUNK), IMAGE_CHUNK)

    def token_slot(p, r, h):
        start = ((p * 4 + r) * 2 + core) * IMAGE_CHUNK + h * half
        return tokens.at[pl.ds(pl.multiple_of(start, half), half), :]

    def weight_slot(p, r, h):
        start = (p * 4 + r) * WEIGHT_ROWS + h * whalf
        return weights.at[0, pl.ds(pl.multiple_of(start, whalf), whalf), :]

    group_rows = pl.ds(pl.multiple_of(group * WEIGHT_ROWS, WEIGHT_ROWS), WEIGHT_ROWS)
    fill_image = pltpu.make_async_copy(image, tokens.at[chunk(own), :], local_sems.at[0])
    fill_weights = [
        pltpu.make_async_copy(
            w_qkv.at[j, :, columns(own)],
            weights.at[0, group_rows, j * HEAD : (j + 1) * HEAD],
            local_sems.at[1 + j],
        )
        for j in range(3)
    ]
    fill_text = pltpu.make_async_copy(text, tokens.at[text_rows, :], local_sems.at[4])
    fill_upstream = [
        pltpu.make_async_copy(
            cotangent.at[:, columns(own)], upstream.at[chunk(own), :], local_sems.at[5]
        ),
        pltpu.make_async_copy(
            text_cotangent.at[:, columns(own)], upstream.at[text_rows, :], local_sems.at[6]
        ),
    ]
    for fill in (fill_image, *fill_weights, fill_text, *fill_upstream):
        fill.start()

    copies = Copies(send, recv)
    t = GatherRing(copies, token_slot, "seq_0", xh, "seq_1", z, True)
    w = GatherRing(copies, weight_slot, "fsdp_0", xl, "fsdp_1", y, False)
    shared = {}
    for plane, d in UNITS:
        for h in range(2):
            piece = token_slot(planes[plane], (z + d) % 4, h)
            shared[plane, d, h] = copies.make(piece, piece, other_core)
    exchanged = []
    for offset in SEQ_OFFSETS:
        peer = seq_peer(offset)
        s = (peer[0] * 4 + peer[1]) * 2 + peer[2]
        exchanged.append(
            copies.make(cotangent.at[:, columns(s)], upstream.at[chunk(own), :], seq_id(peer))
        )
    weights_shared = copies.make(weights.at[0], weights.at[1], other_core)

    def unit_at(plane, d):
        return planes[plane] * 4 + (z + d) % 4

    grads_shared = {}
    for plane, d in UNITS:
        at = unit_at(plane, d)
        grads_shared[plane, d] = copies.make(
            grads.at[chunk(at * 2 + 1 - core), :], grads_other.at[chunk(at), :], other_core
        )
    text_half = text_count // 2

    def text_share(c):
        return pl.ds(pl.multiple_of(IMAGE_ROWS + c * text_half, text_half), text_half)

    text_got = pl.ds(IMAGE_ROWS // 2, text_half)
    text_shared = copies.make(grads.at[text_share(1 - core), :], grads_other.at[text_got, :], other_core)
    gain_first = [
        copies.make(gain_seq.at[own], gain_seq.at[own], seq_id(seq_peer(o))) for o in SEQ_OFFSETS
    ]
    gain_second = [
        copies.make(gain_fsdp.at[group], gain_fsdp.at[group], fsdp_id(fsdp_peer(o)))
        for o in FSDP_OFFSETS
    ]
    other_pair = {"seq_0": 1 - xh}
    text_cross = copies.make(text_part.at[1 - xh], text_pair, other_pair)
    text_first, text_second = [], []
    for d in range(1, 4):
        at = (z + d) % 4
        text_first.append(copies.make(text_sum.at[at], text_in.at[z], {"seq_1": at}))
    for o in FSDP_OFFSETS:
        peer = seq_peer((o[0], o[1], 0))
        text_second.append(
            copies.make(
                text_all.at[core, xh, z],
                text_all.at[core, xh, z],
                {"seq_0": peer[0], "seq_1": peer[1]},
            )
        )
    text_third = copies.make(text_all.at[core], text_all.at[core], other_core)

    def dx_value(plane, d, h):
        start = (plane * 4 + d) * IMAGE_CHUNK + h * half
        return expd[start : start + half, : tokens.shape[1]]

    def dw_value(plane, d, h):
        f = (xl if plane == 0 else 1 - xl) * 4 + (y + d) % 4
        return dw[pl.ds(pl.multiple_of(f * WEIGHT_ROWS + h * whalf, whalf), whalf), :]

    dx_ring = ReduceRing(copies, dx_out, dx_in, dx_value, "seq_0", xh, "seq_1", z)
    dw_ring = PlainReduceRing(copies, dw_out, dw_in, dw_value, "fsdp_0", xl, "fsdp_1", y)

    fill_image.wait()
    pl.semaphore_wait(barrier, len(greeted))
    for h in range(2):
        t.cross[h].start()
        t.up[0][h].start()
        t.down[0][1 - h].start()
    for fill in fill_weights:
        fill.wait()
    for h in range(2):
        w.cross[h].start()
        w.up[0][h].start()
        w.down[0][1 - h].start()
    for h in range(2):
        shared[0, 0, h].start()

    def pass_weights(plane):
        w.up[plane][0].wait_recv()
        w.pass_up[plane].start()
        w.down[plane][1].wait_recv()
        w.pass_down[plane].start()

    t.up[0][0].wait_recv()
    t.pass_up[0].start()
    shared[0, 3, 0].start()
    t.down[0][1].wait_recv()
    t.pass_down[0].start()
    shared[0, 1, 1].start()
    pass_weights(0)
    for h in range(2):
        w.cross[h].wait_recv()
        w.up[1][h].start()
        w.down[1][h].start()
    for h in range(2):
        t.cross[h].wait_recv()
        t.up[1][h].start()
        t.down[1][h].start()
        shared[1, 0, h].start()
    t.up[0][1].wait_recv()
    shared[0, 3, 1].start()
    t.down[0][0].wait_recv()
    shared[0, 1, 0].start()
    pass_weights(1)
    t.pass_up[0].wait_recv()
    t.far[0].start()
    shared[0, 2, 0].start()
    t.pass_down[0].wait_recv()
    t.far[1].start()
    shared[0, 2, 1].start()
    for plane in range(2):
        w.up[plane][1].wait_recv()
        w.down[plane][0].wait_recv()
        w.pass_up[plane].wait_recv()
        w.pass_down[plane].wait_recv()
    weights_shared.start()

    def normed(values, gain):
        inverse = lax.rsqrt(jnp.mean(values * values, axis=-1, keepdims=True) + EPS)
        return (values * inverse * gain).astype(BF16)

    def project(start, count):
        at = pl.ds(start, count)
        result = dot_nn(tokens[at, :], weights[0]).astype(BF16)
        triple[at, :] = result
        qn[at, :] = normed(result[:, :HEAD].astype(F32), qgain[...])
        keys = normed(result[:, HEAD : 2 * HEAD].astype(F32), kgain[...])
        kn[at, :] = keys
        kn_t[:, at] = keys.T

    def unit_start(plane, d):
        return pl.multiple_of(unit_at(plane, d) * Q_ROWS, Q_ROWS)

    def project_unit(plane, d):
        for h in range(2):
            shared[plane, d, h].wait_recv()
        project(unit_start(plane, d), Q_ROWS)

    blocks = IMAGE_ROWS // Q_ROWS

    def exponentials(start, count, keys):
        at = pl.ds(start, count)
        qb = qn[at, :]
        total = jnp.zeros((8, count), F32)
        for key in keys:
            part = pl.ds(key, HEAD)
            e = jnp.exp2(dot_nt(kn[part, :], qb) * scale)
            expd[part, at] = e
            total = total + folded(e)
        esum[:, at] += total

    def plane_keys(plane):
        base = planes[plane] * (IMAGE_ROWS // 2)
        return [pl.multiple_of(base + c, HEAD) for c in range(0, IMAGE_ROWS // 2, HEAD)]

    def exponential_blocks(plane, keys):
        def block(i, carry):
            at = planes[plane] * (blocks // 2) + i
            exponentials(pl.multiple_of(at * Q_ROWS, Q_ROWS), Q_ROWS, keys)
            return carry

        lax.fori_loop(0, blocks // 2, block, 0)

    esum[...] = jnp.zeros_like(esum)
    fill_text.wait()
    project(IMAGE_ROWS, text_count)
    for d in range(4):
        project_unit(0, d)
    own_keys = plane_keys(0) + [IMAGE_ROWS]
    exponential_blocks(0, own_keys)
    exponentials(IMAGE_ROWS, text_count, own_keys)
    for h in range(2):
        t.up[1][h].wait_recv()
        shared[1, 3, h].start()
        t.down[1][h].wait_recv()
        shared[1, 1, h].start()
    for copy in exchanged:
        copy.start()
    project_unit(1, 0)
    project_unit(1, 1)
    project_unit(1, 3)
    for h in range(2):
        t.far[h].wait_recv()
        shared[1, 2, h].start()
    project_unit(1, 2)

    exponential_blocks(1, plane_keys(0) + plane_keys(1) + [IMAGE_ROWS])
    exponential_blocks(0, plane_keys(1))
    exponentials(IMAGE_ROWS, text_count, plane_keys(1))

    dv[...] = jnp.zeros_like(dv)
    gsum[...] = jnp.zeros_like(gsum)
    key_parts = [pl.ds(c, KEY_ROWS) for c in range(0, total_rows, KEY_ROWS)]

    def score_grads(start, count):
        at = pl.ds(start, count)
        ub = upstream[at, :]
        inner = jnp.zeros((8, count), F32)
        for part in key_parts:
            d = dot_nt(triple[part, 2 * HEAD :], ub)
            dpd[part, :count] = d
            inner = inner + folded(expd[part, at] * d)
        recip = 1.0 / jnp.sum(esum[:, at], axis=0, keepdims=True)
        delta = jnp.sum(inner, axis=0, keepdims=True) * recip
        for part in key_parts:
            p = expd[part, at] * recip
            dsd[part, at] = (p * (dpd[part, :count] - delta)).astype(BF16)
            dv[part, :] += dot_nn(p.astype(BF16), ub)

    for fill in fill_upstream:
        fill.wait()
    score_grads(IMAGE_ROWS, text_count)

    def score_block(i, carry):
        for plane in range(2):

            @pl.when(i == 4 * plane)
            def _():
                for offset, copy in zip(SEQ_OFFSETS, exchanged):
                    if offset[0] == plane:
                        copy.wait_recv()

        at = (xh + i // 4) % 2 * 4 + (z + i) % 4
        score_grads(pl.multiple_of(at * Q_ROWS, Q_ROWS), Q_ROWS)
        return carry

    lax.fori_loop(0, blocks, score_block, 0)

    def back(values, gain, incoming):
        floated = values.astype(F32)
        inverse = lax.rsqrt(jnp.mean(floated * floated, axis=-1, keepdims=True) + EPS)
        weighted = incoming * gain
        inner = jnp.mean(weighted * floated, axis=-1, keepdims=True)
        grad = inverse * weighted - floated * (inverse * inverse * inverse * inner)
        return grad.astype(BF16), folded(incoming * floated * inverse)

    def token_grads(start, count):
        at = pl.ds(start, count)
        dq = dot_nn(kn_t[...], dsd[:, at]).T * factor
        dk = dot_nn(dsd[at, :], qn[...]) * factor
        dq, q_part = back(triple[at, :HEAD], qgain[...], dq)
        dk, k_part = back(triple[at, HEAD : 2 * HEAD], kgain[...], dk)
        grads[at, :HEAD] = dq
        grads[at, HEAD : 2 * HEAD] = dk
        grads[at, 2 * HEAD :] = dv[at, :].astype(BF16)
        gsum[0:8, :] += q_part
        gsum[8:16, :] += k_part

    def unit_grads(plane, d):
        token_grads(unit_start(plane, d), Q_ROWS)
        grads_shared[plane, d].start()

    def input_part(mine, theirs):
        return dot_nt(grads[mine, :], weights[0]) + dot_nt(grads_other[theirs, :], weights[1])

    def input_sum(plane, d):
        at = unit_at(plane, d)
        grads_shared[plane, d].wait_recv()
        start = (plane * 4 + d) * IMAGE_CHUNK
        expd[start : start + IMAGE_CHUNK, : tokens.shape[1]] = input_part(
            chunk(at * 2 + core), chunk(at)
        )

    def weight_parts(plane):
        block = 2 * WEIGHT_ROWS
        pair = xl if plane == 0 else 1 - xl
        for j in range(2):
            at = pl.ds(pl.multiple_of((pair * 2 + j) * block, block), block)
            dw[at, :] = dot_tn(tokens[:, at], grads[...])

    unit_grads(1, 1)
    unit_grads(1, 3)
    unit_grads(1, 2)
    weights_shared.wait_recv()
    input_sum(1, 1)
    dx_ring.send_up()
    input_sum(1, 3)
    dx_ring.send_down()
    input_sum(1, 2)
    dx_ring.send_far()
    unit_grads(0, 1)
    token_grads(IMAGE_ROWS, text_count)
    text_shared.start()
    input_sum(0, 1)
    dx_ring.own_up()
    unit_grads(0, 3)
    text_shared.wait_recv()
    text_terms = input_part(text_share(core), text_got).astype(BF16)
    rows, width = text_part.shape[2:]
    for a, b in UNITS:
        text_part[a, b] = text_terms[b * rows : (b + 1) * rows, a * width : (a + 1) * width]
    text_cross.start()
    input_sum(0, 3)
    dx_ring.own_down()
    unit_grads(0, 2)
    unit_grads(1, 0)
    unit_grads(0, 0)
    gain_seq[own] = jnp.zeros(gain_seq.shape[1:], F32)
    gain_seq[own, 0:1, :] = jnp.sum(gsum[0:8, :], axis=0, keepdims=True)
    gain_seq[own, 1:2, :] = jnp.sum(gsum[8:16, :], axis=0, keepdims=True)
    for copy in gain_first:
        copy.start()
    weight_parts(1)
    dw_ring.first(1)
    input_sum(0, 2)
    dx_ring.own_far(0)
    dx_ring.own_far(1)
    text_cross.wait_recv()
    text_sum[...] = (text_part[xh].astype(F32) + text_pair[...].astype(F32)).astype(BF16)
    for copy in text_first:
        copy.start()
    text_in[z] = text_sum[z]
    input_sum(1, 0)
    dx_ring.cross()
    weight_parts(0)
    dw_ring.pass_on(1)
    dw_ring.first(0)
    dx_ring.pass_on(0)
    dx_ring.pass_on(1)
    for copy in text_first:
        copy.wait_recv()
    text_all[core, xh, z] = jnp.sum(text_in[...].astype(F32), axis=0).astype(BF16)
    for copy in text_second:
        copy.start()
    dw_ring.cross()
    for copy in gain_first:
        copy.wait_recv()
    gain_fsdp[group] = jnp.sum(gain_seq[...], axis=0)
    for copy in gain_second:
        copy.start()
    input_sum(0, 0)
    dw_ring.pass_on(0)
    for copy in gain_second:
        copy.wait_recv()
    gain_out[...] = jnp.sum(gain_fsdp[...], axis=0)[0:2]
    for copy in text_second:
        copy.wait_recv()
    text_third.start()
    for h in range(2):
        image_out[h * half : (h + 1) * half, :] = dx_ring.total(h).astype(BF16)
    for h in range(2):
        total = dw_ring.total(h)
        for j in range(3):
            weight_out[j, h * whalf : (h + 1) * whalf, :] = total[:, j * HEAD : (j + 1) * HEAD]
    text_third.wait_recv()
    for c in range(2):
        for a, b in UNITS:
            text_out[
                c * text_half + b * rows : c * text_half + (b + 1) * rows,
                a * width : (a + 1) * width,
            ] = text_all[c, a, b]
    for copy in copies.made:
        copy.wait_send()


def step(image, text, w_qkv, query_gain, key_gain, cotangent, text_cotangent):
    features = image.shape[1]
    text_count = text.shape[0]
    total = IMAGE_ROWS + text_count
    depth = w_qkv.shape[1] * 8
    hbm = pl.BlockSpec(memory_space=pltpu.HBM)
    vmem = pl.BlockSpec(memory_space=pltpu.VMEM)
    half, whalf = IMAGE_CHUNK // 2, WEIGHT_ROWS // 2
    text_piece = (2, 4, text_count // 8, features // 2)
    n_copies = (
        2 * GATHER_COPIES + 16 + len(SEQ_OFFSETS) + 1 + 9
        + len(SEQ_OFFSETS) + len(FSDP_OFFSETS) + 1 + 3 + len(FSDP_OFFSETS) + 1 + 2 * REDUCE_COPIES
    )
    return pl.pallas_call(
        step_kernel,
        out_shape=(
            jax.ShapeDtypeStruct((IMAGE_CHUNK, features), BF16),
            jax.ShapeDtypeStruct((text_count, features), BF16),
            jax.ShapeDtypeStruct((3, WEIGHT_ROWS, HEAD), F32),
            jax.ShapeDtypeStruct((2, HEAD), F32),
        ),
        in_specs=[hbm, hbm, hbm, vmem, vmem, hbm, hbm],
        out_specs=(vmem,) * 4,
        scratch_shapes=[
            pltpu.VMEM((total, features), BF16),
            pltpu.VMEM((2, depth, WIDTH), BF16),
            pltpu.VMEM((total, WIDTH), BF16),
            pltpu.VMEM((total, HEAD), BF16),
            pltpu.VMEM((total, HEAD), BF16),
            pltpu.VMEM((total, HEAD), BF16),
            pltpu.VMEM((HEAD, total), BF16),
            pltpu.VMEM((total, total), F32),
            pltpu.VMEM((8, total), F32),
            pltpu.VMEM((total, total), BF16),
            pltpu.VMEM((total, Q_ROWS), F32),
            pltpu.VMEM((total, HEAD), F32),
            pltpu.VMEM((16, HEAD), F32),
            pltpu.VMEM((total, WIDTH), BF16),
            pltpu.VMEM((total // 2, WIDTH), BF16),
            pltpu.VMEM((depth, WIDTH), F32),
            pltpu.VMEM((REDUCE_COPIES, half, features), BF16),
            pltpu.VMEM((REDUCE_COPIES, half, features), BF16),
            pltpu.VMEM((REDUCE_COPIES, whalf, WIDTH), BF16),
            pltpu.VMEM((REDUCE_COPIES, whalf, WIDTH), BF16),
            pltpu.VMEM(text_piece, BF16),
            pltpu.VMEM(text_piece[1:], BF16),
            pltpu.VMEM(text_piece[1:], BF16),
            pltpu.VMEM(text_piece[1:], BF16),
            pltpu.VMEM((2, *text_piece), BF16),
            pltpu.VMEM((16, 8, HEAD), F32),
            pltpu.VMEM((8, 8, HEAD), F32),
            pltpu.SemaphoreType.DMA((n_copies,)),
            pltpu.SemaphoreType.DMA((n_copies,)),
            pltpu.SemaphoreType.DMA((7,)),
        ],
        compiler_params=pltpu.CompilerParams(
            collective_id=0, has_side_effects=True, vmem_limit_bytes=62 * 1024 * 1024
        ),
        name="step",
    )(image, text, w_qkv, query_gain, key_gain, cotangent, text_cotangent)


def store_kernel(*refs):
    count = (len(refs) - 2) // 3
    taken, kept, held = refs[:count], refs[count : 2 * count], refs[2 * count : 3 * count]
    loads, stores = refs[-2:]
    ins = [pltpu.make_async_copy(taken[i], held[i], loads.at[i]) for i in range(count)]
    outs = [pltpu.make_async_copy(held[i], kept[i], stores.at[i]) for i in range(count)]
    for copy in ins:
        copy.start()
    for i in range(count):
        ins[i].wait()
        outs[i].start()
    for copy in outs:
        copy.wait()


def store(*arrays):
    hbm = pl.BlockSpec(memory_space=pltpu.HBM)
    return pl.pallas_call(
        store_kernel,
        out_shape=tuple(jax.ShapeDtypeStruct(a.shape, a.dtype) for a in arrays),
        in_specs=[hbm] * len(arrays),
        out_specs=(hbm,) * len(arrays),
        scratch_shapes=[pltpu.VMEM(a.shape, a.dtype) for a in arrays]
        + [pltpu.SemaphoreType.DMA((len(arrays),))] * 2,
        compiler_params=pltpu.CompilerParams(vmem_limit_bytes=67043328),
        name="store",
    )(*arrays)


def local(image_input, text_input, w_qkv, query_gain, key_gain, image_cotangent, text_cotangent):
    image_out, text_out, grad_weights, gain_total = store(
        *step(
            image_input[0],
            text_input[0],
            w_qkv.transpose(1, 0, 2),
            query_gain.reshape(1, HEAD),
            key_gain.reshape(1, HEAD),
            image_cotangent[0],
            text_cotangent[0],
        )
    )
    return image_out[None], text_out[None], grad_weights.transpose(1, 0, 2), gain_total


def solution(mesh):
    finer = Mesh(
        mesh.devices.reshape(2, 4, 2, 4, 2), ("fsdp_0", "fsdp_1", "seq_0", "seq_1", "seq_2")
    )
    return jax.shard_map(
        local,
        mesh=finer,
        in_specs=(
            P(FSDP, SEQ, None),
            P(FSDP, None, None),
            P(FSDP, None, None),
            P(),
            P(),
            P(FSDP, SEQ, None),
            P(FSDP, None, None),
        ),
        out_specs=(P(FSDP, SEQ, None), P(FSDP, None, None), P(FSDP, None, SEQ), P()),
        check_vma=False,
    )
```

```python
import math

import jax
import jax.numpy as jnp
from jax import lax
from jax.experimental import pallas as pl
from jax.experimental.pallas import tpu as pltpu
from jax.sharding import Mesh
from jax.sharding import PartitionSpec as P

HEAD = 128
SEQ = ("seq_0", "seq_1", "seq_2")
FSDP = ("fsdp_0", "fsdp_1")
EPS = 1e-06
F32 = jnp.float32
BF16 = jnp.bfloat16
MESH = pl.DeviceIdType.MESH

Q_ROWS = 256
KEY_ROWS = 544
IMAGE_CHUNK = 128
IMAGE_ROWS = 2048
WEIGHT_ROWS = 192
WIDTH = 3 * HEAD


def dot_nt(a, b):
    return lax.dot_general(a, b, (((1,), (1,)), ((), ())), preferred_element_type=F32)


def dot_nn(a, b):
    return lax.dot_general(a, b, (((1,), (0,)), ((), ())), preferred_element_type=F32)


def dot_tn(a, b):
    return lax.dot_general(a, b, (((0,), (0,)), ((), ())), preferred_element_type=F32)


def folded(values):
    rows, width = values.shape
    return jnp.sum(values.reshape(rows // 8, 8, width), axis=0)


class Copies:
    def __init__(self, send, recv):
        self.send, self.recv, self.made = send, recv, []

    def make(self, src, dst, to):
        i = len(self.made)
        copy = pltpu.make_async_remote_copy(
            src_ref=src,
            dst_ref=dst,
            send_sem=self.send.at[i],
            recv_sem=self.recv.at[i],
            device_id=to,
            device_id_type=MESH,
        )
        self.made.append(copy)
        return copy


def where():
    return (
        lax.axis_index("fsdp_0"),
        lax.axis_index("fsdp_1"),
        lax.axis_index("seq_0"),
        lax.axis_index("seq_1"),
        lax.axis_index("seq_2"),
    )


SEQ_OFFSETS = [(a, b, c) for a in range(2) for b in range(4) for c in range(2) if a + b + c > 0]
FSDP_OFFSETS = [(a, b) for a in range(2) for b in range(4) if a + b > 0]
UNITS = [(a, b) for a in range(2) for b in range(4)]


def seq_peer(offset):
    _, _, xh, z, core = where()
    return (xh + offset[0]) % 2, (z + offset[1]) % 4, (core + offset[2]) % 2


def fsdp_peer(offset):
    xl, y, _, _, _ = where()
    return (xl + offset[0]) % 2, (y + offset[1]) % 4


def seq_id(peer):
    return {"seq_0": peer[0], "seq_1": peer[1], "seq_2": peer[2]}


def fsdp_id(peer):
    return {"fsdp_0": peer[0], "fsdp_1": peer[1]}


class GatherRing:
    def __init__(self, copies, slot, pair_axis, pair, ring_axis, ring, far):
        self.planes = (pair, 1 - pair)
        after, before = {ring_axis: (ring + 1) % 4}, {ring_axis: (ring + 3) % 4}
        other = {pair_axis: 1 - pair}

        def same(piece, to):
            return copies.make(piece, piece, to)

        self.cross = [same(slot(pair, ring, h), other) for h in range(2)]
        self.up = [[same(slot(p, ring, h), after) for h in range(2)] for p in self.planes]
        self.down = [[same(slot(p, ring, h), before) for h in range(2)] for p in self.planes]
        passed = self.planes[:1] if far else self.planes
        self.pass_up = [same(slot(p, (ring + 3) % 4, 0), after) for p in passed]
        self.pass_down = [same(slot(p, (ring + 1) % 4, 1), before) for p in passed]
        if far:
            self.far = [same(slot(pair, (ring + 2) % 4, h), other) for h in range(2)]


GATHER_COPIES = 14


class ReduceRing:
    def __init__(self, copies, out, arrived, value, pair_axis, pair, ring_axis, ring):
        up, down = {ring_axis: (ring + 1) % 4}, {ring_axis: (ring + 3) % 4}
        other = {pair_axis: 1 - pair}
        to = [other] * 2 + [up] * 2 + [down] * 2 + [up] * 3 + [down] * 3 + [other] * 2
        self.out, self.arrived, self.value = out, arrived, value
        self.pieces = [copies.make(out.at[i], arrived.at[i], t) for i, t in enumerate(to)]

    def put(self, i, value):
        self.out[i] = value.astype(BF16)
        self.pieces[i].start()

    def got(self, i):
        self.pieces[i].wait_recv()
        return self.arrived[i].astype(F32)

    def send_far(self, h):
        self.put(h, self.value(1, 2, h))

    def send_up(self):
        self.put(2, self.value(1, 1, 0))
        self.put(3, self.value(1, 1, 1))

    def send_down(self):
        self.put(4, self.value(1, 3, 0))
        self.put(5, self.value(1, 3, 1))

    def own_up(self):
        self.put(7, self.value(0, 1, 1))

    def own_down(self):
        self.put(10, self.value(0, 3, 0))

    def own_far(self, h):
        self.put((6, 9)[h], self.value(0, 2, h) + self.got(h))

    def pass_on(self, h):
        self.put((8, 11)[h], self.value(0, (1, 3)[h], h) + self.got((6, 9)[h]))

    def cross(self):
        self.put(12, self.value(1, 0, 0) + self.got(2) + self.got(4))
        self.put(13, self.value(1, 0, 1) + self.got(3) + self.got(5))

    def total(self, h):
        parts = ((8, 10, 12), (7, 11, 13))[h]
        result = self.value(0, 0, h)
        for i in parts:
            result = result + self.got(i)
        return result


class PlainReduceRing(ReduceRing):
    def __init__(self, copies, out, arrived, value, pair_axis, pair, ring_axis, ring):
        up, down = {ring_axis: (ring + 1) % 4}, {ring_axis: (ring + 3) % 4}
        to = ([up] * 3 + [down] * 3) * 2 + [{pair_axis: 1 - pair}] * 2
        self.out, self.arrived, self.value = out, arrived, value
        self.pieces = [copies.make(out.at[i], arrived.at[i], t) for i, t in enumerate(to)]

    def first(self, plane):
        base = 6 * (1 - plane)
        self.put(base, self.value(plane, 2, 0))
        self.put(base + 3, self.value(plane, 2, 1))
        self.put(base + 1, self.value(plane, 1, 1))
        self.put(base + 4, self.value(plane, 3, 0))

    def pass_on(self, plane):
        base = 6 * (1 - plane)
        self.put(base + 2, self.value(plane, 1, 0) + self.got(base))
        self.put(base + 5, self.value(plane, 3, 1) + self.got(base + 3))

    def own(self, plane, h):
        base = 6 * (1 - plane)
        near = self.got(base + (2, 1)[h]) + self.got(base + (4, 5)[h])
        return self.value(plane, 0, h) + near

    def cross(self):
        for h in range(2):
            self.put(12 + h, self.own(1, h))

    def total(self, h):
        return self.own(0, h) + self.got(12 + h)


REDUCE_COPIES = 14


def step_kernel(
    image, text, w_qkv, qgain, kgain, cotangent, text_cotangent,
    image_out, text_out, weight_out, gain_out,
    tokens, weights, triple, upstream, qn, kn, kn_t, expd, esum, dsd, dpd, dv, gsum,
    grads, grads_other, dw, dx_out, dx_in, dw_out, dw_in,
    text_part, text_pair, text_sum, text_in, text_all, gain_seq, gain_fsdp, send, recv, local_sems,
):
    xl, y, xh, z, core = where()
    own = (xh * 4 + z) * 2 + core
    group = xl * 4 + y
    half = IMAGE_CHUNK // 2
    whalf = WEIGHT_ROWS // 2
    total_rows = tokens.shape[0]
    text_count = text.shape[0]
    text_rows = pl.ds(IMAGE_ROWS, text_count)
    factor = 1.0 / math.sqrt(HEAD)
    scale = factor * math.log2(math.e)
    planes = (xh, 1 - xh)
    other_core = {"seq_2": 1 - core}

    barrier = pltpu.get_barrier_semaphore()
    greeted = [seq_id(seq_peer(o)) for o in SEQ_OFFSETS] + [
        fsdp_id(fsdp_peer(o)) for o in FSDP_OFFSETS
    ]
    for peer in greeted:
        pl.semaphore_signal(barrier, inc=1, device_id=peer, device_id_type=MESH)

    def columns(s):
        return pl.ds(pl.multiple_of(s * HEAD, HEAD), HEAD)

    def chunk(s):
        return pl.ds(pl.multiple_of(s * IMAGE_CHUNK, IMAGE_CHUNK), IMAGE_CHUNK)

    def token_slot(p, r, h):
        start = ((p * 4 + r) * 2 + core) * IMAGE_CHUNK + h * half
        return tokens.at[pl.ds(pl.multiple_of(start, half), half), :]

    def weight_slot(p, r, h):
        start = (p * 4 + r) * WEIGHT_ROWS + h * whalf
        return weights.at[0, pl.ds(pl.multiple_of(start, whalf), whalf), :]

    group_rows = pl.ds(pl.multiple_of(group * WEIGHT_ROWS, WEIGHT_ROWS), WEIGHT_ROWS)
    fill_image = pltpu.make_async_copy(image, tokens.at[chunk(own), :], local_sems.at[0])
    fill_weights = [
        pltpu.make_async_copy(
            w_qkv.at[j, :, columns(own)],
            weights.at[0, group_rows, j * HEAD : (j + 1) * HEAD],
            local_sems.at[1 + j],
        )
        for j in range(3)
    ]
    fill_text = pltpu.make_async_copy(text, tokens.at[text_rows, :], local_sems.at[4])
    fill_upstream = [
        pltpu.make_async_copy(
            cotangent.at[:, columns(own)], upstream.at[chunk(own), :], local_sems.at[5]
        ),
        pltpu.make_async_copy(
            text_cotangent.at[:, columns(own)], upstream.at[text_rows, :], local_sems.at[6]
        ),
    ]
    for fill in (fill_image, *fill_weights, fill_text, *fill_upstream):
        fill.start()

    copies = Copies(send, recv)
    t = GatherRing(copies, token_slot, "seq_0", xh, "seq_1", z, True)
    w = GatherRing(copies, weight_slot, "fsdp_0", xl, "fsdp_1", y, False)
    shared = {}
    for plane, d in UNITS:
        for h in range(2):
            piece = token_slot(planes[plane], (z + d) % 4, h)
            shared[plane, d, h] = copies.make(piece, piece, other_core)
    exchanged = []
    for offset in SEQ_OFFSETS:
        peer = seq_peer(offset)
        s = (peer[0] * 4 + peer[1]) * 2 + peer[2]
        exchanged.append(
            copies.make(cotangent.at[:, columns(s)], upstream.at[chunk(own), :], seq_id(peer))
        )
    weights_shared = copies.make(weights.at[0], weights.at[1], other_core)

    def unit_at(plane, d):
        return planes[plane] * 4 + (z + d) % 4

    grads_shared = {}
    for plane, d in UNITS:
        at = unit_at(plane, d)
        grads_shared[plane, d] = copies.make(
            grads.at[chunk(at * 2 + 1 - core), :], grads_other.at[chunk(at), :], other_core
        )
    text_half = text_count // 2

    def text_share(c):
        return pl.ds(pl.multiple_of(IMAGE_ROWS + c * text_half, text_half), text_half)

    text_got = pl.ds(IMAGE_ROWS // 2, text_half)
    text_shared = copies.make(grads.at[text_share(1 - core), :], grads_other.at[text_got, :], other_core)
    gain_first = [
        copies.make(gain_seq.at[own], gain_seq.at[own], seq_id(seq_peer(o))) for o in SEQ_OFFSETS
    ]
    gain_second = [
        copies.make(gain_fsdp.at[group], gain_fsdp.at[group], fsdp_id(fsdp_peer(o)))
        for o in FSDP_OFFSETS
    ]
    other_pair = {"seq_0": 1 - xh}
    text_cross = copies.make(text_part.at[1 - xh], text_pair, other_pair)
    text_first, text_second = [], []
    for d in range(1, 4):
        at = (z + d) % 4
        text_first.append(copies.make(text_sum.at[at], text_in.at[z], {"seq_1": at}))
    for o in FSDP_OFFSETS:
        peer = seq_peer((o[0], o[1], 0))
        text_second.append(
            copies.make(
                text_all.at[core, xh, z],
                text_all.at[core, xh, z],
                {"seq_0": peer[0], "seq_1": peer[1]},
            )
        )
    text_third = copies.make(text_all.at[core], text_all.at[core], other_core)

    def dx_value(plane, d, h):
        start = (plane * 4 + d) * IMAGE_CHUNK + h * half
        return expd[start : start + half, : tokens.shape[1]]

    def dw_value(plane, d, h):
        f = (xl if plane == 0 else 1 - xl) * 4 + (y + d) % 4
        return dw[pl.ds(pl.multiple_of(f * WEIGHT_ROWS + h * whalf, whalf), whalf), :]

    dx_ring = ReduceRing(copies, dx_out, dx_in, dx_value, "seq_0", xh, "seq_1", z)
    dw_ring = PlainReduceRing(copies, dw_out, dw_in, dw_value, "fsdp_0", xl, "fsdp_1", y)

    fill_image.wait()
    pl.semaphore_wait(barrier, len(greeted))
    for h in range(2):
        t.cross[h].start()
        t.up[0][h].start()
        t.down[0][1 - h].start()
    for fill in fill_weights:
        fill.wait()
    for h in range(2):
        w.cross[h].start()
        w.up[0][h].start()
        w.down[0][1 - h].start()
    for h in range(2):
        shared[0, 0, h].start()

    def pass_weights(plane):
        w.up[plane][0].wait_recv()
        w.pass_up[plane].start()
        w.down[plane][1].wait_recv()
        w.pass_down[plane].start()

    t.up[0][0].wait_recv()
    t.pass_up[0].start()
    shared[0, 3, 0].start()
    t.down[0][1].wait_recv()
    t.pass_down[0].start()
    shared[0, 1, 1].start()
    pass_weights(0)
    for h in range(2):
        w.cross[h].wait_recv()
        w.up[1][h].start()
        w.down[1][h].start()
    for h in range(2):
        t.cross[h].wait_recv()
        t.up[1][h].start()
        t.down[1][h].start()
        shared[1, 0, h].start()
    t.up[0][1].wait_recv()
    shared[0, 3, 1].start()
    t.down[0][0].wait_recv()
    shared[0, 1, 0].start()
    pass_weights(1)
    t.pass_up[0].wait_recv()
    t.far[0].start()
    shared[0, 2, 0].start()
    t.pass_down[0].wait_recv()
    t.far[1].start()
    shared[0, 2, 1].start()
    for plane in range(2):
        w.up[plane][1].wait_recv()
        w.down[plane][0].wait_recv()
        w.pass_up[plane].wait_recv()
        w.pass_down[plane].wait_recv()
    weights_shared.start()

    def normed(values, gain):
        inverse = lax.rsqrt(jnp.mean(values * values, axis=-1, keepdims=True) + EPS)
        return (values * inverse * gain).astype(BF16)

    def project(start, count):
        at = pl.ds(start, count)
        result = dot_nn(tokens[at, :], weights[0]).astype(BF16)
        triple[at, :] = result
        qn[at, :] = normed(result[:, :HEAD].astype(F32), qgain[...])
        keys = normed(result[:, HEAD : 2 * HEAD].astype(F32), kgain[...])
        kn[at, :] = keys
        kn_t[:, at] = keys.T

    def unit_start(plane, d):
        return pl.multiple_of(unit_at(plane, d) * Q_ROWS, Q_ROWS)

    def project_unit(plane, d):
        for h in range(2):
            shared[plane, d, h].wait_recv()
        project(unit_start(plane, d), Q_ROWS)

    blocks = IMAGE_ROWS // Q_ROWS

    def exponentials(start, count, keys):
        at = pl.ds(start, count)
        qb = qn[at, :]
        total = jnp.zeros((8, count), F32)
        for key in keys:
            part = pl.ds(key, HEAD)
            e = jnp.exp2(dot_nt(kn[part, :], qb) * scale)
            expd[part, at] = e
            total = total + folded(e)
        esum[:, at] += total

    def plane_keys(plane):
        base = planes[plane] * (IMAGE_ROWS // 2)
        return [pl.multiple_of(base + c, HEAD) for c in range(0, IMAGE_ROWS // 2, HEAD)]

    def exponential_blocks(plane, keys):
        def block(i, carry):
            at = planes[plane] * (blocks // 2) + i
            exponentials(pl.multiple_of(at * Q_ROWS, Q_ROWS), Q_ROWS, keys)
            return carry

        lax.fori_loop(0, blocks // 2, block, 0)

    esum[...] = jnp.zeros_like(esum)
    fill_text.wait()
    project(IMAGE_ROWS, text_count)
    for d in range(4):
        project_unit(0, d)
    own_keys = plane_keys(0) + [IMAGE_ROWS]
    exponential_blocks(0, own_keys)
    exponentials(IMAGE_ROWS, text_count, own_keys)
    for h in range(2):
        t.up[1][h].wait_recv()
        shared[1, 3, h].start()
        t.down[1][h].wait_recv()
        shared[1, 1, h].start()
    for copy in exchanged:
        copy.start()
    project_unit(1, 0)
    project_unit(1, 1)
    project_unit(1, 3)
    for h in range(2):
        t.far[h].wait_recv()
        shared[1, 2, h].start()
    project_unit(1, 2)

    exponential_blocks(1, plane_keys(0) + plane_keys(1) + [IMAGE_ROWS])
    exponential_blocks(0, plane_keys(1))
    exponentials(IMAGE_ROWS, text_count, plane_keys(1))

    dv[...] = jnp.zeros_like(dv)
    gsum[...] = jnp.zeros_like(gsum)
    key_parts = [pl.ds(c, KEY_ROWS) for c in range(0, total_rows, KEY_ROWS)]

    def score_grads(start, count):
        at = pl.ds(start, count)
        ub = upstream[at, :]
        inner = jnp.zeros((8, count), F32)
        for part in key_parts:
            d = dot_nt(triple[part, 2 * HEAD :], ub)
            dpd[part, :count] = d
            inner = inner + folded(expd[part, at] * d)
        recip = 1.0 / jnp.sum(esum[:, at], axis=0, keepdims=True)
        delta = jnp.sum(inner, axis=0, keepdims=True) * recip
        for part in key_parts:
            p = expd[part, at] * recip
            dsd[part, at] = (p * (dpd[part, :count] - delta)).astype(BF16)
            dv[part, :] += dot_nn(p.astype(BF16), ub)

    for fill in fill_upstream:
        fill.wait()
    score_grads(IMAGE_ROWS, text_count)

    def score_block(i, carry):
        for plane in range(2):

            @pl.when(i == 4 * plane)
            def _():
                for offset, copy in zip(SEQ_OFFSETS, exchanged):
                    if offset[0] == plane:
                        copy.wait_recv()

        at = (xh + i // 4) % 2 * 4 + (z + i) % 4
        score_grads(pl.multiple_of(at * Q_ROWS, Q_ROWS), Q_ROWS)
        return carry

    lax.fori_loop(0, blocks, score_block, 0)

    def back(values, gain, incoming):
        floated = values.astype(F32)
        inverse = lax.rsqrt(jnp.mean(floated * floated, axis=-1, keepdims=True) + EPS)
        weighted = incoming * gain
        inner = jnp.mean(weighted * floated, axis=-1, keepdims=True)
        grad = inverse * weighted - floated * (inverse * inverse * inverse * inner)
        return grad.astype(BF16), folded(incoming * floated * inverse)

    def token_grads(start, count):
        at = pl.ds(start, count)
        dq = dot_nn(kn_t[...], dsd[:, at]).T * factor
        dk = dot_nn(dsd[at, :], qn[...]) * factor
        dq, q_part = back(triple[at, :HEAD], qgain[...], dq)
        dk, k_part = back(triple[at, HEAD : 2 * HEAD], kgain[...], dk)
        grads[at, :HEAD] = dq
        grads[at, HEAD : 2 * HEAD] = dk
        grads[at, 2 * HEAD :] = dv[at, :].astype(BF16)
        gsum[0:8, :] += q_part
        gsum[8:16, :] += k_part

    def unit_grads(plane, d):
        token_grads(unit_start(plane, d), Q_ROWS)
        grads_shared[plane, d].start()

    def input_part(mine, theirs):
        return dot_nt(grads[mine, :], weights[0]) + dot_nt(grads_other[theirs, :], weights[1])

    def input_sum(plane, d):
        at = unit_at(plane, d)
        grads_shared[plane, d].wait_recv()
        start = (plane * 4 + d) * IMAGE_CHUNK
        expd[start : start + IMAGE_CHUNK, : tokens.shape[1]] = input_part(
            chunk(at * 2 + core), chunk(at)
        )

    def weight_parts(plane):
        block = 2 * WEIGHT_ROWS
        pair = xl if plane == 0 else 1 - xl
        for j in range(2):
            at = pl.ds(pl.multiple_of((pair * 2 + j) * block, block), block)
            dw[at, :] = dot_tn(tokens[:, at], grads[...])

    unit_grads(1, 1)
    unit_grads(1, 2)
    weights_shared.wait_recv()
    input_sum(1, 1)
    dx_ring.send_up()
    input_sum(1, 2)
    dx_ring.send_far(0)
    unit_grads(1, 3)
    input_sum(1, 3)
    dx_ring.send_down()
    token_grads(IMAGE_ROWS, text_count)
    text_shared.start()
    text_shared.wait_recv()
    text_terms = input_part(text_share(core), text_got).astype(BF16)
    rows, width = text_part.shape[2:]
    for a, b in UNITS:
        text_part[a, b] = text_terms[b * rows : (b + 1) * rows, a * width : (a + 1) * width]
    text_cross.start()
    dx_ring.send_far(1)
    unit_grads(0, 2)
    unit_grads(0, 1)
    unit_grads(0, 3)
    text_cross.wait_recv()
    text_sum[...] = (text_part[xh].astype(F32) + text_pair[...].astype(F32)).astype(BF16)
    for copy in text_first:
        copy.start()
    text_in[z] = text_sum[z]
    unit_grads(1, 0)
    unit_grads(0, 0)
    gain_seq[own] = jnp.zeros(gain_seq.shape[1:], F32)
    gain_seq[own, 0:1, :] = jnp.sum(gsum[0:8, :], axis=0, keepdims=True)
    gain_seq[own, 1:2, :] = jnp.sum(gsum[8:16, :], axis=0, keepdims=True)
    for copy in gain_first:
        copy.start()
    input_sum(0, 2)
    dx_ring.own_far(0)
    weight_parts(1)
    dw_ring.first(1)
    input_sum(0, 1)
    dx_ring.own_up()
    dx_ring.own_far(1)
    input_sum(0, 3)
    dx_ring.own_down()
    for copy in text_first:
        copy.wait_recv()
    text_all[core, xh, z] = jnp.sum(text_in[...].astype(F32), axis=0).astype(BF16)
    for copy in text_second:
        copy.start()
    input_sum(1, 0)
    dx_ring.cross()
    weight_parts(0)
    dw_ring.pass_on(1)
    dw_ring.first(0)
    dx_ring.pass_on(0)
    for copy in gain_first:
        copy.wait_recv()
    gain_fsdp[group] = jnp.sum(gain_seq[...], axis=0)
    for copy in gain_second:
        copy.start()
    dw_ring.cross()
    dx_ring.pass_on(1)
    input_sum(0, 0)
    for copy in text_second:
        copy.wait_recv()
    text_third.start()
    dw_ring.pass_on(0)
    for copy in gain_second:
        copy.wait_recv()
    gain_out[...] = jnp.sum(gain_fsdp[...], axis=0)[0:2]
    for h in range(2):
        image_out[h * half : (h + 1) * half, :] = dx_ring.total(h).astype(BF16)
    for h in range(2):
        total = dw_ring.total(h)
        for j in range(3):
            weight_out[j, h * whalf : (h + 1) * whalf, :] = total[:, j * HEAD : (j + 1) * HEAD]
    text_third.wait_recv()
    for c in range(2):
        for a, b in UNITS:
            text_out[
                c * text_half + b * rows : c * text_half + (b + 1) * rows,
                a * width : (a + 1) * width,
            ] = text_all[c, a, b]
    for copy in copies.made:
        copy.wait_send()


def step(image, text, w_qkv, query_gain, key_gain, cotangent, text_cotangent):
    features = image.shape[1]
    text_count = text.shape[0]
    total = IMAGE_ROWS + text_count
    depth = w_qkv.shape[1] * 8
    hbm = pl.BlockSpec(memory_space=pltpu.HBM)
    vmem = pl.BlockSpec(memory_space=pltpu.VMEM)
    half, whalf = IMAGE_CHUNK // 2, WEIGHT_ROWS // 2
    text_piece = (2, 4, text_count // 8, features // 2)
    n_copies = (
        2 * GATHER_COPIES + 16 + len(SEQ_OFFSETS) + 1 + 9
        + len(SEQ_OFFSETS) + len(FSDP_OFFSETS) + 1 + 3 + len(FSDP_OFFSETS) + 1 + 2 * REDUCE_COPIES
    )
    return pl.pallas_call(
        step_kernel,
        out_shape=(
            jax.ShapeDtypeStruct((IMAGE_CHUNK, features), BF16),
            jax.ShapeDtypeStruct((text_count, features), BF16),
            jax.ShapeDtypeStruct((3, WEIGHT_ROWS, HEAD), F32),
            jax.ShapeDtypeStruct((2, HEAD), F32),
        ),
        in_specs=[hbm, hbm, hbm, vmem, vmem, hbm, hbm],
        out_specs=(vmem,) * 4,
        scratch_shapes=[
            pltpu.VMEM((total, features), BF16),
            pltpu.VMEM((2, depth, WIDTH), BF16),
            pltpu.VMEM((total, WIDTH), BF16),
            pltpu.VMEM((total, HEAD), BF16),
            pltpu.VMEM((total, HEAD), BF16),
            pltpu.VMEM((total, HEAD), BF16),
            pltpu.VMEM((HEAD, total), BF16),
            pltpu.VMEM((total, total), F32),
            pltpu.VMEM((8, total), F32),
            pltpu.VMEM((total, total), BF16),
            pltpu.VMEM((total, Q_ROWS), F32),
            pltpu.VMEM((total, HEAD), F32),
            pltpu.VMEM((16, HEAD), F32),
            pltpu.VMEM((total, WIDTH), BF16),
            pltpu.VMEM((total // 2, WIDTH), BF16),
            pltpu.VMEM((depth, WIDTH), F32),
            pltpu.VMEM((REDUCE_COPIES, half, features), BF16),
            pltpu.VMEM((REDUCE_COPIES, half, features), BF16),
            pltpu.VMEM((REDUCE_COPIES, whalf, WIDTH), BF16),
            pltpu.VMEM((REDUCE_COPIES, whalf, WIDTH), BF16),
            pltpu.VMEM(text_piece, BF16),
            pltpu.VMEM(text_piece[1:], BF16),
            pltpu.VMEM(text_piece[1:], BF16),
            pltpu.VMEM(text_piece[1:], BF16),
            pltpu.VMEM((2, *text_piece), BF16),
            pltpu.VMEM((16, 8, HEAD), F32),
            pltpu.VMEM((8, 8, HEAD), F32),
            pltpu.SemaphoreType.DMA((n_copies,)),
            pltpu.SemaphoreType.DMA((n_copies,)),
            pltpu.SemaphoreType.DMA((7,)),
        ],
        compiler_params=pltpu.CompilerParams(
            collective_id=0, has_side_effects=True, vmem_limit_bytes=62 * 1024 * 1024
        ),
        name="step",
    )(image, text, w_qkv, query_gain, key_gain, cotangent, text_cotangent)


def store_kernel(*refs):
    count = (len(refs) - 2) // 3
    taken, kept, held = refs[:count], refs[count : 2 * count], refs[2 * count : 3 * count]
    loads, stores = refs[-2:]
    ins = [pltpu.make_async_copy(taken[i], held[i], loads.at[i]) for i in range(count)]
    outs = [pltpu.make_async_copy(held[i], kept[i], stores.at[i]) for i in range(count)]
    for copy in ins:
        copy.start()
    for i in range(count):
        ins[i].wait()
        outs[i].start()
    for copy in outs:
        copy.wait()


def store(*arrays):
    hbm = pl.BlockSpec(memory_space=pltpu.HBM)
    return pl.pallas_call(
        store_kernel,
        out_shape=tuple(jax.ShapeDtypeStruct(a.shape, a.dtype) for a in arrays),
        in_specs=[hbm] * len(arrays),
        out_specs=(hbm,) * len(arrays),
        scratch_shapes=[pltpu.VMEM(a.shape, a.dtype) for a in arrays]
        + [pltpu.SemaphoreType.DMA((len(arrays),))] * 2,
        compiler_params=pltpu.CompilerParams(vmem_limit_bytes=67043328),
        name="store",
    )(*arrays)


def local(image_input, text_input, w_qkv, query_gain, key_gain, image_cotangent, text_cotangent):
    image_out, text_out, grad_weights, gain_total = store(
        *step(
            image_input[0],
            text_input[0],
            w_qkv.transpose(1, 0, 2),
            query_gain.reshape(1, HEAD),
            key_gain.reshape(1, HEAD),
            image_cotangent[0],
            text_cotangent[0],
        )
    )
    return image_out[None], text_out[None], grad_weights.transpose(1, 0, 2), gain_total


def solution(mesh):
    finer = Mesh(
        mesh.devices.reshape(2, 4, 2, 4, 2), ("fsdp_0", "fsdp_1", "seq_0", "seq_1", "seq_2")
    )
    return jax.shard_map(
        local,
        mesh=finer,
        in_specs=(
            P(FSDP, SEQ, None),
            P(FSDP, None, None),
            P(FSDP, None, None),
            P(),
            P(),
            P(FSDP, SEQ, None),
            P(FSDP, None, None),
        ),
        out_specs=(P(FSDP, SEQ, None), P(FSDP, None, None), P(FSDP, None, SEQ), P()),
        check_vma=False,
    )
```
